64 devices in a mesh: dp: 4 (over x, y), sp: 16 (over z, core).
Axes of the slice: x: 2, y: 2, z: 8, core: 2. Of those that a mesh axis runs over, the one named last changes fastest.
The devices are a block of a 4x4x8 slice.
Arguments:
- hidden: bfloat16 [4, 4096, 2048], P('dp', 'sp'), parts along dimension 0
- d_out: bfloat16 [4, 4096, 2048], P('dp', 'sp'), parts along dimension 0
- positions: int32 [4, 4096], P('dp', 'sp'), parts along dimension 0
- norm_gain: bfloat16 [2048], replicated
- w_query: bfloat16 [2048, 2048], replicated
- b_query: bfloat16 [2048], replicated
- w_key: bfloat16 [2048, 256], replicated
- b_key: bfloat16 [256], replicated
- w_value: bfloat16 [2048, 256], replicated
- b_value: bfloat16 [256], replicated
- w_out: bfloat16 [2048, 2048], replicated
Outputs:
- output 1: bfloat16 [4, 4096, 2048], P('dp', 'sp'), parts along dimension 0
- output 2: bfloat16 [4, 4096, 2048], P('dp', 'sp'), parts along dimension 0
- output 3: float32 [8192], P('dp'), parts along dimension 0
- output 4: float32 [8192, 2048], P('dp'), parts along dimension 0
- output 5: float32 [8192], P('dp'), parts along dimension 0
- output 6: float32 [8192, 256], P('dp'), parts along dimension 0
- output 7: float32 [1024], P('dp'), parts along dimension 0
- output 8: float32 [8192, 256], P('dp'), parts along dimension 0
- output 9: float32 [1024], P('dp'), parts along dimension 0
- output 10: float32 [8192, 2048], P('dp'), parts along dimension 0
There are 4 independent parts. The reference program is written for one: setup_inputs(seed, part) draws one part's arguments, and reference() takes and returns one part's arrays. A program takes and returns all parts, laid end to end along the dimension named above; an argument that names none is the same for every part.
All inputs are finite; a program needn't handle non-finite values.
Results may differ from the reference program's by a relative error of at most 0.02.
Values are sent between devices in bfloat16 or wider.
A program may use at most 768 MiB of HBM per device.

```python
import math
import jax
import jax.numpy as jnp
from jax import lax

D_MODEL = 2048
Q_HEADS = 16
KV_HEADS = 2
HEAD_DIM = 128
BATCH_SEQS = 1
SEQ_LEN = 4096

ROPE_BASE = 1000000.0
NORM_EPS = 1e-6


def setup_inputs(seed: int = 0, part: int = 0) -> dict:
    base_key = jax.random.key(seed)
    part_keys = jax.random.split(jax.random.fold_in(base_key, part), 4)
    shared_keys = jax.random.split(base_key, 8)
    kv_width = KV_HEADS * HEAD_DIM
    in_scale = D_MODEL ** -0.5
    act_shape = (BATCH_SEQS, SEQ_LEN, D_MODEL)
    hidden = jax.random.normal(part_keys[0], act_shape, jnp.float32)
    d_out = jax.random.normal(part_keys[1], act_shape, jnp.float32)
    pos_steps = jax.random.randint(part_keys[2], (BATCH_SEQS, SEQ_LEN), 1, 3)
    pos_starts = jax.random.randint(part_keys[3], (BATCH_SEQS, 1), 0, 1024)
    positions = jnp.cumsum(pos_steps, axis=1) - pos_steps[:, :1] + pos_starts
    norm_gain = jax.random.uniform(shared_keys[0], (D_MODEL,), jnp.float32, 0.5, 1.5)
    w_query = jax.random.normal(shared_keys[1], (D_MODEL, D_MODEL), jnp.float32) * in_scale
    b_query = jax.random.normal(shared_keys[2], (D_MODEL,), jnp.float32) * 0.3
    w_key = jax.random.normal(shared_keys[3], (D_MODEL, kv_width), jnp.float32) * in_scale
    b_key = jax.random.normal(shared_keys[4], (kv_width,), jnp.float32)
    w_value = jax.random.normal(shared_keys[5], (D_MODEL, kv_width), jnp.float32) * in_scale
    b_value = jax.random.normal(shared_keys[6], (kv_width,), jnp.float32) * 0.3
    w_out = jax.random.normal(shared_keys[7], (D_MODEL, D_MODEL), jnp.float32) * in_scale
    return dict(hidden=hidden.astype(jnp.bfloat16), d_out=d_out.astype(jnp.bfloat16),
                positions=positions.astype(jnp.int32), norm_gain=norm_gain.astype(jnp.bfloat16),
                w_query=w_query.astype(jnp.bfloat16), b_query=b_query.astype(jnp.bfloat16),
                w_key=w_key.astype(jnp.bfloat16), b_key=b_key.astype(jnp.bfloat16),
                w_value=w_value.astype(jnp.bfloat16), b_value=b_value.astype(jnp.bfloat16),
                w_out=w_out.astype(jnp.bfloat16))


def to_bf16(values_in):
    return values_in.astype(jnp.bfloat16).astype(jnp.float32)


def rope_tables(positions):
    half_dim = HEAD_DIM // 2
    inv_freq = ROPE_BASE ** (-jnp.arange(half_dim, dtype=jnp.float32) * (2.0 / HEAD_DIM))
    angles = positions.astype(jnp.float32)[..., None] * inv_freq
    return jnp.cos(angles)[:, :, None, :], jnp.sin(angles)[:, :, None, :]


def rotate(vec, cosine, sine):
    half_dim = vec.shape[-1] // 2
    first = vec[..., :half_dim]
    second = vec[..., half_dim:]
    return jnp.concatenate([first * cosine - second * sine, second * cosine + first * sine], axis=-1)


def attention(query, keys_h, values_h):
    group = Q_HEADS // KV_HEADS
    block_len = math.gcd(SEQ_LEN, max(8, (1 << 24) // (BATCH_SEQS * Q_HEADS * SEQ_LEN)))
    n_blocks = SEQ_LEN // block_len
    q_blocks = jnp.moveaxis(query.reshape(BATCH_SEQS, n_blocks, block_len, KV_HEADS, group, HEAD_DIM), 1, 0)
    key_pos = jnp.arange(SEQ_LEN)
    scale = HEAD_DIM ** -0.5

    def one_block(block_in):
        q_block, index = block_in
        scores = jnp.einsum('bqkgd,bskd->bkgqs', q_block, keys_h) * scale
        q_pos = index * block_len + jnp.arange(block_len)
        scores = jnp.where(key_pos[None, :] <= q_pos[:, None], scores, -1e30)
        probs = to_bf16(jax.nn.softmax(scores, axis=-1))
        return jnp.einsum('bkgqs,bskd->bqkgd', probs, values_h)

    out_blocks = lax.map(jax.checkpoint(one_block), (q_blocks, jnp.arange(n_blocks)))
    return jnp.moveaxis(out_blocks, 0, 1).reshape(BATCH_SEQS, SEQ_LEN, Q_HEADS, HEAD_DIM)


def reference(hidden, d_out, positions, norm_gain, w_query, b_query, w_key, b_key, w_value, b_value, w_out):
    cosine, sine = rope_tables(positions)

    def forward(x_in, gain_f, wq_f, bq_f, wk_f, bk_f, wv_f, bv_f, wo_f):
        inv_rms = lax.rsqrt(jnp.mean(x_in * x_in, axis=-1, keepdims=True) + NORM_EPS)
        normed = to_bf16(x_in * inv_rms * gain_f)
        q_pre = jnp.einsum('bsd,de->bse', normed, wq_f) + bq_f
        query = to_bf16(rotate(q_pre.reshape(BATCH_SEQS, SEQ_LEN, Q_HEADS, HEAD_DIM), cosine, sine))
        k_pre = jnp.einsum('bsd,de->bse', normed, wk_f) + bk_f
        keys_h = to_bf16(rotate(k_pre.reshape(BATCH_SEQS, SEQ_LEN, KV_HEADS, HEAD_DIM), cosine, sine))
        v_pre = jnp.einsum('bsd,de->bse', normed, wv_f) + bv_f
        values_h = to_bf16(v_pre).reshape(BATCH_SEQS, SEQ_LEN, KV_HEADS, HEAD_DIM)
        attended = to_bf16(attention(query, keys_h, values_h)).reshape(BATCH_SEQS, SEQ_LEN, D_MODEL)
        return x_in + jnp.einsum('bsd,de->bse', attended, wo_f)

    result, pullback = jax.vjp(forward, hidden.astype(jnp.float32), norm_gain.astype(jnp.float32),
                               w_query.astype(jnp.float32), b_query.astype(jnp.float32),
                               w_key.astype(jnp.float32), b_key.astype(jnp.float32),
                               w_value.astype(jnp.float32), b_value.astype(jnp.float32),
                               w_out.astype(jnp.float32))
    grads = pullback(d_out.astype(jnp.float32))
    return (result.astype(jnp.bfloat16), grads[0].astype(jnp.bfloat16), grads[1], grads[2], grads[3],
            grads[4], grads[5], grads[6], grads[7], grads[8])
```

```python
import functools, math
import jax
import jax.numpy as jnp
from jax import lax
from jax.experimental import pallas as pl
from jax.experimental.pallas import tpu as pltpu
from jax.sharding import PartitionSpec as P

HEAD_DIM = 128
ROPE_BASE = 1000000.0
NORM_EPS = 1e-6
MESH = pl.DeviceIdType.MESH
NSUB = 4
F32 = jnp.float32
BF16 = jnp.bfloat16
ANY = pl.BlockSpec(memory_space=pl.ANY)
VM = pl.BlockSpec(memory_space=pltpu.VMEM)


class Ring:
    def __init__(self, full, own, rows, nz, sems):
        self.full, self.own, self.rows, self.nz = full, own, rows, nz
        self.send, self.recv, self.dsend, self.drecv = sems
        self.sp = lax.axis_index('sp')
        self.dp = lax.axis_index('dp')
        self.z, self.c = self.sp // 2, self.sp % 2
        self.sub = rows // (2 * NSUB)
        self.nsend = 7 * NSUB

    def dev(self, z, c):
        return (self.dp, z * 2 + c)

    def where(self, d, j, z):
        s = j // (2 * NSUB)
        r = j % (2 * NSUB)
        half = (r // NSUB + d) % 2
        origin = (z + (self.nz - s if d == 0 else s)) % self.nz
        return pl.multiple_of((origin * 2 + self.c) * self.rows + half * (self.rows // 2) + (r % NSUB) * self.sub, self.sub)

    def ici(self, d, j, src=None):
        off = self.where(d, j, self.z)
        to = (self.z + (1 if d == 0 else self.nz - 1)) % self.nz
        return pltpu.make_async_remote_copy(
            src_ref=self.full.at[pl.ds(off, self.sub)] if src is None else src,
            dst_ref=self.full.at[pl.ds(off, self.sub)],
            send_sem=self.send.at[d, j], recv_sem=self.recv.at[d, j],
            device_id=self.dev(to, self.c), device_id_type=MESH)

    def d2d(self, d, j):
        frm = (self.z + (self.nz - 1 if d == 0 else 1)) % self.nz
        off = self.where(d, j, frm)
        return pltpu.make_async_remote_copy(
            src_ref=self.full.at[pl.ds(off, self.sub)], dst_ref=self.full.at[pl.ds(off, self.sub)],
            send_sem=self.dsend.at[d, j], recv_sem=self.drecv.at[d, j],
            device_id=self.dev(self.z, 1 - self.c), device_id_type=MESH)

    def d2d_own(self):
        off = pl.multiple_of(self.sp * self.rows, self.rows)
        return pltpu.make_async_remote_copy(
            src_ref=self.own, dst_ref=self.full.at[pl.ds(off, self.rows)],
            send_sem=self.dsend.at[2, 0], recv_sem=self.drecv.at[2, 0],
            device_id=self.dev(self.z, 1 - self.c), device_id_type=MESH)

    def start(self):
        @pl.loop(0, 2 * NSUB)
        def _(j):
            for d in range(2):
                half = (j // NSUB + d) % 2
                off = pl.multiple_of(half * (self.rows // 2) + (j % NSUB) * self.sub, self.sub)
                self.ici(d, j, self.own.at[pl.ds(off, self.sub)]).start()
        self.d2d_own().start()

    def tick(self, j):
        for d in range(2):
            self.ici(d, j).wait_recv()

            @pl.when(j + 2 * NSUB < self.nsend)
            def _():
                self.ici(d, j + 2 * NSUB).start()
            self.d2d(d, j).start()

    def finish_sends(self):
        @pl.loop(0, self.nsend)
        def _(j):
            for d in range(2):
                self.ici(d, j).wait_send()
                self.d2d(d, j).wait_send()
        self.d2d_own().wait_send()

    def wait_other(self, j):
        for d in range(2):
            self.d2d(d, j).wait_recv()


def ring_sems(nz):
    n = 7 * NSUB
    return [pltpu.SemaphoreType.DMA((2, n)), pltpu.SemaphoreType.DMA((2, n)),
            pltpu.SemaphoreType.DMA((3, n)), pltpu.SemaphoreType.DMA((3, n))]


def greet_all(n_sp):
    sp, dp = lax.axis_index('sp'), lax.axis_index('dp')
    bar = pltpu.get_barrier_semaphore()

    @pl.loop(1, n_sp)
    def _(o):
        pl.semaphore_signal(bar, inc=1, device_id=(dp, (sp + o) % n_sp), device_id_type=MESH)
    pl.semaphore_wait(bar, n_sp - 1)


def k1_kernel(n_sp, h_own, pos, wq, wk, wv, bq, bk, bv, hf, ht, qt, k_o, kt_o, v_o, vt_o, cs_o,
              pos_all, wq_v, wk_v, wv_v, hb, htb, qs, ks, kts, vs, vts, css, send, recv, dsend, drecv, psend, precv, lsem, osem):
    nz = n_sp // 2
    rows, dm = h_own.shape
    qw = wq_v.shape[1]
    sp, dp = lax.axis_index('sp'), lax.axis_index('dp')
    z, c = sp // 2, sp % 2
    heads = qw // HEAD_DIM
    half_dim = HEAD_DIM // 2
    ring = Ring(hf, h_own, rows, nz, (send, recv, dsend, drecv))
    wcopies = [pltpu.make_async_copy(wq.at[:, pl.ds(pl.multiple_of(c * qw, qw), qw)], wq_v, lsem.at[0]),
               pltpu.make_async_copy(wk.at[:, pl.ds(pl.multiple_of(c * HEAD_DIM, HEAD_DIM), HEAD_DIM)], wk_v, lsem.at[1]),
               pltpu.make_async_copy(wv.at[:, pl.ds(pl.multiple_of(c * HEAD_DIM, HEAD_DIM), HEAD_DIM)], wv_v, lsem.at[2])]
    pos_copy = pltpu.make_async_copy(pos, pos_all.at[sp], lsem.at[4])
    for w in wcopies:
        w.start()
    pos_copy.start()
    greet_all(n_sp)
    ring.start()
    own_in = pltpu.make_async_copy(h_own, hb, lsem.at[5])
    own_in.start()

    def pos_send(o):
        return pltpu.make_async_remote_copy(src_ref=pos, dst_ref=pos_all.at[sp], send_sem=psend.at[o], recv_sem=precv.at[o],
                                            device_id=(dp, (sp + o) % n_sp), device_id_type=MESH)

    @pl.loop(1, n_sp)
    def _(o):
        pos_send(o).start()
    own_in.wait()
    own_out = pltpu.make_async_copy(hb, hf.at[pl.ds(pl.multiple_of(sp * rows, rows), rows)], lsem.at[3])
    own_out.start()
    for w in wcopies:
        w.wait()
    pos_copy.wait()
    own_out.wait()

    @pl.loop(1, n_sp)
    def _(o):
        pos_send(o).wait()

    freq = jnp.exp(lax.broadcasted_iota(jnp.int32, (half_dim, 1), 0).astype(F32) * (-2.0 / HEAD_DIM * math.log(ROPE_BASE)))

    def outs(blk):
        cols = pl.ds(pl.multiple_of(blk * rows, rows), rows)
        return [pltpu.make_async_copy(htb, ht.at[:, cols], osem.at[0]),
                pltpu.make_async_copy(qs, qt.at[blk], osem.at[1]),
                pltpu.make_async_copy(ks, k_o.at[cols], osem.at[2]),
                pltpu.make_async_copy(kts, kt_o.at[:, cols], osem.at[3]),
                pltpu.make_async_copy(vs, v_o.at[cols], osem.at[4]),
                pltpu.make_async_copy(vts, vt_o.at[:, cols], osem.at[5]),
                pltpu.make_async_copy(css, cs_o.at[:, cols], osem.at[6])]

    def compute(n, blk):
        load = pltpu.make_async_copy(hf.at[pl.ds(pl.multiple_of(blk * rows, rows), rows)], hb, lsem.at[5])
        load.start()
        load.wait()
        @pl.when(n > 0)
        def _():
            for o in outs(blk):
                o.wait()
        ang = freq * pos_all[blk, 0:1, :].astype(F32)
        cos, sin = jnp.cos(ang), jnp.sin(ang)
        css[0:half_dim, :] = cos
        css[half_dim:, :] = sin
        h = hb[...]
        htb[...] = h.T

        def rope_t(t):
            a, b = t[:half_dim], t[half_dim:]
            return jnp.concatenate([a * cos - b * sin, b * cos + a * sin], axis=0)
        for g in range(heads // 2):
            cols = slice(g * 2 * HEAD_DIM, (g + 1) * 2 * HEAD_DIM)
            q = jnp.dot(h, wq_v[:, cols], preferred_element_type=F32) + bq_c(bq, c, qw, cols)
            t = q.T
            for e in range(2):
                hd = g * 2 + e
                qs[:, hd * rows:(hd + 1) * rows] = rope_t(t[e * HEAD_DIM:(e + 1) * HEAD_DIM]).astype(BF16)
        k = jnp.dot(h, wk_v[...], preferred_element_type=F32) + bk[pl.ds(c, 1), :]
        kt = rope_t(k.T)
        kts[...] = kt.astype(BF16)
        ks[...] = kt.T.astype(BF16)
        v = jnp.dot(h, wv_v[...], preferred_element_type=F32) + bv[pl.ds(c, 1), :]
        vs[...] = v.astype(BF16)
        vts[...] = v.T.astype(BF16)
        for o in outs(blk):
            o.start()

    def bq_c(bq, c, qw, cols):
        return bq[pl.ds(c, 1), cols]

    @pl.loop(0, n_sp)
    def _(n):
        m = n - 2
        s = m // 4
        b = jnp.where(s == 3, (m % 4) * 2, m % 4)
        other = jnp.where(n < 2, n, b // 2)
        left = b % 2 == 0
        dist = jnp.where(n < 2, 0, s + 1)

        @pl.when((n >= 2) & (m % 4 == 0))
        def _():
            @pl.loop(0, jnp.where(s == 3, NSUB, 2 * NSUB))
            def _(r):
                ring.tick(s * 2 * NSUB + r)

        @pl.when(n == 1)
        def _():
            ring.d2d_own().wait_recv()

        @pl.when((n >= 2) & (other == 1) & left)
        def _():
            @pl.loop(0, jnp.where(s == 3, NSUB, 2 * NSUB))
            def _(r):
                ring.wait_other(s * 2 * NSUB + r)
        zb = (z + jnp.where(left, nz - dist, dist)) % nz
        cb = jnp.where(other == 1, 1 - c, c)
        compute(n, zb * 2 + cb)
    for o in outs(0):
        o.wait()
    ring.finish_sends()


def k1(n_sp, h_own, pos8, wq, wk, wv, bq, bk, bv):
    rows, dm = h_own.shape
    seq = rows * n_sp
    nz = n_sp // 2
    qw = wq.shape[1] // 2
    heads = qw // HEAD_DIM
    sds = jax.ShapeDtypeStruct
    outs = [sds((seq, dm), BF16), sds((dm, seq), BF16), sds((n_sp, HEAD_DIM, heads * rows), BF16),
            sds((seq, HEAD_DIM), BF16), sds((HEAD_DIM, seq), BF16), sds((seq, HEAD_DIM), BF16), sds((HEAD_DIM, seq), BF16),
            sds((HEAD_DIM, seq), F32)]
    vm = pltpu.VMEM
    scratch = [vm((n_sp,) + pos8.shape, jnp.int32), vm((dm, qw), BF16), vm((dm, HEAD_DIM), BF16), vm((dm, HEAD_DIM), BF16),
               vm((rows, dm), BF16), vm((dm, rows), BF16), vm((HEAD_DIM, heads * rows), BF16),
               vm((rows, HEAD_DIM), BF16), vm((HEAD_DIM, rows), BF16), vm((rows, HEAD_DIM), BF16), vm((HEAD_DIM, rows), BF16),
               vm((HEAD_DIM, rows), F32)] + ring_sems(nz) + [
               pltpu.SemaphoreType.DMA((n_sp,)), pltpu.SemaphoreType.DMA((n_sp,)),
               pltpu.SemaphoreType.DMA((6,)), pltpu.SemaphoreType.DMA((7,))]
    return pl.pallas_call(
        functools.partial(k1_kernel, n_sp), out_shape=outs,
        in_specs=[ANY, ANY, ANY, ANY, ANY, VM, VM, VM], out_specs=[ANY] * len(outs), scratch_shapes=scratch,
        compiler_params=pltpu.CompilerParams(collective_id=0, has_side_effects=True, vmem_limit_bytes=60 * 2 ** 20),
        name='gather_project')(h_own, pos8, wq, wk, wv, bq, bk, bv)


LOG2E = math.log2(math.e)
NEG = -1e30

def split_scaled(q, scale):
    qs = q.astype(F32) * scale
    hi = qs.astype(BF16)
    lo = (qs - hi.astype(F32)).astype(BF16)
    return jnp.concatenate([hi, lo], axis=0)

def decode(n, nblk):
    one = int if isinstance(n, int) else (lambda x: x.astype(jnp.int32))
    j = sum(one(n >= i * (i + 1)) for i in range(1, nblk // 2))
    r = n - j * (j + 1)
    odd = one(r > j)
    return 2 * j + odd, r - odd * (j + 1)

def fwd_steps(nblk):
    return (nblk // 2) * (nblk // 2 + 1)

class Fwd:
    def __init__(self, nblk, rows, heads, qt, at, lse, kk, vt, qb, q2, acc, mx, cm, ls, al, rt, lsv, sb, pb, bias, ats, qsem, osem):
        self.__dict__.update(locals())
        self.bk = 2 * rows
        self.cols = [slice(g * rows, (g + 1) * rows) for g in range(heads)]
        self.halves = (range(0, heads // 2), range(heads // 2, heads))
        self.nstep = fwd_steps(nblk)

    def load_q(self, blk):
        return pltpu.make_async_copy(self.qt.at[blk], self.qb, self.qsem)

    def make_q2(self, blk):
        for g in range(self.heads):
            self.q2[blk % 2, :, self.cols[g]] = split_scaled(self.qb[:, self.cols[g]], LOG2E * HEAD_DIM ** -0.5)

    def prepare(self):
        for b in range(2):
            self.load_q(b).start()
            self.load_q(b).wait()
            self.make_q2(b)
        self.load_q(2).start()
        d = lax.broadcasted_iota(jnp.int32, (self.bk, self.rows), 0) - lax.broadcasted_iota(jnp.int32, (self.bk, self.rows), 1)
        self.bias[0] = jnp.zeros((self.bk, self.rows), F32)
        self.bias[1] = jnp.where(d <= 0, 0.0, NEG)
        self.bias[2] = jnp.where(d <= self.rows, 0.0, NEG)
        self.acc[...] = jnp.zeros_like(self.acc)
        self.pb[...] = jnp.zeros_like(self.pb)
        self.ls[...] = jnp.zeros_like(self.ls)
        self.al[...] = jnp.zeros_like(self.al)
        self.mx[...] = jnp.zeros_like(self.mx)
        self.scores(0, 0)

    def scores(self, n, part):
        blk, t = decode(n, self.nblk)
        kb = self.kk[pl.ds(pl.multiple_of(t * self.bk, self.bk), self.bk), :]
        kind = jnp.where(t == blk // 2, 1 + blk % 2, 0)
        for g in self.halves[part]:
            s = jnp.dot(kb, self.q2[blk % 2, :, self.cols[g]], preferred_element_type=F32) + self.bias[kind]
            self.sb[g] = s
            self.cm[:, self.cols[g]] = jnp.max(s.reshape(self.bk // 8, 8, self.rows), axis=0)

    def soft(self, n, part):
        blk, t = decode(n, self.nblk)
        for g in self.halves[part]:
            c = self.cols[g]
            m0 = jnp.where(t == 0, NEG, self.mx[0:1, c])
            m1 = jnp.maximum(m0, jnp.max(self.cm[:, c], axis=0, keepdims=True))
            p = jnp.exp2(self.sb[g] - m1)
            a = jnp.exp2(m0 - m1)
            self.mx[0:1, c] = m1
            self.al[0:1, c] = a
            self.ls[:, c] = self.ls[:, c] * a + jnp.sum(p.reshape(self.bk // 8, 8, self.rows), axis=0)
            self.pb[g] = p.astype(BF16)

    def values(self, n, part):
        blk, t = decode(n, self.nblk)
        vb = self.vt[:, pl.ds(pl.multiple_of(t * self.bk, self.bk), self.bk)]
        for g in self.halves[part]:
            c = self.cols[g]
            self.acc[:, c] = self.acc[:, c] * self.al[0:1, c] + jnp.dot(vb, self.pb[g], preferred_element_type=F32)

    def outs(self, blk, part):
        nh = self.heads // 2
        r = slice(part * nh * HEAD_DIM, (part + 1) * nh * HEAD_DIM)
        return pltpu.make_async_copy(self.ats.at[r], self.at.at[r, pl.ds(pl.multiple_of(blk * self.rows, self.rows), self.rows)], self.osem.at[part])

    def out_lse(self, blk):
        return pltpu.make_async_copy(self.lsv, self.lse.at[blk], self.osem.at[2])

    def finish(self, blk, part):
        @pl.when(blk > 0)
        def _():
            self.outs(blk, part).wait()
        for g in self.halves[part]:
            c = self.cols[g]
            self.ats[g * HEAD_DIM:(g + 1) * HEAD_DIM, :] = (self.acc[:, c] * self.rt[0:1, c]).astype(BF16)
        self.outs(blk, part).start()

    def end_block(self, blk):
        @pl.when(blk > 0)
        def _():
            self.out_lse(blk).wait()
        tot = jnp.sum(self.ls[...], axis=0, keepdims=True)
        self.rt[0:1, :] = 1.0 / tot
        self.lsv[0:1, :] = self.mx[0:1, :] + jnp.log2(tot)
        self.out_lse(blk).start()
        self.finish(blk, 0)

        @pl.when(blk + 2 < self.nblk)
        def _():
            self.load_q(blk + 2).wait()
            self.make_q2(blk + 2)

        @pl.when(blk + 3 < self.nblk)
        def _():
            self.load_q(blk + 3).start()

    def run(self, lo, hi, on_step=lambda n: None):
        @pl.loop(lo, hi)
        def _(n):
            on_step(n)
            self.step(n)
            blk, t = decode(n, self.nblk)

            @pl.when((t == 0) & (n > 0))
            def _():
                self.finish(blk - 1, 1)

            @pl.when(t == blk // 2)
            def _():
                self.end_block(blk)

    def drain(self):
        n, blk = self.nstep - 1, self.nblk - 1
        self.values(n, 1)
        self.finish(blk, 1)
        self.outs(blk, 0).wait()
        self.outs(blk, 1).wait()
        self.out_lse(blk).wait()

    def step(self, n):
        n1 = jnp.minimum(n + 1, self.nstep - 1)
        self.scores(n, 1)
        self.soft(n, 0)
        self.values(jnp.maximum(n - 1, 0), 1)
        self.scores(n1, 0)
        self.soft(n, 1)
        self.values(n, 0)


def fwd_scratch(nblk, rows, heads):
    vm = pltpu.VMEM
    w, seq, bk = heads * rows, nblk * rows, 2 * rows
    return [vm((seq, 2 * HEAD_DIM), BF16), vm((HEAD_DIM, seq), BF16), vm((HEAD_DIM, w), BF16), vm((2, 2 * HEAD_DIM, w), BF16), vm((HEAD_DIM, w), F32),
            vm((8, w), F32), vm((8, w), F32), vm((8, w), F32), vm((8, w), F32), vm((8, w), F32), vm((8, w), F32),
            vm((heads, bk, rows), F32), vm((heads, bk, rows), BF16), vm((3, bk, rows), F32), vm((heads * HEAD_DIM, rows), BF16),
            pltpu.SemaphoreType.DMA, pltpu.SemaphoreType.DMA((3,))]


NT = (((1,), (1,)), ((), ()))
SCALE = HEAD_DIM ** -0.5

def dot_nt(a, b):
    return lax.dot_general(a, b, NT, preferred_element_type=F32)

def decode_down(n, nq):
    one = int if isinstance(n, int) else (lambda x: x.astype(jnp.int32))
    k = sum(one(n >= nq * m - m * (m - 1) // 2) for m in range(1, nq))
    return nq - 1 - k, n - (nq * k - k * (k - 1) // 2)

def bwd_steps(nq):
    return nq * (nq + 1) // 2

class Bwd:
    def __init__(self, nq, rows, head, qt, at, lse, dqo, kk, kt, vv, dat, dlt, lsv, qb, q2, cs, dk, dv, dq, dbq, sb, dpb, pb, dsb, bias, dqs, psem, dqsem, on_chunk, on_tile):
        self.__dict__.update(locals())
        self.bk = 2 * rows
        self.nstep = bwd_steps(nq)
        self.cols = [slice(0, rows), slice(rows, 2 * rows)]

    def loads(self, i):
        slot = i % 2
        c = pl.ds(pl.multiple_of(self.head * self.rows, self.rows), self.rows)
        return [pltpu.make_async_copy(self.qt.at[2 * i + e, :, c], self.qb.at[slot, :, self.cols[e]], self.psem.at[slot, e]) for e in range(2)]

    def make_q2(self, i):
        for e in range(2):
            self.q2[i % 2, :, self.cols[e]] = split_scaled(self.qb[i % 2, :, self.cols[e]], LOG2E * SCALE)

    def prepare(self):
        nq = self.nq
        for i in (nq - 1, nq - 2):
            for cp in self.loads(i):
                cp.start()
            for cp in self.loads(i):
                cp.wait()
            self.make_q2(i)
        d = lax.broadcasted_iota(jnp.int32, (self.bk, self.rows), 0) - lax.broadcasted_iota(jnp.int32, (self.bk, self.rows), 1)
        self.bias[0] = jnp.zeros((self.bk, self.rows), F32)
        self.bias[1] = jnp.where(d <= 0, 0.0, NEG)
        self.bias[2] = jnp.where(d <= self.rows, 0.0, NEG)
        self.dk[...] = jnp.zeros_like(self.dk)
        self.dv[...] = jnp.zeros_like(self.dv)
        self.dq[...] = jnp.zeros_like(self.dq)
        self.dbq[...] = jnp.zeros_like(self.dbq)
        self.pb[...] = jnp.zeros_like(self.pb)
        self.dsb[...] = jnp.zeros_like(self.dsb)
        self.scores(0, 0)

    def keys(self, t):
        return pl.ds(pl.multiple_of(t * self.bk, self.bk), self.bk)

    def qcols(self, i, e):
        return pl.ds(pl.multiple_of(i * self.bk + e * self.rows, self.rows), self.rows)

    def scores(self, n, e):
        i, t = decode_down(n, self.nq)
        kind = jnp.where(t == i, 1 + e, 0)
        s = jnp.dot(self.kk[self.keys(t), :], self.q2[i % 2, :, self.cols[e]], preferred_element_type=F32)
        self.sb[e] = s + self.bias[kind]
        self.dpb[e] = jnp.dot(self.vv[self.keys(t), :], self.dat[:, self.qcols(i, e)], preferred_element_type=F32)

    def soft(self, n, e):
        i, t = decode_down(n, self.nq)
        c = self.qcols(i, e)
        p = jnp.exp2(self.sb[e] - self.lsv[0:1, c])
        self.pb[e] = p.astype(BF16)
        self.dsb[e] = (p * (self.dpb[e] - self.dlt[0:1, c])).astype(BF16)

    def grads(self, n, e):
        i, t = decode_down(n, self.nq)
        r = self.keys(t)
        self.dv[r, :] += dot_nt(self.pb[e], self.dat[:, self.qcols(i, e)])
        self.dk[r, :] += dot_nt(self.dsb[e], self.qb[i % 2, :, self.cols[e]])
        keep = jnp.where(t == 0, 0.0, 1.0)
        self.dq[:, self.cols[e]] = self.dq[:, self.cols[e]] * keep + jnp.dot(self.kt[:, self.keys(t)], self.dsb[e], preferred_element_type=F32)

    def step(self, n):
        n1 = jnp.minimum(n + 1, self.nstep - 1)
        self.scores(n, 1)
        self.soft(n, 0)
        self.grads(jnp.maximum(n - 1, 0), 1)
        self.scores(n1, 0)
        self.soft(n, 1)
        self.grads(n, 0)

    def finish(self, i, e):
        c = self.qcols(i, e)
        g = self.dq[:, self.cols[e]] * SCALE
        hd = HEAD_DIM // 2
        cos, sin = self.cs[0:hd, c], self.cs[hd:, c]
        a, b = g[:hd], g[hd:]
        a, b = a * cos + b * sin, b * cos - a * sin
        self.dbq[0:hd, :] += a
        self.dbq[hd:, :] += b
        blk = 2 * i + e
        self.dqs[blk, 0:hd, :] = a.astype(BF16)
        self.dqs[blk, hd:, :] = b.astype(BF16)
        self.on_chunk(blk)

    def run(self):
        @pl.loop(0, self.nstep)
        def _(n):
            self.step(n)
            i, t = decode_down(n, self.nq)

            @pl.when((t == 0) & (n > 0))
            def _():
                self.finish(i + 1, 1)
                self.on_tile(i + 1)

                @pl.when(i >= 1)
                def _():
                    for cp in self.loads(i - 1):
                        cp.start()
                    for cp in self.loads(i - 1):
                        cp.wait()
                    self.make_q2(i - 1)

            @pl.when(t == i)
            def _():
                self.finish(i, 0)
        self.grads(self.nstep - 1, 1)
        self.finish(0, 1)
        self.on_tile(0)


def bwd_scratch(nq, rows):
    vm = pltpu.VMEM
    bk, seq = 2 * rows, 2 * rows * nq
    return [vm((seq, 2 * HEAD_DIM), BF16), vm((HEAD_DIM, seq), BF16), vm((seq, HEAD_DIM), BF16), vm((HEAD_DIM, seq), BF16), vm((8, seq), F32), vm((8, seq), F32),
            vm((2, HEAD_DIM, bk), BF16), vm((2, 2 * HEAD_DIM, bk), BF16), vm((HEAD_DIM, seq), F32), vm((seq, HEAD_DIM), F32), vm((seq, HEAD_DIM), F32),
            vm((HEAD_DIM, bk), F32), vm((HEAD_DIM, rows), F32), vm((2, bk, rows), F32), vm((2, bk, rows), F32), vm((2, bk, rows), BF16), vm((2, bk, rows), BF16),
            vm((3, bk, rows), F32), vm((2 * nq, HEAD_DIM, rows), BF16), pltpu.SemaphoreType.DMA((2, 2)), pltpu.SemaphoreType.DMA((2 * nq,))]


def load_bwd(k_h, kt_h, v_h, cs_h, lse_h, head, rows, nblk, kk, kt, vv, cs, lsv, sem):
    cps = [pltpu.make_async_copy(k_h, kk.at[:, 0:HEAD_DIM], sem.at[0]), pltpu.make_async_copy(k_h, kk.at[:, HEAD_DIM:], sem.at[1]),
           pltpu.make_async_copy(kt_h, kt, sem.at[2]), pltpu.make_async_copy(v_h, vv, sem.at[3]), pltpu.make_async_copy(cs_h, cs, sem.at[4])]
    for c in cps:
        c.start()

    def lcopy(b):
        return pltpu.make_async_copy(lse_h.at[b, :, pl.ds(pl.multiple_of(head * rows, rows), rows)], lsv.at[:, pl.ds(pl.multiple_of(b * rows, rows), rows)], sem.at[5 + b])

    @pl.loop(0, nblk)
    def _(b):
        lcopy(b).start()
    for c in cps:
        c.wait()

    @pl.loop(0, nblk)
    def _(b):
        lcopy(b).wait()


def grad_att(dy_h, at_h, wo_h, head, seq, dat, dlt, wo_v, dyb, atb, sem):
    blk = dyb.shape[1]
    w = pltpu.make_async_copy(wo_h, wo_v, sem.at[2])
    w.start()

    def cp(b):
        s = b % 2
        r = pl.ds(pl.multiple_of(b * blk, blk), blk)
        return [pltpu.make_async_copy(dy_h.at[r], dyb.at[s], sem.at[s]),
                pltpu.make_async_copy(at_h.at[pl.ds(pl.multiple_of(head * HEAD_DIM, HEAD_DIM), HEAD_DIM), r], atb.at[s], sem.at[3 + s])]
    for c in cp(0):
        c.start()
    w.wait()
    nb = seq // blk

    @pl.loop(0, nb)
    def _(b):
        @pl.when(b + 1 < nb)
        def _():
            for c in cp(b + 1):
                c.start()
        for c in cp(b):
            c.wait()
        d = dot_nt(dyb[b % 2], wo_v[...]).T.astype(BF16)
        r = pl.ds(pl.multiple_of(b * blk, blk), blk)
        dat[:, r] = d
        dlt[0:1, r] = jnp.sum(d.astype(F32) * atb[b % 2].astype(F32), axis=0, keepdims=True)


def k2_kernel(n_sp, own_dy, qt, k_h, vt_h, dyf, at, lse, ao, *scr):
    *scr, send, recv, dsend, drecv, lsem, xsem = scr
    kk, vt, qb = scr[:3]
    rows = own_dy.shape[0]
    heads = qt.shape[2] // rows
    nz = n_sp // 2
    sp, dp = lax.axis_index('sp'), lax.axis_index('dp')
    ring = Ring(dyf, own_dy, rows, nz, (send, recv, dsend, drecv))
    loads = [pltpu.make_async_copy(k_h, kk.at[:, 0:HEAD_DIM], lsem.at[0]), pltpu.make_async_copy(k_h, kk.at[:, HEAD_DIM:], lsem.at[1]),
             pltpu.make_async_copy(vt_h, vt, lsem.at[2])]
    for c in loads:
        c.start()
    greet_all(n_sp)
    ring.start()
    mine = pltpu.make_async_copy(own_dy, dyf.at[pl.ds(pl.multiple_of(sp * rows, rows), rows)], lsem.at[3])
    mine.start()
    for c in loads:
        c.wait()
    f = Fwd(n_sp, rows, heads, qt, at, lse, *scr)
    f.prepare()

    def due(n):
        return jnp.clip((n - 2) * 5 // 11, 0, ring.nsend)

    def on_step(n):
        @pl.loop(due(n), due(n + 1))
        def _(j):
            ring.tick(j)
    f.run(0, f.nstep, on_step)
    f.drain()
    other = (sp // 2) * 2 + 1 - sp % 2
    give = pltpu.make_async_remote_copy(
        src_ref=at.at[:, pl.ds(pl.multiple_of(other * rows, rows), rows)], dst_ref=ao, send_sem=xsem.at[0], recv_sem=xsem.at[1],
        device_id=(dp, other), device_id_type=MESH)
    give.start()

    @pl.loop(due(f.nstep), ring.nsend)
    def _(j):
        ring.tick(j)

    @pl.loop(0, ring.nsend)
    def _(j):
        ring.wait_other(j)
    ring.d2d_own().wait_recv()
    give.wait()
    mine.wait()
    ring.finish_sends()


def k2(n_sp, own_dy, qt, k, vt):
    rows, dm = own_dy.shape
    seq = rows * n_sp
    heads = qt.shape[2] // rows
    sds = jax.ShapeDtypeStruct
    outs = [sds((seq, dm), BF16), sds((heads * HEAD_DIM, seq), BF16), sds((n_sp, 8, heads * rows), F32), sds((heads * HEAD_DIM, rows), BF16)]
    return pl.pallas_call(
        functools.partial(k2_kernel, n_sp), out_shape=outs, in_specs=[ANY] * 4, out_specs=[ANY] * 4,
        scratch_shapes=fwd_scratch(n_sp, rows, heads) + ring_sems(n_sp // 2) + [pltpu.SemaphoreType.DMA((4,)), pltpu.SemaphoreType.DMA((2,))],
        compiler_params=pltpu.CompilerParams(collective_id=1, has_side_effects=True, vmem_limit_bytes=62 * 2 ** 20),
        name='gather_attend')(own_dy, qt, k, vt)


def k3_kernel(nq, rows, qt, at, lse, k_h, kt_h, v_h, cs_h, dy_h, wo_h, dq_o, dk_o, dv_o, db_o, *scr):
    *scr, wo_v, dyb, atb, sem, sem2 = scr
    kk, kt, vv, dat, dlt, lsv, qb, q2, cs, dk, dv, dq, dbq, sb, dpb, pb, dsb, bias, dqs, psem, dqsem = scr
    sp = lax.axis_index('sp')
    head = sp // 2
    load_bwd(k_h, kt_h, v_h, cs_h, lse, head, rows, 2 * nq, kk, kt, vv, cs, lsv, sem)
    row0 = pl.multiple_of((sp % 2) * at.shape[0] + head * HEAD_DIM, HEAD_DIM)
    grad_att(dy_h, at, wo_h.at[pl.ds(row0, HEAD_DIM)], head, dy_h.shape[0], dat, dlt, wo_v, dyb, atb, sem2)

    def chunk(b):
        return pltpu.make_async_copy(dqs.at[b], dq_o.at[b], dqsem.at[b])
    b = Bwd(nq, rows, head, qt, at, lse, dq_o, *scr[:20], dqsem, lambda b: chunk(b).start(), lambda i: None)
    b.prepare()
    b.run()
    dk[...] = dk[...] * SCALE
    last = [pltpu.make_async_copy(dk, dk_o, sem.at[0]), pltpu.make_async_copy(dv, dv_o, sem.at[1]), pltpu.make_async_copy(dbq, db_o, sem.at[2])]
    for c in last:
        c.start()
    for c in last:
        c.wait()

    @pl.loop(0, 2 * nq)
    def _(b):
        chunk(b).wait()


def k3(qt, at, lse, k, kt, v, cs, dy, wo):
    nblk, seq = qt.shape[0], k.shape[0]
    rows = seq // nblk
    sds, vm = jax.ShapeDtypeStruct, pltpu.VMEM
    return pl.pallas_call(
        functools.partial(k3_kernel, nblk // 2, rows),
        out_shape=[sds((nblk, HEAD_DIM, rows), BF16), sds((seq, HEAD_DIM), F32), sds((seq, HEAD_DIM), F32), sds((HEAD_DIM, rows), F32)],
        in_specs=[ANY] * 9, out_specs=[ANY] * 4,
        scratch_shapes=bwd_scratch(nblk // 2, rows) + [vm((HEAD_DIM, dy.shape[1]), BF16), vm((2, 512, dy.shape[1]), BF16), vm((2, HEAD_DIM, 512), BF16),
                                                       pltpu.SemaphoreType.DMA((5 + nblk,)), pltpu.SemaphoreType.DMA((5,))],
        compiler_params=pltpu.CompilerParams(vmem_limit_bytes=62 * 2 ** 20), name='attend_back')(qt, at, lse, k, kt, v, cs, dy, wo)


def norm_forward(hidden, norm_gain):
    hidden_f = hidden.astype(F32)
    inv_rms = lax.rsqrt(jnp.mean(hidden_f * hidden_f, axis=-1, keepdims=True) + NORM_EPS)
    unit = hidden_f * inv_rms
    return (unit * norm_gain.astype(F32)).astype(BF16), unit, inv_rms


def norm_backward(d_normed, unit, inv_rms, norm_gain):
    d_unit = d_normed * norm_gain.astype(F32)
    d_input = inv_rms * (d_unit - unit * jnp.mean(d_unit * unit, axis=-1, keepdims=True))
    return d_input, d_normed * unit


def mm(spec, a, b):
    return jnp.einsum(spec, a, b, preferred_element_type=F32)


def solution(mesh):
    n_sp = mesh.shape['sp']
    planes = [[z * 2 + c for z in range(n_sp // 2)] for c in range(2)]

    def step(hidden, d_out, positions, norm_gain, w_query, b_query, w_key, b_key, w_value, b_value, w_out):
        x, dy = hidden[0], d_out[0]
        rows, dm = x.shape
        seq = rows * n_sp
        heads = w_query.shape[1] // HEAD_DIM
        nz = n_sp // 2
        sp = lax.axis_index('sp')
        h, unit, inv_rms = norm_forward(x, norm_gain)
        pos8 = jnp.broadcast_to(positions, (8, rows))
        two = lambda b: b.astype(F32).reshape(2, -1)
        hf, ht, qt, k, kt, v, vt, cs = k1(n_sp, h, pos8, w_query, w_key, w_value, two(b_query), two(b_key), two(b_value))
        dyf, at, lse, ao = k2(n_sp, dy, qt, k, vt)
        dq, dk, dv, dbq = k3(qt, at, lse, k, kt, v, cs, dyf, w_out)

        am = lax.dynamic_slice_in_dim(at, sp * rows, rows, axis=1)
        c = sp % 2
        a_all = jnp.where(c == 0, jnp.concatenate([am, ao]), jnp.concatenate([ao, am]))
        y = (x.astype(F32) + mm('ep,ed->pd', a_all, w_out)).astype(BF16)
        dw_o = mm('es,sd->ed', at, dyf)
        dw_out = lax.psum(lax.dynamic_update_slice(jnp.zeros((dm, dm), F32), jnp.where(sp // 2 == 0, dw_o, 0.0), (c * dw_o.shape[0], 0)), 'sp')

        dq_all = lax.all_gather(dq, 'sp', axis=0)
        hb = hf.reshape(n_sp, rows, dm)
        dw_q = mm('bpd,vbep->vde', hb, dq_all)
        dw_q = dw_q.reshape(nz, 2, dm, HEAD_DIM).transpose(2, 1, 0, 3).reshape(dm, heads * HEAD_DIM)
        kv = lax.psum(jnp.concatenate([dk, dv], axis=1), 'sp', axis_index_groups=planes)
        kv = lax.all_gather(kv, 'sp', axis=0, axis_index_groups=[[2 * z, 2 * z + 1] for z in range(nz)])
        dkr, dvr = kv[:, :, :HEAD_DIM], kv[:, :, HEAD_DIM:]
        hd = HEAD_DIM // 2
        cos, sin = cs[:hd].T, cs[hd:].T
        a, b = dkr[..., :hd], dkr[..., hd:]
        dkp = jnp.concatenate([a * cos + b * sin, b * cos - a * sin], axis=-1)
        dk_bf, dv_bf = dkp.astype(BF16), dvr.astype(BF16)
        dw_k = mm('sd,gse->dge', hf, dk_bf).reshape(dm, -1)
        dw_v = mm('sd,gse->dge', hf, dv_bf).reshape(dm, -1)
        dqm = lax.dynamic_index_in_dim(dq_all, sp, axis=1, keepdims=False).reshape(nz, 2, HEAD_DIM, rows).transpose(1, 0, 2, 3).reshape(-1, rows)
        own = lambda t: lax.dynamic_slice_in_dim(t, sp * rows, rows, axis=1)
        d_normed = mm('ep,de->pd', dqm, w_query) + mm('gpe,dge->pd', own(dk_bf), w_key.reshape(dm, 2, -1)) + mm('gpe,dge->pd', own(dv_bf), w_value.reshape(dm, 2, -1))
        d_input, gain_terms = norm_backward(d_normed, unit, inv_rms, norm_gain)
        dx = (dy.astype(F32) + d_input).astype(BF16)
        db_q = lax.all_gather(jnp.sum(dbq, axis=1), 'sp', axis=0).reshape(nz, 2, HEAD_DIM).transpose(1, 0, 2).reshape(-1)
        d_gain = lax.psum(jnp.sum(gain_terms, axis=0), 'sp')
        return (y[None], dx[None], d_gain, dw_q, db_q, dw_k, jnp.sum(dkp, axis=1).reshape(-1), dw_v, jnp.sum(dvr, axis=1).reshape(-1), dw_out)

    seq_spec = P('dp', 'sp', None)
    in_specs = (seq_spec, seq_spec, P('dp', 'sp')) + (P(),) * 8
    out_specs = (seq_spec, seq_spec, P('dp'), P('dp', None), P('dp'), P('dp', None), P('dp'), P('dp', None), P('dp'), P('dp', None))
    return jax.shard_map(step, mesh=mesh, in_specs=in_specs, out_specs=out_specs, check_vma=False)
```

```python
import functools, math
import jax
import jax.numpy as jnp
from jax import lax
from jax.experimental import pallas as pl
from jax.experimental.pallas import tpu as pltpu
from jax.sharding import PartitionSpec as P

HEAD_DIM = 128
ROPE_BASE = 1000000.0
NORM_EPS = 1e-6
MESH = pl.DeviceIdType.MESH
PAIR = 2
TOP = slice(0, 1)
KEYS = 0
YES = True
MIB = 1 << 20
NSUB = PAIR
F32 = jnp.float32
BF16 = jnp.bfloat16
ANY = pl.BlockSpec(memory_space=pl.ANY)
VM = pl.BlockSpec(memory_space=pltpu.VMEM)


def span(i, n):
    return slice(i * n, (i + 1) * n)


def turns(n):
    return pl.loop(0, n)


class Ring:
    def __init__(self, full, own, rows, nz, sems):
        self.full, self.own, self.rows, self.nz = full, own, rows, nz
        self.send, self.recv, self.drecv = sems
        self.sp = lax.axis_index('sp')
        self.dp = lax.axis_index('dp')
        self.z, self.c = self.sp // PAIR, self.sp % PAIR
        self.sub = rows // (PAIR * NSUB)
        self.nsend = 7 * NSUB

    def dev(self, z, c):
        return (self.dp, z * PAIR + c)

    def where(self, d, j, z):
        s = j // (PAIR * NSUB)
        r = j % (PAIR * NSUB)
        half = (r // NSUB + d) % PAIR
        origin = (z + (self.nz - s if d == 0 else s)) % self.nz
        return pl.multiple_of((origin * PAIR + self.c) * self.rows + half * (self.rows // PAIR) + (r % NSUB) * self.sub, self.sub)

    def ici(self, d, j, src=None):
        off = self.where(d, j, self.z)
        to = (self.z + (1 if d == 0 else self.nz - 1)) % self.nz
        return pltpu.make_async_remote_copy(
            src_ref=self.full.at[pl.ds(off, self.sub)] if src is None else src,
            dst_ref=self.full.at[pl.ds(off, self.sub)],
            send_sem=self.send.at[d], recv_sem=self.recv.at[d, j],
            device_id=self.dev(to, self.c), device_id_type=MESH)

    def d2d(self, d, j):
        frm = (self.z + (self.nz - 1 if d == 0 else 1)) % self.nz
        off = self.where(d, j, frm)
        return pltpu.make_async_remote_copy(
            src_ref=self.full.at[pl.ds(off, self.sub)], dst_ref=self.full.at[pl.ds(off, self.sub)],
            send_sem=self.send.at[PAIR], recv_sem=self.drecv.at[j // (PAIR * NSUB)],
            device_id=self.dev(self.z, 1 - self.c), device_id_type=MESH)

    def d2d_own(self):
        off = pl.multiple_of(self.sp * self.rows, self.rows)
        return pltpu.make_async_remote_copy(
            src_ref=self.own, dst_ref=self.full.at[pl.ds(off, self.rows)],
            send_sem=self.send.at[3], recv_sem=self.drecv.at[4],
            device_id=self.dev(self.z, 1 - self.c), device_id_type=MESH)

    def start(self):
        @turns(PAIR * NSUB)
        def _(j):
            for d in range(PAIR):
                half = (j // NSUB + d) % PAIR
                off = pl.multiple_of(half * (self.rows // PAIR) + (j % NSUB) * self.sub, self.sub)
                self.ici(d, j, self.own.at[pl.ds(off, self.sub)]).start()
        self.d2d_own().start()

    def tick(self, j):
        for d in range(PAIR):
            self.ici(d, j).wait_recv()

            @pl.when(j + PAIR * NSUB < self.nsend)
            def _():
                self.ici(d, j + PAIR * NSUB).start()
            self.d2d(d, j).start()

    def total(self, rows, sem):
        ref = self.full.at[pl.ds(0, rows)]
        pltpu.make_async_copy(ref, ref, sem).wait()

    def finish_sends(self):
        each = self.nsend * self.sub
        self.total(each, self.send.at[0])
        self.total(each, self.send.at[1])
        self.total(PAIR * each, self.send.at[PAIR])
        self.d2d_own().wait_send()

    def wait_other(self, s):
        self.total(self.rows if s == 3 else PAIR * self.rows, self.drecv.at[s])


def ring_sems(nz):
    return [pltpu.SemaphoreType.DMA((4,)), pltpu.SemaphoreType.DMA((PAIR, 7 * NSUB)), pltpu.SemaphoreType.DMA((5,))]


def greet_all(n_sp):
    sp, dp = lax.axis_index('sp'), lax.axis_index('dp')
    bar = pltpu.get_barrier_semaphore()

    @pl.loop(1, n_sp)
    def _(o):
        pl.semaphore_signal(bar, inc=1, device_id=(dp, (sp + o) % n_sp), device_id_type=MESH)
    pl.semaphore_wait(bar, n_sp - 1)


def k1_kernel(n_sp, x_h, pos, par, wq, wk, wv, hf, ht, qt, k_o, kt_o, v_o, vt_o, cs_o,
              pos_all, wq_v, wk_v, wv_v, hb, htb, qs, ks, kts, vs, vts, css, send, recv, drecv, psend, precv, lsem, wsem, osem):
    nz = n_sp // PAIR
    rows, dm = x_h.shape
    qw = wq_v.shape[1]
    sp, dp = lax.axis_index('sp'), lax.axis_index('dp')
    z, c = sp // PAIR, sp % PAIR
    far = 1 - c
    heads = qw // HEAD_DIM
    half_dim = HEAD_DIM // PAIR
    ng = dm // HEAD_DIM
    mine = pl.ds(pl.multiple_of(sp * rows, rows), rows)
    ring = Ring(hf, hf.at[mine], rows, nz, (send, recv, drecv))
    x_in = pltpu.make_async_copy(x_h, hb, lsem.at[0])
    x_in.start()
    pos_copy = pltpu.make_async_copy(pos, pos_all.at[sp], lsem.at[1])
    pos_copy.start()

    def head_of(g):
        return (z + g) % heads

    wcopies = [pltpu.make_async_copy(wq.at[:, pl.ds(pl.multiple_of(c * qw + head_of(g) * HEAD_DIM, HEAD_DIM), HEAD_DIM)],
                                     wq_v.at[:, span(g, HEAD_DIM)], wsem.at[g]) for g in range(heads)]
    cols = pl.ds(pl.multiple_of(c * HEAD_DIM, HEAD_DIM), HEAD_DIM)
    wcopies += [pltpu.make_async_copy(wk.at[:, cols], wk_v, lsem.at[PAIR]), pltpu.make_async_copy(wv.at[:, cols], wv_v, lsem.at[3])]
    for w in wcopies:
        w.start()
    x_in.wait()
    gain = jnp.concatenate([par[g:g + 1, :] for g in range(ng)], axis=1)
    nr = 16

    @turns(rows // nr)
    def _(i):
        rr = pl.ds(pl.multiple_of(i * nr, nr), nr)
        xf = hb[rr, :].astype(F32)
        inv = lax.rsqrt(jnp.mean(xf * xf, axis=-1, keepdims=YES) + NORM_EPS)
        hb[rr, :] = (xf * inv * gain).astype(BF16)
    own_out = pltpu.make_async_copy(hb, hf.at[mine], lsem.at[0])
    own_out.start()
    greet_all(n_sp)

    def pos_send(o):
        return pltpu.make_async_remote_copy(src_ref=pos, dst_ref=pos_all.at[sp], send_sem=psend.at[0], recv_sem=precv.at[0],
                                            device_id=(dp, (sp + o) % n_sp), device_id_type=MESH)

    @pl.loop(1, n_sp)
    def _(o):
        pos_send(o).start()
    own_out.wait()
    ring.start()
    for w in wcopies:
        w.wait()
    pos_copy.wait()
    others = pos_all.at[pl.ds(0, n_sp - 1)]
    pltpu.make_async_copy(others, others, psend.at[0]).wait()
    pltpu.make_async_copy(others, others, precv.at[0]).wait()

    freq = jnp.exp(lax.broadcasted_iota(jnp.int32, (half_dim, 1), 0).astype(F32) * (-2.0 / HEAD_DIM * math.log(ROPE_BASE)))

    def outs(blk):
        cols = pl.ds(pl.multiple_of(blk * rows, rows), rows)
        return [pltpu.make_async_copy(htb, ht.at[:, cols], osem.at[0]),
                pltpu.make_async_copy(qs, qt.at[blk], osem.at[1]),
                pltpu.make_async_copy(ks, k_o.at[cols], osem.at[PAIR]),
                pltpu.make_async_copy(kts, kt_o.at[:, cols], osem.at[3]),
                pltpu.make_async_copy(vs, v_o.at[cols], osem.at[4]),
                pltpu.make_async_copy(vts, vt_o.at[:, cols], osem.at[5]),
                pltpu.make_async_copy(css, cs_o.at[:, cols], osem.at[6])]

    def compute(n, blk):
        load = pltpu.make_async_copy(hf.at[pl.ds(pl.multiple_of(blk * rows, rows), rows)], hb, lsem.at[0])
        load.start()
        load.wait()
        @pl.when(n > 0)
        def _():
            for o in outs(blk):
                o.wait()
        ang = freq * pos_all[blk].astype(F32)
        cos, sin = jnp.cos(ang), jnp.sin(ang)
        css[0:half_dim, :] = cos
        css[half_dim:, :] = sin
        h = hb[...]
        htb[...] = h.T

        def rope_t(t):
            a, b = t[:half_dim], t[half_dim:]
            return jnp.concatenate([a * cos - b * sin, b * cos + a * sin], axis=KEYS)
        for g in range(heads // PAIR):
            cols = slice(g * PAIR * HEAD_DIM, (g + 1) * PAIR * HEAD_DIM)
            bias = jnp.concatenate([par[pl.ds(ng + c * heads + head_of(g * PAIR + e), 1), :] for e in range(PAIR)], axis=1)
            q = jnp.dot(h, wq_v[:, cols], preferred_element_type=F32) + bias
            t = q.T
            for e in range(PAIR):
                hd = g * PAIR + e
                qs[:, span(hd, rows)] = rope_t(t[span(e, HEAD_DIM)]).astype(BF16)
        k = jnp.dot(h, wk_v[...], preferred_element_type=F32) + par[pl.ds(PAIR * ng + c, 1), :]
        kt = rope_t(k.T)
        kts[...] = kt.astype(BF16)
        ks[...] = kt.T.astype(BF16)
        v = jnp.dot(h, wv_v[...], preferred_element_type=F32) + par[pl.ds(PAIR * ng + PAIR + c, 1), :]
        vs[...] = v.astype(BF16)
        vts[...] = v.T.astype(BF16)
        for o in outs(blk):
            o.start()

    @turns(n_sp)
    def _(n):
        m = n - PAIR
        s = m // 4
        b = jnp.where(s == 3, (m % 4) * PAIR, m % 4)
        other = jnp.where(n < PAIR, n, b // PAIR)
        left = b % PAIR == 0
        dist = jnp.where(n < PAIR, 0, s + 1)

        @pl.when((n >= PAIR) & (m % 4 == 0))
        def _():
            @turns(jnp.where(s == 3, NSUB, PAIR * NSUB))
            def _(r):
                ring.tick(s * PAIR * NSUB + r)

        @pl.when(n == 1)
        def _():
            ring.d2d_own().wait_recv()

        for h in range(4):
            @pl.when((n >= PAIR) & (other == 1) & left & (s == h))
            def _():
                ring.wait_other(h)
        zb = (z + jnp.where(left, nz - dist, dist)) % nz
        cb = jnp.where(other == 1, 1 - c, c)
        compute(n, zb * PAIR + cb)
    for o in outs(0):
        o.wait()
    ring.finish_sends()


def k1(n_sp, x, pos, par, wq, wk, wv):
    rows, dm = x.shape
    seq = rows * n_sp
    nz = n_sp // PAIR
    qw = wq.shape[1] // PAIR
    heads = qw // HEAD_DIM
    sds = jax.ShapeDtypeStruct
    outs = [sds((seq, dm), BF16), sds((dm, seq), BF16), sds((n_sp, HEAD_DIM, heads * rows), BF16),
            sds((seq, HEAD_DIM), BF16), sds((HEAD_DIM, seq), BF16), sds((seq, HEAD_DIM), BF16), sds((HEAD_DIM, seq), BF16),
            sds((HEAD_DIM, seq), F32)]
    vm, dma = pltpu.VMEM, pltpu.SemaphoreType.DMA
    scratch = [vm((n_sp,) + pos.shape, jnp.int32), vm((dm, qw), BF16), vm((dm, HEAD_DIM), BF16), vm((dm, HEAD_DIM), BF16),
               vm((rows, dm), BF16), vm((dm, rows), BF16), vm((HEAD_DIM, heads * rows), BF16),
               vm((rows, HEAD_DIM), BF16), vm((HEAD_DIM, rows), BF16), vm((rows, HEAD_DIM), BF16), vm((HEAD_DIM, rows), BF16),
               vm((HEAD_DIM, rows), F32)] + ring_sems(nz) + [dma((1,)), dma((1,)), dma((4,)), dma((heads,)), dma((7,))]
    return pl.pallas_call(
        functools.partial(k1_kernel, n_sp), out_shape=outs,
        in_specs=[ANY, ANY, VM, ANY, ANY, ANY], out_specs=[ANY] * len(outs), scratch_shapes=scratch,
        compiler_params=pltpu.CompilerParams(collective_id=0, has_side_effects=YES, vmem_limit_bytes=60 * MIB),
        name='gather_project')(x, pos, par, wq, wk, wv)


LOG2E = math.log2(math.e)
NEG = -1e30

def split_scaled(q, scale):
    qs = q.astype(F32) * scale
    hi = qs.astype(BF16)
    lo = (qs - hi.astype(F32)).astype(BF16)
    return jnp.concatenate([hi, lo], axis=KEYS)

def decode(n, nblk):
    one = int if isinstance(n, int) else (lambda x: x.astype(jnp.int32))
    j = sum(one(n >= i * (i + 1)) for i in range(1, nblk // PAIR))
    r = n - j * (j + 1)
    odd = one(r > j)
    return PAIR * j + odd, r - odd * (j + 1)

def fwd_steps(nblk):
    return (nblk // PAIR) * (nblk // PAIR + 1)

def decode_up(n, nq):
    one = int if isinstance(n, int) else (lambda x: x.astype(jnp.int32))
    i = sum(one(n >= m * (m + 1) // PAIR) for m in range(1, nq))
    return i, n - i * (i + 1) // PAIR


def causal_bias(bias, bk, rows):
    d = lax.broadcasted_iota(jnp.int32, (bk, rows), 0) - lax.broadcasted_iota(jnp.int32, (bk, rows), 1)
    bias[0] = jnp.zeros((bk, rows), F32)
    bias[1] = jnp.where(d <= 0, 0.0, NEG)
    bias[PAIR] = jnp.where(d <= rows, 0.0, NEG)


class Fwd:
    def __init__(self, nblk, rows, heads, first, wide, qt, sink, lse, kk, vt, qb, q2, acc, mx, cm, ls, al, rt, lsv, sb, pb, bias, qsem, osem):
        self.__dict__.update(locals())
        self.bk = PAIR * rows
        self.groups = heads * wide
        self.cols = [span(u, rows) for u in range(self.groups)]
        self.halves = (range(0, self.groups // PAIR), range(self.groups // PAIR, self.groups))
        self.nq = nblk // wide
        self.nstep = fwd_steps(nblk) if wide == 1 else self.nq * (self.nq + 1) // PAIR

    def where(self, n):
        if self.wide == 1:
            i, t = decode(n, self.nblk)
            return i, t, t == i // PAIR
        i, t = decode_up(n, self.nq)
        return i, t, t == i

    def load_q(self, i):
        w = self.heads * self.rows
        src = slice(self.first * self.rows, self.first * self.rows + w)
        return [pltpu.make_async_copy(self.qt.at[self.wide * i + e, :, src], self.qb.at[:, span(e, w)], self.qsem.at[e]) for e in range(self.wide)]

    def make_q2(self, i):
        for u in range(self.groups):
            self.q2[i % PAIR, :, self.cols[u]] = split_scaled(self.qb[:, self.cols[u]], LOG2E * HEAD_DIM ** -0.5)

    def prepare(self):
        causal_bias(self.bias, self.bk, self.rows)
        for i in range(PAIR):
            for cp in self.load_q(i):
                cp.start()
            for cp in self.load_q(i):
                cp.wait()
            self.make_q2(i)
        for cp in self.load_q(PAIR):
            cp.start()
        self.acc[...] = jnp.zeros_like(self.acc)
        self.pb[...] = jnp.zeros_like(self.pb)
        self.ls[...] = jnp.zeros_like(self.ls)
        self.al[...] = jnp.zeros_like(self.al)
        self.mx[...] = jnp.zeros_like(self.mx)
        self.scores(0, 0)

    def keys(self, t):
        return pl.ds(pl.multiple_of(t * self.bk, self.bk), self.bk)

    def scores(self, n, part):
        i, t, last = self.where(n)
        kb = self.kk[self.keys(t), :]
        for u in self.halves[part]:
            kind = jnp.where(last, 1 + (i % PAIR if self.wide == 1 else u // self.heads), 0)
            s = jnp.dot(kb, self.q2[i % PAIR, :, self.cols[u]], preferred_element_type=F32) + self.bias[kind]
            self.sb[u] = s
            self.cm[:, self.cols[u]] = jnp.max(s.reshape(self.bk // 8, 8, self.rows), axis=KEYS)

    def soft(self, n, part):
        i, t, last = self.where(n)
        for u in self.halves[part]:
            c = self.cols[u]
            m0 = jnp.where(t == 0, NEG, self.mx[TOP, c])
            m1 = jnp.maximum(m0, jnp.max(self.cm[:, c], axis=KEYS, keepdims=YES))
            p = jnp.exp2(self.sb[u] - m1)
            a = jnp.exp2(m0 - m1)
            self.mx[TOP, c] = m1
            self.al[TOP, c] = a
            self.ls[:, c] = self.ls[:, c] * a + jnp.sum(p.reshape(self.bk // 8, 8, self.rows), axis=KEYS)
            self.pb[u] = p.astype(BF16)

    def values(self, n, part):
        i, t, last = self.where(n)
        vb = self.vt[:, self.keys(t)]
        for u in self.halves[part]:
            c = self.cols[u]
            self.acc[:, c] = self.acc[:, c] * self.al[TOP, c] + jnp.dot(vb, self.pb[u], preferred_element_type=F32)

    def out_lse(self, i):
        return pltpu.make_async_copy(self.lsv, self.lse.at[i], self.osem)

    def finish(self, i, part):
        self.sink.before(i, part)
        for u in self.halves[part]:
            c = self.cols[u]
            self.sink.store(u % self.heads, self.wide * i + u // self.heads, (self.acc[:, c] * self.rt[TOP, c]).astype(BF16))
        self.sink.after(i, part)

    def end_block(self, i):
        tot = jnp.sum(self.ls[...], axis=KEYS, keepdims=YES)
        self.rt[TOP, :] = 1.0 / tot
        if self.lse is not None:
            @pl.when(i > 0)
            def _():
                self.out_lse(i).wait()
            self.lsv[TOP, :] = self.mx[TOP, :] + jnp.log2(tot)
            self.out_lse(i).start()
        self.finish(i, 0)

        @pl.when(i + PAIR < self.nq)
        def _():
            for cp in self.load_q(i + PAIR):
                cp.wait()
            self.make_q2(i + PAIR)

        @pl.when(i + 3 < self.nq)
        def _():
            for cp in self.load_q(i + 3):
                cp.start()

    def step(self, n):
        n1 = jnp.minimum(n + 1, self.nstep - 1)
        self.scores(n, 1)
        self.soft(n, 0)
        self.values(jnp.maximum(n - 1, 0), 1)
        self.scores(n1, 0)
        self.soft(n, 1)
        self.values(n, 0)

    def run(self, on_step):
        @turns(self.nstep)
        def _(n):
            on_step(n)
            self.step(n)
            i, t, last = self.where(n)

            @pl.when((t == 0) & (n > 0))
            def _():
                self.finish(i - 1, 1)

            @pl.when(last)
            def _():
                self.end_block(i)

    def drain(self):
        self.values(self.nstep - 1, 1)
        self.finish(self.nq - 1, 1)
        if self.lse is not None:
            self.out_lse(self.nq - 1).wait()


def fwd_scratch(nblk, rows, groups, wide):
    vm = pltpu.VMEM
    w, bk = groups * rows, PAIR * rows
    return [vm((HEAD_DIM, w), BF16), vm((PAIR, PAIR * HEAD_DIM, w), BF16), vm((HEAD_DIM, w), F32)] + [vm((8, w), F32)] * 6 + [
            vm((groups, bk, rows), F32), vm((groups, bk, rows), BF16), vm((3, bk, rows), F32),
            pltpu.SemaphoreType.DMA((wide,)), pltpu.SemaphoreType.DMA]


NT = (((1,), (1,)), ((), ()))
SCALE = HEAD_DIM ** -0.5

def dot_nt(a, b):
    return lax.dot_general(a, b, NT, preferred_element_type=F32)

def bwd_steps(nq):
    return nq * (nq + 1) // PAIR

class Bwd:
    def __init__(self, nq, rows, qt, kk, kt, vv, dat, dlt, lsv, qb, q2, cs, dk, dv, dq, dbq, sb, dpb, pb, dsb, bias, dqs, psem):
        self.__dict__.update(locals())
        self.bk = PAIR * rows
        self.nstep = bwd_steps(nq)
        self.cols = [slice(0, rows), slice(rows, PAIR * rows)]

    def loads(self, i):
        slot = i % PAIR
        return [pltpu.make_async_copy(self.qt.at[PAIR * i + e, :, 0:self.rows], self.qb.at[slot, :, self.cols[e]], self.psem.at[slot, e]) for e in range(PAIR)]

    def make_q2(self, i):
        for e in range(PAIR):
            self.q2[i % PAIR, :, self.cols[e]] = split_scaled(self.qb[i % PAIR, :, self.cols[e]], LOG2E * SCALE)

    def prepare(self):
        nq = self.nq
        for i in (0, 1):
            for cp in self.loads(i):
                cp.start()
            for cp in self.loads(i):
                cp.wait()
            self.make_q2(i)
        causal_bias(self.bias, self.bk, self.rows)
        self.dk[...] = jnp.zeros_like(self.dk)
        self.dv[...] = jnp.zeros_like(self.dv)
        self.dq[...] = jnp.zeros_like(self.dq)
        self.dbq[...] = jnp.zeros_like(self.dbq)
        self.pb[...] = jnp.zeros_like(self.pb)
        self.dsb[...] = jnp.zeros_like(self.dsb)
        self.scores(0, 0)

    def keys(self, t):
        return pl.ds(pl.multiple_of(t * self.bk, self.bk), self.bk)

    def qcols(self, i, e):
        return pl.ds(pl.multiple_of(i * self.bk + e * self.rows, self.rows), self.rows)

    def scores(self, n, e):
        i, t = decode_up(n, self.nq)
        kind = jnp.where(t == i, 1 + e, 0)
        s = jnp.dot(self.kk[self.keys(t), :], self.q2[i % PAIR, :, self.cols[e]], preferred_element_type=F32)
        self.sb[e] = s + self.bias[kind]
        self.dpb[e] = jnp.dot(self.vv[self.keys(t), :], self.dat[:, self.qcols(i, e)], preferred_element_type=F32)

    def soft(self, n, e):
        i, t = decode_up(n, self.nq)
        c = self.qcols(i, e)
        p = jnp.exp2(self.sb[e] - self.lsv[TOP, c])
        self.pb[e] = p.astype(BF16)
        self.dsb[e] = (p * (self.dpb[e] - self.dlt[TOP, c])).astype(BF16)

    def grads(self, n, e):
        i, t = decode_up(n, self.nq)
        r = self.keys(t)
        self.dv[r, :] += dot_nt(self.pb[e], self.dat[:, self.qcols(i, e)])
        self.dk[r, :] += dot_nt(self.dsb[e], self.qb[i % PAIR, :, self.cols[e]])
        keep = jnp.where(t == 0, 0.0, 1.0)
        self.dq[:, self.cols[e]] = self.dq[:, self.cols[e]] * keep + jnp.dot(self.kt[:, self.keys(t)], self.dsb[e], preferred_element_type=F32)

    def step(self, n):
        n1 = jnp.minimum(n + 1, self.nstep - 1)
        self.scores(n, 1)
        self.soft(n, 0)
        self.grads(jnp.maximum(n - 1, 0), 1)
        self.scores(n1, 0)
        self.soft(n, 1)
        self.grads(n, 0)

    def finish(self, i, e):
        c = self.qcols(i, e)
        g = self.dq[:, self.cols[e]] * SCALE
        hd = HEAD_DIM // PAIR
        cos, sin = self.cs[0:hd, c], self.cs[hd:, c]
        a, b = g[:hd], g[hd:]
        a, b = a * cos + b * sin, b * cos - a * sin
        self.dbq[0:hd, :] += a
        self.dbq[hd:, :] += b
        blk = PAIR * i + e
        self.dqs[blk, 0:hd, :] = a.astype(BF16)
        self.dqs[blk, hd:, :] = b.astype(BF16)

    def run(self, on_step=lambda n: None):
        @turns(self.nstep)
        def _(n):
            on_step(n)
            self.step(n)
            i, t = decode_up(n, self.nq)

            @pl.when((t == 0) & (n > 0))
            def _():
                self.finish(i - 1, 1)

                @pl.when(i + 1 < self.nq)
                def _():
                    for cp in self.loads(i + 1):
                        cp.start()
                    for cp in self.loads(i + 1):
                        cp.wait()
                    self.make_q2(i + 1)

            @pl.when(t == i)
            def _():
                self.finish(i, 0)
        self.grads(self.nstep - 1, 1)
        self.finish(self.nq - 1, 1)


def bwd_scratch(nq, rows):
    vm = pltpu.VMEM
    bk, seq = PAIR * rows, PAIR * rows * nq
    return [vm((seq, PAIR * HEAD_DIM), BF16), vm((HEAD_DIM, seq), BF16), vm((seq, HEAD_DIM), BF16), vm((HEAD_DIM, seq), BF16), vm((8, seq), F32), vm((8, seq), F32),
            vm((PAIR, HEAD_DIM, bk), BF16), vm((PAIR, PAIR * HEAD_DIM, bk), BF16), vm((HEAD_DIM, seq), F32), vm((seq, HEAD_DIM), F32), vm((seq, HEAD_DIM), F32),
            vm((HEAD_DIM, bk), F32), vm((HEAD_DIM, rows), F32), vm((PAIR, bk, rows), F32), vm((PAIR, bk, rows), F32), vm((PAIR, bk, rows), BF16), vm((PAIR, bk, rows), BF16),
            vm((3, bk, rows), F32), vm((PAIR * nq, HEAD_DIM, rows), BF16), pltpu.SemaphoreType.DMA((PAIR, PAIR)), pltpu.SemaphoreType.DMA((PAIR * nq,))]


def load_bwd(k_h, kt_h, v_h, cs_h, lse_h, rows, nblk, kk, kt, vv, cs, lsv, sem):
    cps = [pltpu.make_async_copy(k_h, kk.at[:, 0:HEAD_DIM], sem.at[0]), pltpu.make_async_copy(k_h, kk.at[:, HEAD_DIM:], sem.at[1]),
           pltpu.make_async_copy(kt_h, kt, sem.at[PAIR]), pltpu.make_async_copy(v_h, vv, sem.at[3]), pltpu.make_async_copy(cs_h, cs, sem.at[4])]
    for c in cps:
        c.start()

    cps += [pltpu.make_async_copy(lse_h.at[b, :, 0:rows], lsv.at[:, span(b, rows)], sem.at[5 + b]) for b in range(nblk)]
    for c in cps[5:]:
        c.start()
    return cps


class GradAtt:
    def __init__(self, dy_h, at_h, nb, dat, dlt, wo_v, dyb, atb, sem):
        self.__dict__.update(locals())
        self.blk = dyb.shape[1]

    def copies(self, b):
        s = b % PAIR
        r = pl.ds(pl.multiple_of(b * self.blk, self.blk), self.blk)
        return [pltpu.make_async_copy(self.dy_h.at[r], self.dyb.at[s], self.sem.at[s]),
                pltpu.make_async_copy(self.at_h.at[0:HEAD_DIM, r], self.atb.at[s], self.sem.at[PAIR + s])]

    def start(self, b):
        for c in self.copies(b):
            c.start()

    def block(self, b):
        for c in self.copies(b):
            c.wait()
        d = dot_nt(self.dyb[b % PAIR], self.wo_v[...]).T.astype(BF16)
        r = pl.ds(pl.multiple_of(b * self.blk, self.blk), self.blk)
        self.dat[:, r] = d
        self.dlt[TOP, r] = jnp.sum(d.astype(F32) * self.atb[b % PAIR].astype(F32), axis=KEYS, keepdims=YES)


class Rows:
    def __init__(self, at, ats, rows, sem):
        self.at, self.ats, self.rows, self.sem = at, ats, rows, sem

    def copy(self, i, part):
        n = self.ats.shape[0] // PAIR
        r = span(part, n)
        return pltpu.make_async_copy(self.ats.at[r], self.at.at[r, pl.ds(pl.multiple_of(i * self.rows, self.rows), self.rows)], self.sem.at[part])

    def before(self, i, part):
        @pl.when(i > 0)
        def _():
            self.copy(i, part).wait()

    def store(self, g, blk, value):
        self.ats[span(g, HEAD_DIM), :] = value

    def after(self, i, part):
        self.copy(i, part).start()


def k2_kernel(n_sp, own_dy, qt, k_h, vt_h, dyf, at, lse, ao, kk, vt, ats, *scr):
    *scr, asem, send, recv, drecv, lsem, xsem = scr
    rows = own_dy.shape[0]
    heads = at.shape[0] // HEAD_DIM
    nz = n_sp // PAIR
    sp, dp = lax.axis_index('sp'), lax.axis_index('dp')
    ring = Ring(dyf, own_dy, rows, nz, (send, recv, drecv))
    loads = [pltpu.make_async_copy(k_h, kk.at[:, 0:HEAD_DIM], lsem.at[0]), pltpu.make_async_copy(k_h, kk.at[:, HEAD_DIM:], lsem.at[1]),
             pltpu.make_async_copy(vt_h, vt, lsem.at[PAIR])]
    for c in loads:
        c.start()
    greet_all(n_sp)
    ring.start()
    mine = pltpu.make_async_copy(own_dy, dyf.at[pl.ds(pl.multiple_of(sp * rows, rows), rows)], lsem.at[3])
    mine.start()
    for c in loads:
        c.wait()
    sink = Rows(at, ats, rows, asem)
    f = Fwd(n_sp, rows, heads, 0, 1, qt, sink, lse, kk, vt, *scr)
    f.prepare()

    def due(n):
        return jnp.clip((n - 3) // 5, 0, ring.nsend)

    def on_step(n):
        @pl.loop(due(n), due(n + 1))
        def _(j):
            ring.tick(j)
    f.run(on_step)
    f.drain()
    for part in range(PAIR):
        sink.copy(0, part).wait()
    other = (sp // PAIR) * PAIR + 1 - sp % PAIR
    give = pltpu.make_async_remote_copy(
        src_ref=at.at[:, pl.ds(pl.multiple_of(other * rows, rows), rows)], dst_ref=ao, send_sem=xsem.at[0], recv_sem=xsem.at[1],
        device_id=(dp, other), device_id_type=MESH)
    give.start()

    @pl.loop(due(f.nstep), ring.nsend)
    def _(j):
        ring.tick(j)

    for s in range(4):
        ring.wait_other(s)
    ring.d2d_own().wait_recv()
    give.wait()
    mine.wait()
    ring.finish_sends()


def k2(n_sp, own_dy, qt, k, vt):
    rows, dm = own_dy.shape
    seq = rows * n_sp
    heads = qt.shape[PAIR] // rows * 3 // 4
    sds, vm, dma = jax.ShapeDtypeStruct, pltpu.VMEM, pltpu.SemaphoreType.DMA
    outs = [sds((seq, dm), BF16), sds((heads * HEAD_DIM, seq), BF16), sds((n_sp, 8, heads * rows), F32), sds((heads * HEAD_DIM, rows), BF16)]
    return pl.pallas_call(
        functools.partial(k2_kernel, n_sp), out_shape=outs, in_specs=[ANY] * 4, out_specs=[ANY] * 4,
        scratch_shapes=[vm((seq, PAIR * HEAD_DIM), BF16), vm((HEAD_DIM, seq), BF16), vm((heads * HEAD_DIM, rows), BF16)] + fwd_scratch(n_sp, rows, heads, 1)
        + [dma((PAIR,))] + ring_sems(n_sp // PAIR) + [dma((4,)), dma((PAIR,))],
        compiler_params=pltpu.CompilerParams(collective_id=1, has_side_effects=YES, vmem_limit_bytes=62 * MIB),
        name='gather_attend')(own_dy, qt, k, vt)


TICK0 = (5, 6, 7, 9, 13, 15, 18, 19, 21, 24, 31, 32, 34, 35)
TICK1 = (10, 20, 25, 26, 27, 33)


class Relay:
    def __init__(self, blk, nr, nz, send, recv):
        self.blk, self.nr, self.nz, self.send, self.recv = blk, nr, nz, send, recv
        sp = lax.axis_index('sp')
        self.dp, self.z, self.c = lax.axis_index('dp'), sp // PAIR, sp % PAIR

    def copy(self, d, s, r):
        origin = (self.z + (self.nz - s if d == 0 else s)) % self.nz
        to = (self.z + (1 if d == 0 else self.nz - 1)) % self.nz
        ref = self.blk(origin, r)
        i = s * self.nr + r
        return pltpu.make_async_remote_copy(src_ref=ref, dst_ref=ref, send_sem=self.send.at[d], recv_sem=self.recv.at[d, i],
                                            device_id=(self.dp, to * PAIR + self.c), device_id_type=MESH)

    def own(self, r):
        for d in range(PAIR):
            self.copy(d, 0, r).start()

    def tick(self, s, r):
        for d in range(PAIR):
            if s == 3:
                @pl.when(r % PAIR == d)
                def _():
                    self.copy(d, 3, r).wait_recv()
            else:
                self.copy(d, s, r).wait_recv()
                if s == PAIR:
                    @pl.when(r % PAIR == d)
                    def _():
                        self.copy(d, 3, r).start()
                else:
                    self.copy(d, s + 1, r).start()

    def ticks(self, s, lo, hi):
        @pl.loop(lo, hi)
        def _(r):
            self.tick(s, r)

    def finish(self, ref):
        for d in range(PAIR):
            pltpu.make_async_copy(ref, ref, self.send.at[d]).wait()


def k3_kernel(nq, rows, dims, x_h, dyo_h, par, qt, at, ao, lse, k_h, kt_h, v_h, vt_h, cs_h, ht_h, dy_h, wq_h, wk_h, wv_h, wo_h,
              y_o, dx_o, dwq_o, dwk_o, dwv_o, dwo_o, small_o,
              kk, vt, ao2, cs, dk, dv, dqa, dqo, rs, kva, kvo, sma, smo, qsend, qrecv, rsend, rrecv, ksend, krecv, xsend, xrecv, ssend, srecv, tsend, trecv, tl, lq):
    nz, n_sp, heads = dims
    nblk = PAIR * nq
    hd = HEAD_DIM // PAIR
    qw = heads * HEAD_DIM
    bk = PAIR * rows
    dm = x_h.shape[1]
    cw = PAIR * HEAD_DIM
    vm = pltpu.VMEM
    dma = pltpu.SemaphoreType.DMA
    sp, dp = lax.axis_index('sp'), lax.axis_index('dp')
    z, c = sp // PAIR, sp % PAIR
    far = 1 - c
    other = z * PAIR + 1 - c
    peer = dict(device_id=(dp, other), device_id_type=MESH)

    relay = Relay(lambda o, r: dqa.at[o, r], nblk, nz, qsend, qrecv)
    kvr = Relay(lambda o, r: kva.at[o, pl.ds(pl.multiple_of(r * HEAD_DIM, HEAD_DIM), HEAD_DIM)], PAIR, nz, ksend, krecv)
    greet_all(n_sp)
    sma[sp] = jnp.zeros(sma.shape[1:], F32)

    nstep = bwd_steps(nq)
    own_at = [(r // PAIR + 1) * (r // PAIR + PAIR) // PAIR + r % PAIR + PAIR for r in range(nblk)]

    def count(n, at_step):
        return sum((n >= a).astype(jnp.int32) for a in at_step)

    def back(*scr):
        *scr, wo_v, dyb, atb, sem, sem2 = scr
        kt, vv, dat, dlt, lsv, qb, q2, dq, dbq, sb, dpb, pb, dsb, bias, psem = scr
        row0 = pl.multiple_of(c * qw + z * HEAD_DIM, HEAD_DIM)
        w_in = pltpu.make_async_copy(wo_h.at[pl.ds(row0, HEAD_DIM)], wo_v, sem2.at[4])
        w_in.start()
        vt_in = pltpu.make_async_copy(vt_h, vt, lq.at[0])
        vt_in.start()
        ga = GradAtt(dy_h, at, nq, dat, dlt, wo_v, dyb, atb, sem2)
        ga.start(0)
        kin = load_bwd(k_h, kt_h, v_h, cs_h, lse, rows, nblk, kk, kt, vv, cs, lsv, sem)
        ga.start(1)
        w_in.wait()
        ga.block(0)
        for cp in kin:
            cp.wait()
        vt_in.wait()
        b = Bwd(nq, rows, qt, kk, kt, vv, dat, dlt, lsv, qb, q2, cs, dk, dv, dq, dbq, sb, dpb, pb, dsb, bias, dqa.at[z], psem)
        b.prepare()
        t0 = [min(t, nstep) + 1 for t in TICK0]
        t1 = [min(t, nstep) + 1 for t in TICK1]

        def on_step(n):
            @pl.loop(count(n, own_at), count(n + 1, own_at))
            def _(r):
                relay.own(r)
            relay.ticks(0, count(n, t0), count(n + 1, t0))
            relay.ticks(1, count(n, t1), count(n + 1, t1))
            i, t = decode_up(n, nq)

            @pl.when((t == 0) & (i + 1 < nq))
            def _():
                @pl.when(i + PAIR < nq)
                def _():
                    ga.start(i + PAIR)
                ga.block(i + 1)
        b.run(on_step)
        own_in = sum(1 for a in own_at if a <= nstep)

        @pl.loop(own_in, nblk)
        def _(r):
            relay.own(r)
        sma[sp, 16:17, :] = jnp.sum(dbq[...].T, axis=KEYS, keepdims=YES)
    scr = bwd_scratch(nq, rows)
    keep = scr[1:8] + scr[11:18] + [scr[19]]
    pl.run_scoped(back, *keep, vm((HEAD_DIM, dm), BF16), vm((PAIR, bk, dm), BF16), vm((PAIR, HEAD_DIM, bk), BF16), dma((5 + nblk,)), dma((5,)))
    h0, h1 = sum(1 for t in TICK0 if t + 1 <= nstep), sum(1 for t in TICK1 if t + 1 <= nstep)

    def rs_block(d, s):
        b = (z + (PAIR * nz - 1 - s if d == 0 else 1 + s)) % nz
        return (dk if d == 0 else dv).at[pl.ds(pl.multiple_of(b * bk, bk), bk)]

    def rs_copy(d, s):
        to = (z + (1 if d == 0 else nz - 1)) % nz
        return pltpu.make_async_remote_copy(src_ref=rs_block(d, 0) if s == 0 else rs.at[d, s - 1], dst_ref=rs.at[d, s],
                                            send_sem=rsend.at[d], recv_sem=rrecv.at[d, s], device_id=(dp, to * PAIR + c), device_id_type=MESH)
    for d in range(PAIR):
        rs_copy(d, 0).start()

    def rs_step(s):
        for d in range(PAIR):
            rs_copy(d, s - 1).wait_recv()
            rs[d, s - 1] = rs[d, s - 1] + rs_block(d, s)[...]
        for d in range(PAIR):
            rs_copy(d, s).start()

    kv_give = pltpu.make_async_remote_copy(src_ref=kva.at[z, :, pl.ds(pl.multiple_of(far * rows, rows), rows)], dst_ref=kvo,
                                           send_sem=xsend.at[0], recv_sem=xrecv.at[0], **peer)

    def keys_whole():
        for d in range(PAIR):
            rs_copy(d, nz - PAIR).wait_recv()
        own = pl.ds(pl.multiple_of(z * bk, bk), bk)
        g = ((rs[0, nz - PAIR] + dk[own, :]) * SCALE).T
        a, b = g[:hd], g[hd:]
        cos, sin = cs[0:hd, own], cs[hd:, own]
        g = jnp.concatenate([a * cos + b * sin, b * cos - a * sin], axis=KEYS)
        sma[sp, 17:18, :] = jnp.sum(g.T, axis=KEYS, keepdims=YES)
        kva[z, 0:HEAD_DIM, :] = g.astype(BF16)
        g = rs[1, nz - PAIR] + dv[own, :]
        sma[sp, 18:19, :] = jnp.sum(g, axis=KEYS, keepdims=YES)
        kva[z, HEAD_DIM:, :] = g.T.astype(BF16)
        for r in range(PAIR):
            kvr.own(r)
        kv_give.start()

    def late(tile, aT, hta, sem):
        nslot = tile.shape[0]
        ht_in = [pltpu.make_async_copy(ht_h.at[0:qw], hta, lq.at[1])]

        def put(dst, piece, e):
            slot = piece % nslot
            src = tile.at[slot, :, span(e, HEAD_DIM)]
            return (pltpu.make_async_copy(src, dst, tl.at[slot, e]),
                    pltpu.make_async_remote_copy(src_ref=src, dst_ref=dst, send_sem=tsend.at[slot, e], recv_sem=trecv.at[piece // (dm // cw + 4 * (dm // qw))], **peer))

        def give(dsts, piece):
            for e in range(PAIR):
                for cp in put(dsts[e], piece, e):
                    cp.start()

        def free(piece):
            for e in range(PAIR):
                a, b = put(dwk_o.at[0:qw, 0:HEAD_DIM], piece, e)
                a.wait()
                b.wait_send()

        def att_part(atv, aob, xo, hsem):
            have = at.shape[0] // HEAD_DIM

            def head_rows(g):
                return pl.ds(pl.multiple_of((z + g) % heads * HEAD_DIM, HEAD_DIM), HEAD_DIM)

            def spread(src, dst, base):
                return [pltpu.make_async_copy(src.at[span(g, HEAD_DIM)], dst.at[head_rows(g)], hsem.at[base + g]) for g in range(have)]
            ins = spread(at, atv, 0) + spread(ao, aob, heads) + [pltpu.make_async_copy(x_h, xo, lq.at[3])]
            for cp in ins:
                cp.start()
            turn_rs, turn0, turn1 = [7, 14, 21, 28, 35], [PAIR, PAIR], [4, 10, 17, 24, 31]

            class Here:
                def before(self, i, part):
                    pass

                def store(self, g, blk, value):
                    atv[head_rows(have + g), pl.ds(pl.multiple_of(blk * rows, rows), rows)] = value

                def after(self, i, part):
                    pass

            def rest(*fscr):
                f = Fwd(nblk, rows, heads - have, have, PAIR, qt, Here(), None, kk, vt, *fscr)
                f.prepare()

                def on_step(n):
                    relay.ticks(0, h0 + count(n, turn0), h0 + count(n + 1, turn0))
                    relay.ticks(1, h1 + count(n, turn1), h1 + count(n + 1, turn1))
                    for s in range(1, 6):
                        @pl.when(n + 1 == turn_rs[s - 1])
                        def _():
                            rs_step(s)
                f.run(on_step)
                f.drain()
            pl.run_scoped(rest, *fwd_scratch(nblk, rows, PAIR * (heads - have), PAIR))
            gives = [pltpu.make_async_remote_copy(src_ref=atv.at[head_rows(have + g), pl.ds(pl.multiple_of(other * rows, rows), rows)],
                                                  dst_ref=ao2.at[span(g, HEAD_DIM)], send_sem=xsend.at[PAIR + g], recv_sem=xrecv.at[PAIR + g], **peer)
                     for g in range(heads - have)]
            ht_in[0].start()
            for cp in ins:
                cp.wait()

            def products(dyt, wt):
                nw = wt.shape[0]

                def dy_tile(n):
                    return pltpu.make_async_copy(dy_h.at[:, pl.ds(pl.multiple_of(n * cw, cw), cw)], dyt.at[n % PAIR], sem.at[n % PAIR])

                def w_tile(n):
                    return pltpu.make_async_copy(wo_h.at[:, pl.ds(pl.multiple_of(n * cw, cw), cw)], wt.at[n % nw], sem.at[PAIR + n % nw])
                dy_tile(0).start()
                for i in range(nw - 1):
                    w_tile(i).start()
                for cp in gives:
                    cp.start()
                ntile = dm // cw
                w1 = [PAIR, 5, 6, 8, 8]
                k1 = h1 + len(turn1)

                @turns(ntile)
                def _(n):
                    @pl.when(n + 1 < ntile)
                    def _():
                        dy_tile(n + 1).start()
                    relay.ticks(1, k1 + count(n, w1), k1 + count(n + 1, w1))

                    @pl.when(n == 3)
                    def _():
                        rs_step(6)

                    @pl.when(n == 6)
                    def _():
                        keys_whole()
                    dy_tile(n).wait()

                    @pl.when(n >= nslot)
                    def _():
                        free(n - nslot)
                    tile[n % nslot] = jnp.dot(atv[...], dyt[n % PAIR], preferred_element_type=F32)
                    rws = pl.ds(pl.multiple_of(c * qw, qw), qw)
                    give([dwo_o.at[rws, pl.ds(pl.multiple_of(n * cw + e * HEAD_DIM, HEAD_DIM), HEAD_DIM)] for e in range(PAIR)], n)
                relay.ticks(PAIR, 0, nblk // PAIR)

                for cp in gives:
                    cp.wait()
                for g in range(heads - have):
                    aob[head_rows(have + g), :] = ao2[span(g, HEAD_DIM), :]
                aT[:, pl.ds(pl.multiple_of(c * qw, qw), qw)] = atv[:, pl.ds(pl.multiple_of(sp * rows, rows), rows)].T
                aT[:, pl.ds(pl.multiple_of(far * qw, qw), qw)] = aob[...].T

                @turns(ntile)
                def _(n):
                    @pl.when(n + nw - 1 < ntile)
                    def _():
                        w_tile(n + nw - 1).start()
                    w_tile(n).wait()
                    cl = pl.ds(pl.multiple_of(n * cw, cw), cw)
                    xo[:, cl] = (xo[:, cl].astype(F32) + jnp.dot(aT[...], wt[n % nw], preferred_element_type=F32)).astype(BF16)
                out = pltpu.make_async_copy(xo, y_o, lq.at[PAIR])
                out.start()
                out.wait()
            pl.run_scoped(products, vm((PAIR, dy_h.shape[0], cw), BF16), vm((3, dm, cw), BF16))
        pl.run_scoped(att_part, vm((qw, dy_h.shape[0]), BF16), vm((qw, rows), BF16), vm((rows, dm), BF16), dma((PAIR * heads,)))
        pl.run_scoped(functools.partial(later, tile, aT, hta, ht_in[0], sem, nslot, give, free), vm((dm - qw, nblk * rows), BF16))

    def later(tile, aT, hta, hta_in, sem, nslot, give, free, htb):
        htb_in = pltpu.make_async_copy(ht_h.at[qw:], htb, lq.at[0])
        htb_in.start()
        nm = dm // qw
        once = jnp.minimum(z + 1, 1)

        def product(rhs_of, cols_of, nr, m, piece):
            free(piece - nslot)

            @turns(once)
            def _(_):
                acc = None
                for r in range(nr):
                    part = dot_nt((hta, htb)[m][:, cols_of(r)], rhs_of(r))
                    acc = part if acc is None else acc + part
                tile[piece % nslot] = acc

        def pair(p, piece, between):
            ha = (z + nz - p) % nz
            hb = jnp.where(p < nz // PAIR, (z + p) % nz, z)
            for m in range(nm):
                product(lambda r: jnp.concatenate([dqa[ha, r], dqa[hb, r]], axis=KEYS), lambda r: span(r, rows), nblk, m, piece + m)
                give([dwq_o.at[span(m, qw), pl.ds(pl.multiple_of(c * qw + h * HEAD_DIM, HEAD_DIM), HEAD_DIM)] for h in (ha, hb)], piece + m)
                if m == 0:
                    between()
        hta_in.wait()
        base = dm // cw
        def in_rows(wr, xo, dyo, wkv, dkp, dn):
            ins = [pltpu.make_async_copy(x_h, xo, lq.at[PAIR]), pltpu.make_async_copy(dyo_h, dyo, lq.at[3]),
                   pltpu.make_async_copy(wk_h, wkv.at[0], lq.at[5]), pltpu.make_async_copy(wv_h, wkv.at[1], lq.at[6])]
            for cp in ins:
                cp.start()

            nw = wr.shape[0]

            def w_tile(n):
                return pltpu.make_async_copy(wq_h.at[pl.ds(pl.multiple_of(n * cw, cw), cw)], wr.at[n % nw], sem.at[n % nw])
            for i in range(nw - 1):
                w_tile(i).start()
            dq_give = pltpu.make_async_remote_copy(src_ref=dqa.at[:, other], dst_ref=dqo, send_sem=xsend.at[1], recv_sem=xrecv.at[1], **peer)
            kvr.ticks(0, 0, PAIR)
            relay.ticks(PAIR, nblk // PAIR, nblk)
            @turns(nz // PAIR)
            def _(q):
                @pl.when(q == 1)
                def _():
                    kvr.ticks(1, 0, PAIR)

                @pl.when(q == PAIR)
                def _():
                    kvr.ticks(PAIR, 0, PAIR)

                @pl.when(q == 3)
                def _():
                    relay.ticks(3, 0, nblk)
                    dq_give.start()

                def between():
                    @pl.when(q == 0)
                    def _():
                        htb_in.wait()
                pair(q + 1, base + q * nm, between)
            kv_give.wait()
            dq_give.wait()
            for cp in ins:
                cp.wait()
            for h in range(nz):
                aT[:, pl.ds(pl.multiple_of(c * qw + h * HEAD_DIM, HEAD_DIM), HEAD_DIM)] = dqa[h, sp].T
                aT[:, pl.ds(pl.multiple_of(far * qw + h * HEAD_DIM, HEAD_DIM), HEAD_DIM)] = dqo[h].T
            for e in range(PAIR):
                er = span(e, HEAD_DIM)
                dkp[e, :, pl.ds(pl.multiple_of(c * HEAD_DIM, HEAD_DIM), HEAD_DIM)] = kva[z, er, pl.ds(pl.multiple_of(c * rows, rows), rows)].T
                dkp[e, :, pl.ds(pl.multiple_of(far * HEAD_DIM, HEAD_DIM), HEAD_DIM)] = kvo[er, :].T

            @turns(dm // cw)
            def _(n):
                @pl.when(n + nw - 1 < dm // cw)
                def _():
                    w_tile(n + nw - 1).start()
                w_tile(n).wait()
                rr = pl.ds(pl.multiple_of(n * cw, cw), cw)
                dn[:, rr] = dot_nt(aT[...], wr[n % nw]) + dot_nt(dkp[0], wkv[0, rr, :]) + dot_nt(dkp[1], wkv[1, rr, :])
            nr = 16
            gain = jnp.concatenate([par[g:g + 1, :] for g in range(dm // HEAD_DIM)], axis=1)

            @turns(rows // nr)
            def _(i):
                rr = pl.ds(pl.multiple_of(i * nr, nr), nr)
                xf = xo[rr, :].astype(F32)
                inv = lax.rsqrt(jnp.mean(xf * xf, axis=-1, keepdims=YES) + NORM_EPS)
                unit = xf * inv
                g = dn[rr, :]
                du = g * gain
                di = inv * (du - unit * jnp.mean(du * unit, axis=-1, keepdims=YES))
                xo[rr, :] = (dyo[rr, :].astype(F32) + di).astype(BF16)
                dn[rr, :] = g * unit
            tot = jnp.sum(dn[...], axis=KEYS, keepdims=YES)
            for j in range(dm // HEAD_DIM):
                sma[sp, j:j + 1, :] = tot[:, span(j, HEAD_DIM)]
            dx_out = pltpu.make_async_copy(xo, dx_o, lq.at[PAIR])
            dx_out.start()
            dx_out.wait()
        pl.run_scoped(in_rows, vm((4, cw, dm), BF16), vm((rows, dm), BF16), vm((rows, dm), BF16), vm((PAIR, dm, cw), BF16),
                      vm((PAIR, rows, cw), BF16), vm((rows, dm), F32))

        def small(o):
            return pltpu.make_async_remote_copy(src_ref=sma.at[sp], dst_ref=sma.at[sp], send_sem=ssend.at[0], recv_sem=srecv.at[0],
                                                device_id=(dp, (sp + o) % n_sp), device_id_type=MESH)

        @pl.loop(1, n_sp)
        def _(o):
            small(o).start()
        kvr.ticks(3, 0, PAIR)

        for m in range(nm):
            piece = base + 4 * nm + m
            product(lambda o: kva[o], lambda o: span(o, bk), nz, m, piece)
            give([w.at[span(m, qw), pl.ds(pl.multiple_of(c * HEAD_DIM, HEAD_DIM), HEAD_DIM)] for w in (dwk_o, dwv_o)], piece)
        npiece = base + 5 * nm
        for i in range(nslot):
            free(npiece - nslot + i)

        for i, got in enumerate((dwo_o, dwo_o.at[0:npiece * qw * cw // dm - dm, :])):
            pltpu.make_async_copy(got, got, trecv.at[i]).wait()
        ref = sma.at[pl.ds(0, n_sp - 1)]
        pltpu.make_async_copy(ref, ref, ssend.at[0]).wait()
        pltpu.make_async_copy(ref, ref, srecv.at[0]).wait()
        ng = dm // HEAD_DIM
        tot = sma[0, 0:ng, :]
        for o in range(1, n_sp):
            tot = tot + sma[o, 0:ng, :]
        smo[0:ng, :] = tot
        for cc in range(PAIR):
            for zz in range(nz):
                smo[ng + cc * nz + zz:ng + cc * nz + zz + 1, :] = sma[zz * PAIR + cc, 16:17, :]
            for e in range(PAIR):
                tot = sma[cc, 17 + e:18 + e, :]
                for zz in range(1, nz):
                    tot = tot + sma[zz * PAIR + cc, 17 + e:18 + e, :]
                smo[PAIR * ng + PAIR * e + cc:PAIR * ng + PAIR * e + cc + 1, :] = tot
        out = pltpu.make_async_copy(smo, small_o, lq.at[PAIR])
        out.start()
        out.wait()
    pl.run_scoped(late, vm((3, qw, cw), F32), vm((rows, dm), BF16), vm((qw, nblk * rows), BF16), dma((6,)))
    relay.finish(ht_h.at[0:7 * HEAD_DIM // PAIR, :])
    kvr.finish(dy_h.at[0:7 * HEAD_DIM * bk // dm, :])
    for d in range(PAIR):
        pltpu.make_async_copy(rs.at[d], rs.at[d], rsend.at[d]).wait()


def k3(n_sp, x, dy_own, par, qt, at, ao, lse, k, kt, v, vt, cs, ht, dyf, wq, wk, wv, wo):
    rows, dm = x.shape
    nblk, seq, nz = qt.shape[0], k.shape[0], n_sp // PAIR
    heads = qt.shape[PAIR] // rows
    npiece = dm // (PAIR * HEAD_DIM) + 5 * (dm // (heads * HEAD_DIM))
    sds, vm, dma = jax.ShapeDtypeStruct, pltpu.VMEM, pltpu.SemaphoreType.DMA
    ns = PAIR * (dm // HEAD_DIM) + 8
    scratch = [vm((seq, PAIR * HEAD_DIM), BF16), vm((HEAD_DIM, seq), BF16), vm((heads * HEAD_DIM - at.shape[0], rows), BF16), vm((HEAD_DIM, seq), F32), vm((seq, HEAD_DIM), F32), vm((seq, HEAD_DIM), F32), vm((nz, nblk, HEAD_DIM, rows), BF16), vm((nz, HEAD_DIM, rows), BF16),
               vm((PAIR, nz - 1, PAIR * rows, HEAD_DIM), F32), vm((nz, PAIR * HEAD_DIM, PAIR * rows), BF16), vm((PAIR * HEAD_DIM, rows), BF16), vm((n_sp, 24, HEAD_DIM), F32), vm((ns, HEAD_DIM), F32),
               dma((PAIR,)), dma((PAIR, 4 * nblk)), dma((PAIR,)), dma((PAIR, nz - 1)), dma((PAIR,)), dma((PAIR, 8)), dma((4,)), dma((4,)),
               dma((1,)), dma((1,)), dma((4, PAIR)), dma((PAIR,)), dma((4, PAIR)), dma((8,))]
    outs = [sds((rows, dm), BF16), sds((rows, dm), BF16), sds(wq.shape, F32), sds(wk.shape, F32), sds(wv.shape, F32), sds(wo.shape, F32), sds((ns, HEAD_DIM), F32)]
    return pl.pallas_call(
        functools.partial(k3_kernel, nblk // PAIR, rows, (nz, n_sp, heads)), out_shape=outs, in_specs=[ANY, ANY, VM] + [ANY] * 15, out_specs=[ANY] * len(outs),
        scratch_shapes=scratch, compiler_params=pltpu.CompilerParams(collective_id=PAIR, has_side_effects=YES, vmem_limit_bytes=63 * MIB),
        name='attend_back')(x, dy_own, par, qt, at, ao, lse, k, kt, v, vt, cs, ht, dyf, wq, wk, wv, wo)


def solution(mesh):
    n_sp = mesh.shape['sp']

    def step(hidden, d_out, positions, norm_gain, w_query, b_query, w_key, b_key, w_value, b_value, w_out):
        x, dy = hidden[0], d_out[0]
        rows, dm = x.shape
        par = jnp.concatenate([b.astype(F32).reshape(-1, HEAD_DIM) for b in (norm_gain, b_query, b_key, b_value)])
        hf, ht, qt, k, kt, v, vt, cs = k1(n_sp, x, positions, par, w_query, w_key, w_value)
        dyf, at, lse, ao = k2(n_sp, dy, qt, k, vt)
        y, dx, dwq, dwk, dwv, dwo, small = k3(n_sp, x, dy, par, qt, at, ao, lse, k, kt, v, vt, cs, ht, dyf, w_query, w_key, w_value, w_out)
        ng = dm // HEAD_DIM
        return (y[None], dx[None], small[:ng].reshape(-1), dwq, small[ng:PAIR * ng].reshape(-1), dwk, small[PAIR * ng:PAIR * ng + PAIR].reshape(-1),
                dwv, small[PAIR * ng + PAIR:PAIR * ng + 4].reshape(-1), dwo)

    seq_spec = P('dp', 'sp', None)
    in_specs = (seq_spec, seq_spec, P('dp', 'sp')) + (P(),) * 8
    out_specs = (seq_spec, seq_spec, P('dp'), P('dp', None), P('dp'), P('dp', None), P('dp'), P('dp', None), P('dp'), P('dp', None))
    return jax.shard_map(step, mesh=mesh, in_specs=in_specs, out_specs=out_specs, check_vma=False)
```

```python
import functools, math
import jax
import jax.numpy as jnp
from jax import lax
from jax.experimental import pallas as pl
from jax.experimental.pallas import tpu as pltpu
from jax.sharding import PartitionSpec as P

HEAD_DIM = 128
ROPE_BASE = 1000000.0
NORM_EPS = 1e-6
MESH = pl.DeviceIdType.MESH
PAIR, TRIO, QUAD = 2, 3, 4
TOP = slice(0, 1)
KEYS = 0
YES = True
MIB = 1 << 20
NSUB = PAIR
F32 = jnp.float32
BF16 = jnp.bfloat16
ANY = pl.BlockSpec(memory_space=pl.ANY)
VM = pl.BlockSpec(memory_space=pltpu.VMEM)


def span(i, n):
    return slice(i * n, (i + 1) * n)


def turns(n):
    return pl.loop(0, n)


class Ring:
    def __init__(self, full, own, rows, nz, sems):
        self.full, self.own, self.rows, self.nz = full, own, rows, nz
        self.send, self.recv, self.drecv = sems
        self.sp = lax.axis_index('sp')
        self.dp = lax.axis_index('dp')
        self.z, self.c = self.sp // PAIR, self.sp % PAIR
        self.sub = rows // (PAIR * NSUB)
        self.nsend = 7 * NSUB

    def dev(self, z, c):
        return (self.dp, z * PAIR + c)

    def where(self, d, j, z):
        s = j // (PAIR * NSUB)
        r = j % (PAIR * NSUB)
        half = (r // NSUB + d) % PAIR
        origin = (z + (self.nz - s if d == 0 else s)) % self.nz
        return pl.multiple_of((origin * PAIR + self.c) * self.rows + half * (self.rows // PAIR) + (r % NSUB) * self.sub, self.sub)

    def ici(self, d, j, src=None):
        off = self.where(d, j, self.z)
        to = (self.z + (1 if d == 0 else self.nz - 1)) % self.nz
        return pltpu.make_async_remote_copy(
            src_ref=self.full.at[pl.ds(off, self.sub)] if src is None else src,
            dst_ref=self.full.at[pl.ds(off, self.sub)],
            send_sem=self.send.at[d], recv_sem=self.recv.at[d, j],
            device_id=self.dev(to, self.c), device_id_type=MESH)

    def d2d(self, d, j):
        frm = (self.z + (self.nz - 1 if d == 0 else 1)) % self.nz
        off = self.where(d, j, frm)
        return pltpu.make_async_remote_copy(
            src_ref=self.full.at[pl.ds(off, self.sub)], dst_ref=self.full.at[pl.ds(off, self.sub)],
            send_sem=self.send.at[PAIR], recv_sem=self.drecv.at[j // (PAIR * NSUB)],
            device_id=self.dev(self.z, 1 - self.c), device_id_type=MESH)

    def d2d_own(self):
        off = pl.multiple_of(self.sp * self.rows, self.rows)
        return pltpu.make_async_remote_copy(
            src_ref=self.own, dst_ref=self.full.at[pl.ds(off, self.rows)],
            send_sem=self.send.at[TRIO], recv_sem=self.drecv.at[QUAD],
            device_id=self.dev(self.z, 1 - self.c), device_id_type=MESH)

    def start(self):
        @turns(PAIR * NSUB)
        def _(j):
            for d in range(PAIR):
                half = (j // NSUB + d) % PAIR
                off = pl.multiple_of(half * (self.rows // PAIR) + (j % NSUB) * self.sub, self.sub)
                self.ici(d, j, self.own.at[pl.ds(off, self.sub)]).start()
        self.d2d_own().start()

    def tick(self, j):
        for d in range(PAIR):
            self.ici(d, j).wait_recv()

            @pl.when(j + PAIR * NSUB < self.nsend)
            def _():
                self.ici(d, j + PAIR * NSUB).start()
            self.d2d(d, j).start()

    def total(self, rows, sem):
        ref = self.full.at[pl.ds(0, rows)]
        pltpu.make_async_copy(ref, ref, sem).wait()

    def finish_sends(self):
        each = self.nsend * self.sub
        self.total(each, self.send.at[0])
        self.total(each, self.send.at[1])
        self.total(PAIR * each, self.send.at[PAIR])
        self.d2d_own().wait_send()

    def wait_other(self, s):
        self.total(self.rows if s == TRIO else PAIR * self.rows, self.drecv.at[s])


def ring_sems(nz):
    return [pltpu.SemaphoreType.DMA((QUAD,)), pltpu.SemaphoreType.DMA((PAIR, 7 * NSUB)), pltpu.SemaphoreType.DMA((5,))]


def greet_all(n_sp):
    sp, dp = lax.axis_index('sp'), lax.axis_index('dp')
    bar = pltpu.get_barrier_semaphore()

    @pl.loop(1, n_sp)
    def _(o):
        pl.semaphore_signal(bar, inc=1, device_id=(dp, (sp + o) % n_sp), device_id_type=MESH)

    def all_here():
        pl.semaphore_wait(bar, n_sp - 1)
    return all_here


def k1_kernel(n_sp, x_h, pos, par, wq, wk, wv, hf, ht, qt, k_o, kt_o, v_o, vt_o, cs_o,
              pos_all, wq_v, wk_v, wv_v, hb, htb, qs, ks, kts, vs, vts, css, send, recv, drecv, psend, precv, lsem, wsem, osem):
    nz = n_sp // PAIR
    rows, dm = x_h.shape
    qw = wq_v.shape[1]
    sp, dp = lax.axis_index('sp'), lax.axis_index('dp')
    z, c = sp // PAIR, sp % PAIR
    far = 1 - c
    heads = qw // HEAD_DIM
    half_dim = HEAD_DIM // PAIR
    ng = dm // HEAD_DIM
    mine = pl.ds(pl.multiple_of(sp * rows, rows), rows)
    ring = Ring(hf, hf.at[mine], rows, nz, (send, recv, drecv))
    x_in = pltpu.make_async_copy(x_h, hb, lsem.at[0])
    x_in.start()
    all_here = greet_all(n_sp)
    pos_copy = pltpu.make_async_copy(pos, pos_all.at[sp], lsem.at[1])
    pos_copy.start()

    def head_of(g):
        return (z + g) % heads

    wcopies = [pltpu.make_async_copy(wq.at[:, pl.ds(pl.multiple_of(c * qw + head_of(g) * HEAD_DIM, HEAD_DIM), HEAD_DIM)],
                                     wq_v.at[:, span(g, HEAD_DIM)], wsem.at[g]) for g in range(heads)]
    cols = pl.ds(pl.multiple_of(c * HEAD_DIM, HEAD_DIM), HEAD_DIM)
    wcopies += [pltpu.make_async_copy(wk.at[:, cols], wk_v, lsem.at[PAIR]), pltpu.make_async_copy(wv.at[:, cols], wv_v, lsem.at[TRIO])]
    for w in wcopies:
        w.start()
    x_in.wait()
    gain = jnp.concatenate([par[g:g + 1, :] for g in range(ng)], axis=1)
    nr = 16

    @turns(rows // nr)
    def _(i):
        rr = pl.ds(pl.multiple_of(i * nr, nr), nr)
        xf = hb[rr, :].astype(F32)
        inv = lax.rsqrt(jnp.mean(xf * xf, axis=-1, keepdims=YES) + NORM_EPS)
        hb[rr, :] = (xf * inv * gain).astype(BF16)
    own_out = pltpu.make_async_copy(hb, hf.at[mine], lsem.at[0])
    own_out.start()
    all_here()

    def pos_send(o):
        return pltpu.make_async_remote_copy(src_ref=pos, dst_ref=pos_all.at[sp], send_sem=psend.at[0], recv_sem=precv.at[0],
                                            device_id=(dp, (sp + o) % n_sp), device_id_type=MESH)

    @pl.loop(1, n_sp)
    def _(o):
        pos_send(o).start()
    own_out.wait()
    ring.start()
    for w in wcopies:
        w.wait()
    pos_copy.wait()
    others = pos_all.at[pl.ds(0, n_sp - 1)]
    pltpu.make_async_copy(others, others, psend.at[0]).wait()
    pltpu.make_async_copy(others, others, precv.at[0]).wait()

    freq = jnp.exp(lax.broadcasted_iota(jnp.int32, (half_dim, 1), 0).astype(F32) * (-2.0 / HEAD_DIM * math.log(ROPE_BASE)))

    def outs(blk):
        cols = pl.ds(pl.multiple_of(blk * rows, rows), rows)
        return [pltpu.make_async_copy(htb, ht.at[:, cols], osem.at[0]),
                pltpu.make_async_copy(qs, qt.at[blk], osem.at[1]),
                pltpu.make_async_copy(ks, k_o.at[cols], osem.at[PAIR]),
                pltpu.make_async_copy(kts, kt_o.at[:, cols], osem.at[TRIO]),
                pltpu.make_async_copy(vs, v_o.at[cols], osem.at[QUAD]),
                pltpu.make_async_copy(vts, vt_o.at[:, cols], osem.at[5]),
                pltpu.make_async_copy(css, cs_o.at[:, cols], osem.at[6])]

    def compute(n, blk):
        load = pltpu.make_async_copy(hf.at[pl.ds(pl.multiple_of(blk * rows, rows), rows)], hb, lsem.at[0])
        load.start()
        load.wait()
        @pl.when(n > 0)
        def _():
            for o in outs(blk):
                o.wait()
        ang = freq * pos_all[blk].astype(F32)
        cos, sin = jnp.cos(ang), jnp.sin(ang)
        css[0:half_dim, :] = cos
        css[half_dim:, :] = sin
        h = hb[...]
        htb[...] = h.T

        def rope_t(t):
            a, b = t[:half_dim], t[half_dim:]
            return jnp.concatenate([a * cos - b * sin, b * cos + a * sin], axis=KEYS)
        for g in range(heads // PAIR):
            cols = slice(g * PAIR * HEAD_DIM, (g + 1) * PAIR * HEAD_DIM)
            bias = jnp.concatenate([par[pl.ds(ng + c * heads + head_of(g * PAIR + e), 1), :] for e in range(PAIR)], axis=1)
            q = jnp.dot(h, wq_v[:, cols], preferred_element_type=F32) + bias
            t = q.T
            for e in range(PAIR):
                hd = g * PAIR + e
                qs[:, span(hd, rows)] = rope_t(t[span(e, HEAD_DIM)]).astype(BF16)
        k = jnp.dot(h, wk_v[...], preferred_element_type=F32) + par[pl.ds(PAIR * ng + c, 1), :]
        kt = rope_t(k.T)
        kts[...] = kt.astype(BF16)
        ks[...] = kt.T.astype(BF16)
        v = jnp.dot(h, wv_v[...], preferred_element_type=F32) + par[pl.ds(PAIR * ng + PAIR + c, 1), :]
        vs[...] = v.astype(BF16)
        vts[...] = v.T.astype(BF16)
        for o in outs(blk):
            o.start()

    @turns(n_sp)
    def _(n):
        m = n - PAIR
        s = m // QUAD
        b = jnp.where(s == TRIO, (m % QUAD) * PAIR, m % QUAD)
        other = jnp.where(n < PAIR, n, b // PAIR)
        left = b % PAIR == 0
        dist = jnp.where(n < PAIR, 0, s + 1)

        @pl.when((n >= PAIR) & (m % QUAD == 0))
        def _():
            @turns(jnp.where(s == TRIO, NSUB, PAIR * NSUB))
            def _(r):
                ring.tick(s * PAIR * NSUB + r)

        @pl.when(n == 1)
        def _():
            ring.d2d_own().wait_recv()

        for h in range(QUAD):
            @pl.when((n >= PAIR) & (other == 1) & left & (s == h))
            def _():
                ring.wait_other(h)
        zb = (z + jnp.where(left, nz - dist, dist)) % nz
        cb = jnp.where(other == 1, 1 - c, c)
        compute(n, zb * PAIR + cb)
    for o in outs(0):
        o.wait()
    ring.finish_sends()


def k1(n_sp, x, pos, par, wq, wk, wv):
    rows, dm = x.shape
    seq = rows * n_sp
    nz = n_sp // PAIR
    qw = wq.shape[1] // PAIR
    heads = qw // HEAD_DIM
    sds = jax.ShapeDtypeStruct
    outs = [sds((seq, dm), BF16), sds((dm, seq), BF16), sds((n_sp, HEAD_DIM, heads * rows), BF16),
            sds((seq, HEAD_DIM), BF16), sds((HEAD_DIM, seq), BF16), sds((seq, HEAD_DIM), BF16), sds((HEAD_DIM, seq), BF16),
            sds((HEAD_DIM, seq), F32)]
    vm, dma = pltpu.VMEM, pltpu.SemaphoreType.DMA
    scratch = [vm((n_sp,) + pos.shape, jnp.int32), vm((dm, qw), BF16), vm((dm, HEAD_DIM), BF16), vm((dm, HEAD_DIM), BF16),
               vm((rows, dm), BF16), vm((dm, rows), BF16), vm((HEAD_DIM, heads * rows), BF16),
               vm((rows, HEAD_DIM), BF16), vm((HEAD_DIM, rows), BF16), vm((rows, HEAD_DIM), BF16), vm((HEAD_DIM, rows), BF16),
               vm((HEAD_DIM, rows), F32)] + ring_sems(nz) + [dma((1,)), dma((1,)), dma((QUAD,)), dma((heads,)), dma((7,))]
    return pl.pallas_call(
        functools.partial(k1_kernel, n_sp), out_shape=outs,
        in_specs=[ANY, ANY, VM, ANY, ANY, ANY], out_specs=[ANY] * len(outs), scratch_shapes=scratch,
        compiler_params=pltpu.CompilerParams(collective_id=0, has_side_effects=YES, vmem_limit_bytes=60 * MIB),
        name='gather_project')(x, pos, par, wq, wk, wv)


LOG2E = math.log2(math.e)
NEG = -1e30

def split_scaled(q, scale):
    qs = q.astype(F32) * scale
    hi = qs.astype(BF16)
    lo = (qs - hi.astype(F32)).astype(BF16)
    return jnp.concatenate([hi, lo], axis=KEYS)

def decode(n, nblk):
    one = int if isinstance(n, int) else (lambda x: x.astype(jnp.int32))
    j = sum(one(n >= i * (i + 1)) for i in range(1, nblk // PAIR))
    r = n - j * (j + 1)
    odd = one(r > j)
    return PAIR * j + odd, r - odd * (j + 1)

def fwd_steps(nblk):
    return (nblk // PAIR) * (nblk // PAIR + 1)

def decode_up(n, nq):
    one = int if isinstance(n, int) else (lambda x: x.astype(jnp.int32))
    i = sum(one(n >= m * (m + 1) // PAIR) for m in range(1, nq))
    return i, n - i * (i + 1) // PAIR


def causal_bias(bias, bk, rows):
    d = lax.broadcasted_iota(jnp.int32, (bk, rows), 0) - lax.broadcasted_iota(jnp.int32, (bk, rows), 1)
    bias[0] = jnp.zeros((bk, rows), F32)
    bias[1] = jnp.where(d <= 0, 0.0, NEG)
    bias[PAIR] = jnp.where(d <= rows, 0.0, NEG)


class Fwd:
    def __init__(self, nblk, rows, heads, first, wide, qt, sink, lse, kk, vt, qb, q2, acc, mx, cm, ls, al, rt, lsv, sb, pb, bias, qsem, osem):
        self.__dict__.update(locals())
        self.bk = PAIR * rows
        self.groups = heads * wide
        self.cols = [span(u, rows) for u in range(self.groups)]
        self.halves = (range(0, self.groups // PAIR), range(self.groups // PAIR, self.groups))
        self.nq = nblk // wide
        self.nstep = fwd_steps(nblk) if wide == 1 else self.nq * (self.nq + 1) // PAIR

    def where(self, n):
        if self.wide == 1:
            i, t = decode(n, self.nblk)
            return i, t, t == i // PAIR
        i, t = decode_up(n, self.nq)
        return i, t, t == i

    def load_q(self, i):
        w = self.heads * self.rows
        src = slice(self.first * self.rows, self.first * self.rows + w)
        return [pltpu.make_async_copy(self.qt.at[self.wide * i + e, :, src], self.qb.at[:, span(e, w)], self.qsem.at[e]) for e in range(self.wide)]

    def make_q2(self, i):
        for u in range(self.groups):
            self.q2[i % PAIR, :, self.cols[u]] = split_scaled(self.qb[:, self.cols[u]], LOG2E * HEAD_DIM ** -0.5)

    def prepare(self):
        causal_bias(self.bias, self.bk, self.rows)
        for i in range(PAIR):
            for cp in self.load_q(i):
                cp.start()
            for cp in self.load_q(i):
                cp.wait()
            self.make_q2(i)
        for cp in self.load_q(PAIR):
            cp.start()
        self.acc[...] = jnp.zeros_like(self.acc)
        self.pb[...] = jnp.zeros_like(self.pb)
        self.ls[...] = jnp.zeros_like(self.ls)
        self.al[...] = jnp.zeros_like(self.al)
        self.mx[...] = jnp.zeros_like(self.mx)
        self.scores(0, 0, YES)

    def keys(self, t):
        return pl.ds(pl.multiple_of(t * self.bk, self.bk), self.bk)

    def scores(self, n, part, masked):
        i, t, last = self.where(n)
        kb = self.kk[self.keys(t), :]
        for u in self.halves[part]:
            kind = jnp.where(last, 1 + (i % PAIR if self.wide == 1 else u // self.heads), 0)
            s = jnp.dot(kb, self.q2[i % PAIR, :, self.cols[u]], preferred_element_type=F32)
            if masked:
                s = s + self.bias[kind]
            self.sb[u] = s
            self.cm[:, self.cols[u]] = jnp.max(s.reshape(self.bk // 8, 8, self.rows), axis=KEYS)

    def soft(self, n, part):
        i, t, last = self.where(n)
        for u in self.halves[part]:
            c = self.cols[u]
            m0 = jnp.where(t == 0, NEG, self.mx[TOP, c])
            m1 = jnp.maximum(m0, jnp.max(self.cm[:, c], axis=KEYS, keepdims=YES))
            p = jnp.exp2(self.sb[u] - m1)
            a = jnp.exp2(m0 - m1)
            self.mx[TOP, c] = m1
            self.al[TOP, c] = a
            self.ls[:, c] = self.ls[:, c] * a + jnp.sum(p.reshape(self.bk // 8, 8, self.rows), axis=KEYS)
            self.pb[u] = p.astype(BF16)

    def values(self, n, part):
        i, t, last = self.where(n)
        vb = self.vt[:, self.keys(t)]
        for u in self.halves[part]:
            c = self.cols[u]
            self.acc[:, c] = self.acc[:, c] * self.al[TOP, c] + jnp.dot(vb, self.pb[u], preferred_element_type=F32)

    def out_lse(self, i):
        return pltpu.make_async_copy(self.lsv, self.lse.at[i], self.osem)

    def finish(self, i, part):
        self.sink.before(i, part)
        for u in self.halves[part]:
            c = self.cols[u]
            self.sink.store(u % self.heads, self.wide * i + u // self.heads, (self.acc[:, c] * self.rt[TOP, c]).astype(BF16))
        self.sink.after(i, part)

    def end_block(self, i):
        tot = jnp.sum(self.ls[...], axis=KEYS, keepdims=YES)
        self.rt[TOP, :] = 1.0 / tot
        if self.lse is not None:
            @pl.when(i > 0)
            def _():
                self.out_lse(i).wait()
            self.lsv[TOP, :] = self.mx[TOP, :] + jnp.log2(tot)
            self.out_lse(i).start()
        self.finish(i, 0)

        @pl.when(i + PAIR < self.nq)
        def _():
            for cp in self.load_q(i + PAIR):
                cp.wait()
            self.make_q2(i + PAIR)

        @pl.when(i + TRIO < self.nq)
        def _():
            for cp in self.load_q(i + TRIO):
                cp.start()

    def step(self, n, masked):
        n1 = jnp.minimum(n + 1, self.nstep - 1)
        self.scores(n, 1, masked)
        self.soft(n, 0)
        self.values(jnp.maximum(n - 1, 0), 1)
        self.scores(n1, 0, masked)
        self.soft(n, 1)
        self.values(n, 0)

    def run(self, on_step):
        @turns(self.nstep)
        def _(n):
            on_step(n)
            i, t, last = self.where(n)
            if self.wide == 1:
                self.step(n, YES)
            else:
                masked = last | self.where(n + 1)[PAIR]

                @pl.when(masked)
                def _():
                    self.step(n, YES)

                @pl.when(jnp.logical_not(masked))
                def _():
                    self.step(n, False)

            @pl.when((t == 0) & (n > 0))
            def _():
                self.finish(i - 1, 1)

            @pl.when(last)
            def _():
                self.end_block(i)

    def drain(self):
        self.values(self.nstep - 1, 1)
        self.finish(self.nq - 1, 1)
        if self.lse is not None:
            self.out_lse(self.nq - 1).wait()


def fwd_scratch(nblk, rows, groups, wide):
    vm = pltpu.VMEM
    w, bk = groups * rows, PAIR * rows
    return [vm((HEAD_DIM, w), BF16), vm((PAIR, PAIR * HEAD_DIM, w), BF16), vm((HEAD_DIM, w), F32)] + [vm((8, w), F32)] * 6 + [
            vm((groups, bk, rows), F32), vm((groups, bk, rows), BF16), vm((TRIO, bk, rows), F32),
            pltpu.SemaphoreType.DMA((wide,)), pltpu.SemaphoreType.DMA]


NT = (((1,), (1,)), ((), ()))
SCALE = HEAD_DIM ** -0.5

def dot_nt(a, b):
    return lax.dot_general(a, b, NT, preferred_element_type=F32)

def bwd_steps(nq):
    return nq * (nq + 1) // PAIR

class Bwd:
    def __init__(self, nq, rows, qt, kk, kt, vv, dat, dlt, lsv, qb, q2, cs, dk, dv, dq, dbq, sb, dpb, pb, dsb, bias, dqs, psem):
        self.__dict__.update(locals())
        self.bk = PAIR * rows
        self.nstep = bwd_steps(nq)
        self.cols = [slice(0, rows), slice(rows, PAIR * rows)]

    def loads(self, i):
        slot = i % PAIR
        return [pltpu.make_async_copy(self.qt.at[PAIR * i + e, :, 0:self.rows], self.qb.at[slot, :, self.cols[e]], self.psem.at[slot, e]) for e in range(PAIR)]

    def make_q2(self, i):
        for e in range(PAIR):
            self.q2[i % PAIR, :, self.cols[e]] = split_scaled(self.qb[i % PAIR, :, self.cols[e]], LOG2E * SCALE)

    def prepare(self):
        nq = self.nq
        for i in (0, 1):
            for cp in self.loads(i):
                cp.start()
            for cp in self.loads(i):
                cp.wait()
            self.make_q2(i)
        causal_bias(self.bias, self.bk, self.rows)
        self.dk[...] = jnp.zeros_like(self.dk)
        self.dv[...] = jnp.zeros_like(self.dv)
        self.dq[...] = jnp.zeros_like(self.dq)
        self.dbq[...] = jnp.zeros_like(self.dbq)
        self.pb[...] = jnp.zeros_like(self.pb)
        self.dsb[...] = jnp.zeros_like(self.dsb)
        self.scores(0, 0)

    def keys(self, t):
        return pl.ds(pl.multiple_of(t * self.bk, self.bk), self.bk)

    def qcols(self, i, e):
        return pl.ds(pl.multiple_of(i * self.bk + e * self.rows, self.rows), self.rows)

    def scores(self, n, e):
        i, t = decode_up(n, self.nq)
        kind = jnp.where(t == i, 1 + e, 0)
        s = jnp.dot(self.kk[self.keys(t), :], self.q2[i % PAIR, :, self.cols[e]], preferred_element_type=F32)
        self.sb[e] = s + self.bias[kind]
        self.dpb[e] = jnp.dot(self.vv[self.keys(t), :], self.dat[:, self.qcols(i, e)], preferred_element_type=F32)

    def soft(self, n, e):
        i, t = decode_up(n, self.nq)
        c = self.qcols(i, e)
        p = jnp.exp2(self.sb[e] - self.lsv[TOP, c])
        self.pb[e] = p.astype(BF16)
        self.dsb[e] = (p * (self.dpb[e] - self.dlt[TOP, c])).astype(BF16)

    def grads(self, n, e):
        i, t = decode_up(n, self.nq)
        r = self.keys(t)
        self.dv[r, :] += dot_nt(self.pb[e], self.dat[:, self.qcols(i, e)])
        self.dk[r, :] += dot_nt(self.dsb[e], self.qb[i % PAIR, :, self.cols[e]])
        keep = jnp.where(t == 0, 0.0, 1.0)
        self.dq[:, self.cols[e]] = self.dq[:, self.cols[e]] * keep + jnp.dot(self.kt[:, self.keys(t)], self.dsb[e], preferred_element_type=F32)

    def step(self, n):
        n1 = jnp.minimum(n + 1, self.nstep - 1)
        self.scores(n, 1)
        self.soft(n, 0)
        self.grads(jnp.maximum(n - 1, 0), 1)
        self.scores(n1, 0)
        self.soft(n, 1)
        self.grads(n, 0)

    def finish(self, i, e):
        c = self.qcols(i, e)
        g = self.dq[:, self.cols[e]] * SCALE
        hd = HEAD_DIM // PAIR
        cos, sin = self.cs[0:hd, c], self.cs[hd:, c]
        a, b = g[:hd], g[hd:]
        a, b = a * cos + b * sin, b * cos - a * sin
        self.dbq[0:hd, :] += a
        self.dbq[hd:, :] += b
        blk = PAIR * i + e
        self.dqs[blk, 0:hd, :] = a.astype(BF16)
        self.dqs[blk, hd:, :] = b.astype(BF16)

    def run(self, on_step=lambda n: None):
        @turns(self.nstep)
        def _(n):
            on_step(n)
            i, t = decode_up(n, self.nq)

            @pl.when((t == i) & (i > 0) & (i + 1 < self.nq))
            def _():
                for cp in self.loads(i + 1):
                    cp.wait()
                self.make_q2(i + 1)
            self.step(n)

            @pl.when((t == 0) & (n > 0))
            def _():
                self.finish(i - 1, 1)

                @pl.when(i + 1 < self.nq)
                def _():
                    for cp in self.loads(i + 1):
                        cp.start()

            @pl.when(t == i)
            def _():
                self.finish(i, 0)
        self.grads(self.nstep - 1, 1)
        self.finish(self.nq - 1, 1)


def bwd_scratch(nq, rows):
    vm = pltpu.VMEM
    bk, seq = PAIR * rows, PAIR * rows * nq
    return [vm((seq, PAIR * HEAD_DIM), BF16), vm((HEAD_DIM, seq), BF16), vm((seq, HEAD_DIM), BF16), vm((HEAD_DIM, seq), BF16), vm((8, seq), F32), vm((8, seq), F32),
            vm((PAIR, HEAD_DIM, bk), BF16), vm((PAIR, PAIR * HEAD_DIM, bk), BF16), vm((HEAD_DIM, seq), F32), vm((seq, HEAD_DIM), F32), vm((seq, HEAD_DIM), F32),
            vm((HEAD_DIM, bk), F32), vm((HEAD_DIM, rows), F32), vm((PAIR, bk, rows), F32), vm((PAIR, bk, rows), F32), vm((PAIR, bk, rows), BF16), vm((PAIR, bk, rows), BF16),
            vm((TRIO, bk, rows), F32), vm((PAIR * nq, HEAD_DIM, rows), BF16), pltpu.SemaphoreType.DMA((PAIR, PAIR)), pltpu.SemaphoreType.DMA((PAIR * nq,))]


def load_bwd(k_h, kt_h, v_h, cs_h, lse_h, rows, nblk, kk, kt, vv, cs, lsv, sem):
    cps = [pltpu.make_async_copy(k_h, kk.at[:, 0:HEAD_DIM], sem.at[0]), pltpu.make_async_copy(k_h, kk.at[:, HEAD_DIM:], sem.at[1]),
           pltpu.make_async_copy(kt_h, kt, sem.at[PAIR]), pltpu.make_async_copy(v_h, vv, sem.at[TRIO]), pltpu.make_async_copy(cs_h, cs, sem.at[QUAD])]
    for c in cps:
        c.start()

    cps += [pltpu.make_async_copy(lse_h.at[b, :, 0:rows], lsv.at[:, span(b, rows)], sem.at[5 + b]) for b in range(nblk)]
    for c in cps[5:]:
        c.start()
    return cps


class GradAtt:
    def __init__(self, dy_h, at_h, nb, dat, dlt, wo_v, dyb, atb, sem):
        self.__dict__.update(locals())
        self.blk = dyb.shape[1]

    def copies(self, b):
        s = b % PAIR
        r = pl.ds(pl.multiple_of(b * self.blk, self.blk), self.blk)
        return [pltpu.make_async_copy(self.dy_h.at[r], self.dyb.at[s], self.sem.at[s]),
                pltpu.make_async_copy(self.at_h.at[0:HEAD_DIM, r], self.atb.at[s], self.sem.at[PAIR + s])]

    def start(self, b):
        for c in self.copies(b):
            c.start()

    def block(self, b):
        for c in self.copies(b):
            c.wait()
        d = dot_nt(self.dyb[b % PAIR], self.wo_v[...]).T.astype(BF16)
        r = pl.ds(pl.multiple_of(b * self.blk, self.blk), self.blk)
        self.dat[:, r] = d
        self.dlt[TOP, r] = jnp.sum(d.astype(F32) * self.atb[b % PAIR].astype(F32), axis=KEYS, keepdims=YES)


class Rows:
    def __init__(self, at, ats, rows, sem):
        self.at, self.ats, self.rows, self.sem = at, ats, rows, sem

    def copy(self, i, part):
        cut = self.ats.shape[0] // HEAD_DIM // PAIR * HEAD_DIM
        r = slice(cut, None) if part else slice(0, cut)
        return pltpu.make_async_copy(self.ats.at[r], self.at.at[r, pl.ds(pl.multiple_of(i * self.rows, self.rows), self.rows)], self.sem.at[part])

    def before(self, i, part):
        @pl.when(i > 0)
        def _():
            self.copy(i, part).wait()

    def store(self, g, blk, value):
        self.ats[span(g, HEAD_DIM), :] = value

    def after(self, i, part):
        self.copy(i, part).start()


def k2_kernel(n_sp, own_dy, qt, k_h, vt_h, dyf, at, lse, ao, kk, vt, ats, *scr):
    *scr, asem, send, recv, drecv, lsem, xsem = scr
    rows = own_dy.shape[0]
    heads = at.shape[0] // HEAD_DIM
    nz = n_sp // PAIR
    sp, dp = lax.axis_index('sp'), lax.axis_index('dp')
    ring = Ring(dyf, own_dy, rows, nz, (send, recv, drecv))
    loads = [pltpu.make_async_copy(k_h, kk.at[:, 0:HEAD_DIM], lsem.at[0]), pltpu.make_async_copy(k_h, kk.at[:, HEAD_DIM:], lsem.at[1]),
             pltpu.make_async_copy(vt_h, vt, lsem.at[PAIR])]
    for c in loads:
        c.start()
    greet_all(n_sp)()
    ring.start()
    mine = pltpu.make_async_copy(own_dy, dyf.at[pl.ds(pl.multiple_of(sp * rows, rows), rows)], lsem.at[TRIO])
    mine.start()
    for c in loads:
        c.wait()
    sink = Rows(at, ats, rows, asem)
    f = Fwd(n_sp, rows, heads, 0, 1, qt, sink, lse, kk, vt, *scr)
    f.prepare()

    def due(n):
        return jnp.clip((n - TRIO) // 6, 0, ring.nsend)

    def on_step(n):
        @pl.loop(due(n), due(n + 1))
        def _(j):
            ring.tick(j)
    f.run(on_step)
    f.drain()
    for part in range(PAIR):
        sink.copy(0, part).wait()
    other = (sp // PAIR) * PAIR + 1 - sp % PAIR
    give = pltpu.make_async_remote_copy(
        src_ref=at.at[:, pl.ds(pl.multiple_of(other * rows, rows), rows)], dst_ref=ao, send_sem=xsem.at[0], recv_sem=xsem.at[1],
        device_id=(dp, other), device_id_type=MESH)
    give.start()

    @pl.loop(due(f.nstep), ring.nsend)
    def _(j):
        ring.tick(j)

    for s in range(QUAD):
        ring.wait_other(s)
    ring.d2d_own().wait_recv()
    give.wait()
    mine.wait()
    ring.finish_sends()


def k2(n_sp, own_dy, qt, k, vt):
    rows, dm = own_dy.shape
    seq = rows * n_sp
    heads = qt.shape[PAIR] // rows * 5 // 8
    sds, vm, dma = jax.ShapeDtypeStruct, pltpu.VMEM, pltpu.SemaphoreType.DMA
    outs = [sds((seq, dm), BF16), sds((heads * HEAD_DIM, seq), BF16), sds((n_sp, 8, heads * rows), F32), sds((heads * HEAD_DIM, rows), BF16)]
    return pl.pallas_call(
        functools.partial(k2_kernel, n_sp), out_shape=outs, in_specs=[ANY] * QUAD, out_specs=[ANY] * QUAD,
        scratch_shapes=[vm((seq, PAIR * HEAD_DIM), BF16), vm((HEAD_DIM, seq), BF16), vm((heads * HEAD_DIM, rows), BF16)] + fwd_scratch(n_sp, rows, heads, 1)
        + [dma((PAIR,))] + ring_sems(n_sp // PAIR) + [dma((QUAD,)), dma((PAIR,))],
        compiler_params=pltpu.CompilerParams(collective_id=1, has_side_effects=YES, vmem_limit_bytes=62 * MIB),
        name='gather_attend')(own_dy, qt, k, vt)


TICK0 = (5, 6, 7, 9, 13, 15, 18, 19, 21, 24, 31, 32, 34, 35)
TICK1 = (10, 20, 25, 26, 27, 33)


class Relay:
    def __init__(self, blk, nr, nz, send, recv):
        self.blk, self.nr, self.nz, self.send, self.recv = blk, nr, nz, send, recv
        sp = lax.axis_index('sp')
        self.dp, self.z, self.c = lax.axis_index('dp'), sp // PAIR, sp % PAIR

    def copy(self, d, s, r):
        origin = (self.z + (self.nz - s if d == 0 else s)) % self.nz
        to = (self.z + (1 if d == 0 else self.nz - 1)) % self.nz
        ref = self.blk(origin, r)
        i = s * self.nr + r
        return pltpu.make_async_remote_copy(src_ref=ref, dst_ref=ref, send_sem=self.send.at[d], recv_sem=self.recv.at[d, i],
                                            device_id=(self.dp, to * PAIR + self.c), device_id_type=MESH)

    def own(self, r):
        for d in range(PAIR):
            self.copy(d, 0, r).start()

    def tick(self, s, r):
        for d in range(PAIR):
            if s == TRIO:
                @pl.when(r % PAIR == d)
                def _():
                    self.copy(d, TRIO, r).wait_recv()
            else:
                self.copy(d, s, r).wait_recv()
                if s == PAIR:
                    @pl.when(r % PAIR == d)
                    def _():
                        self.copy(d, TRIO, r).start()
                else:
                    self.copy(d, s + 1, r).start()

    def ticks(self, s, lo, hi):
        @pl.loop(lo, hi)
        def _(r):
            self.tick(s, r)

    def finish(self, ref):
        for d in range(PAIR):
            pltpu.make_async_copy(ref, ref, self.send.at[d]).wait()


def k3_kernel(nq, rows, dims, x_h, dyo_h, par, qt, at, ao, lse, k_h, kt_h, v_h, vt_h, cs_h, ht_h, dy_h, wq_h, wk_h, wv_h, wo_h,
              y_o, dx_o, dwq_o, dwo_o, small_o, kv_o, kvf_o,
              kk, vt, ao2, cs, dk, dv, dqa, dqo, rs, kva, kvo, sma, smo, qsend, qrecv, rsend, rrecv, ksend, krecv, xsend, xrecv, ssend, srecv, tsend, trecv, tl, lq):
    nz, n_sp, heads = dims
    nblk = PAIR * nq
    hd = HEAD_DIM // PAIR
    qw = heads * HEAD_DIM
    bk = PAIR * rows
    dm = x_h.shape[1]
    cw = PAIR * HEAD_DIM
    vm = pltpu.VMEM
    dma = pltpu.SemaphoreType.DMA
    sp, dp = lax.axis_index('sp'), lax.axis_index('dp')
    z, c = sp // PAIR, sp % PAIR
    far = 1 - c
    other = z * PAIR + 1 - c
    peer = dict(device_id=(dp, other), device_id_type=MESH)

    relay = Relay(lambda o, r: dqa.at[o, r], nblk, nz, qsend, qrecv)
    kvr = Relay(lambda o, r: kva.at[o, pl.ds(pl.multiple_of(r * HEAD_DIM, HEAD_DIM), HEAD_DIM)], PAIR, nz, ksend, krecv)
    all_here = greet_all(n_sp)
    sma[sp] = jnp.zeros(sma.shape[1:], F32)

    nstep = bwd_steps(nq)
    own_at = [(r // PAIR + 1) * (r // PAIR + PAIR) // PAIR + r % PAIR + PAIR for r in range(nblk)]

    def count(n, at_step):
        return sum((n >= a).astype(jnp.int32) for a in at_step)

    def back(*scr):
        *scr, wo_v, dyb, atb, sem, sem2 = scr
        kt, vv, dat, dlt, lsv, qb, q2, dq, dbq, sb, dpb, pb, dsb, bias, psem = scr
        row0 = pl.multiple_of(c * qw + z * HEAD_DIM, HEAD_DIM)
        w_in = pltpu.make_async_copy(wo_h.at[pl.ds(row0, HEAD_DIM)], wo_v, sem2.at[QUAD])
        w_in.start()
        vt_in = pltpu.make_async_copy(vt_h, vt, lq.at[0])
        vt_in.start()
        ga = GradAtt(dy_h, at, nq, dat, dlt, wo_v, dyb, atb, sem2)
        ga.start(0)
        kin = load_bwd(k_h, kt_h, v_h, cs_h, lse, rows, nblk, kk, kt, vv, cs, lsv, sem)
        ga.start(1)
        w_in.wait()
        ga.block(0)
        for cp in kin:
            cp.wait()
        vt_in.wait()
        all_here()
        b = Bwd(nq, rows, qt, kk, kt, vv, dat, dlt, lsv, qb, q2, cs, dk, dv, dq, dbq, sb, dpb, pb, dsb, bias, dqa.at[z], psem)
        b.prepare()
        t0 = [min(t, nstep) + 1 for t in TICK0]
        t1 = [min(t, nstep) + 1 for t in TICK1]

        def on_step(n):
            @pl.loop(count(n, own_at), count(n + 1, own_at))
            def _(r):
                relay.own(r)
            relay.ticks(0, count(n, t0), count(n + 1, t0))
            relay.ticks(1, count(n, t1), count(n + 1, t1))
            i, t = decode_up(n, nq)

            @pl.when((t == 0) & (i + 1 < nq))
            def _():
                @pl.when(i + PAIR < nq)
                def _():
                    ga.start(i + PAIR)
                ga.block(i + 1)
        b.run(on_step)
        own_in = sum(1 for a in own_at if a <= nstep)

        @pl.loop(own_in, nblk)
        def _(r):
            relay.own(r)
        sma[sp, 16:17, :] = jnp.sum(dbq[...].T, axis=KEYS, keepdims=YES)
    scr = bwd_scratch(nq, rows)
    keep = scr[1:8] + scr[11:18] + [scr[19]]
    pl.run_scoped(back, *keep, vm((HEAD_DIM, dm), BF16), vm((PAIR, bk, dm), BF16), vm((PAIR, HEAD_DIM, bk), BF16), dma((5 + nblk,)), dma((5,)))
    h0, h1 = sum(1 for t in TICK0 if t + 1 <= nstep), sum(1 for t in TICK1 if t + 1 <= nstep)

    def rs_block(d, s):
        b = (z + (PAIR * nz - 1 - s if d == 0 else 1 + s)) % nz
        return (dk if d == 0 else dv).at[pl.ds(pl.multiple_of(b * bk, bk), bk)]

    def rs_copy(d, s):
        to = (z + (1 if d == 0 else nz - 1)) % nz
        return pltpu.make_async_remote_copy(src_ref=rs_block(d, 0) if s == 0 else rs.at[d, s - 1], dst_ref=rs.at[d, s],
                                            send_sem=rsend.at[d], recv_sem=rrecv.at[d, s], device_id=(dp, to * PAIR + c), device_id_type=MESH)
    for d in range(PAIR):
        rs_copy(d, 0).start()

    def rs_step(s):
        for d in range(PAIR):
            rs_copy(d, s - 1).wait_recv()
            rs[d, s - 1] = rs[d, s - 1] + rs_block(d, s)[...]
        for d in range(PAIR):
            rs_copy(d, s).start()

    kv_give = pltpu.make_async_remote_copy(src_ref=kva.at[z, :, pl.ds(pl.multiple_of(far * rows, rows), rows)], dst_ref=kvo,
                                           send_sem=xsend.at[0], recv_sem=xrecv.at[0], **peer)

    def keys_whole():
        for d in range(PAIR):
            rs_copy(d, nz - PAIR).wait_recv()
        own = pl.ds(pl.multiple_of(z * bk, bk), bk)
        g = ((rs[0, nz - PAIR] + dk[own, :]) * SCALE).T
        a, b = g[:hd], g[hd:]
        cos, sin = cs[0:hd, own], cs[hd:, own]
        g = jnp.concatenate([a * cos + b * sin, b * cos - a * sin], axis=KEYS)
        sma[sp, 17:18, :] = jnp.sum(g.T, axis=KEYS, keepdims=YES)
        kva[z, 0:HEAD_DIM, :] = g.astype(BF16)
        g = rs[1, nz - PAIR] + dv[own, :]
        sma[sp, 18:19, :] = jnp.sum(g, axis=KEYS, keepdims=YES)
        kva[z, HEAD_DIM:, :] = g.T.astype(BF16)
        for r in range(PAIR):
            kvr.own(r)
        kv_give.start()
        kv_far(z).start()

    def kv_far(o):
        return pltpu.make_async_remote_copy(src_ref=kva.at[o], dst_ref=kvf_o.at[o], send_sem=tsend.at[0, PAIR], recv_sem=trecv.at[1], **peer)

    def kv_tick(s):
        kvr.ticks(s, 0, PAIR)
        for o in (((z + nz - 1 - s) % nz, (z + 1 + s) % nz) if s < TRIO else ((z + nz // PAIR) % nz,)):
            kv_far(o).start()

    def late(tile, aT, hta, sem):
        nslot = tile.shape[0]
        ht_in = [pltpu.make_async_copy(ht_h.at[0:qw], hta, lq.at[1])]

        def put(dst, piece, e):
            slot = piece % nslot
            src = tile.at[slot, :, span(e, HEAD_DIM)]
            return (pltpu.make_async_copy(src, dst, tl.at[slot, e]),
                    pltpu.make_async_remote_copy(src_ref=src, dst_ref=dst, send_sem=tsend.at[slot, e], recv_sem=trecv.at[0], **peer))

        def give(dsts, piece):
            for e in range(PAIR):
                for cp in put(dsts[e], piece, e):
                    cp.start()

        def free(piece):
            for e in range(PAIR):
                a, b = put(dwo_o.at[0:qw, 0:HEAD_DIM], piece, e)
                a.wait()
                b.wait_send()

        def att_part(atv, aob, xo, hsem):
            have = at.shape[0] // HEAD_DIM

            def head_rows(g):
                return pl.ds(pl.multiple_of((z + g) % heads * HEAD_DIM, HEAD_DIM), HEAD_DIM)

            def spread(src, dst, base):
                return [pltpu.make_async_copy(src.at[span(g, HEAD_DIM)], dst.at[head_rows(g)], hsem.at[base + g]) for g in range(have)]
            ins = spread(at, atv, 0) + spread(ao, aob, heads) + [pltpu.make_async_copy(x_h, xo, lq.at[TRIO])]
            for cp in ins:
                cp.start()
            turn_rs, turn0, turn1 = [6, 12, 18, 24, 30, 36], [PAIR, PAIR], [QUAD, 15, 27]

            class Here:
                def before(self, i, part):
                    pass

                def store(self, g, blk, value):
                    atv[head_rows(have + g), pl.ds(pl.multiple_of(blk * rows, rows), rows)] = value

                def after(self, i, part):
                    pass

            def rest(*fscr):
                f = Fwd(nblk, rows, heads - have, have, PAIR, qt, Here(), None, kk, vt, *fscr)
                f.prepare()

                def on_step(n):
                    relay.ticks(0, h0 + count(n, turn0), h0 + count(n + 1, turn0))
                    relay.ticks(1, h1 + count(n, turn1), h1 + count(n + 1, turn1))
                    for s in range(1, nz - 1):
                        @pl.when(n + 1 == turn_rs[s - 1])
                        def _():
                            rs_step(s)
                f.run(on_step)
                f.drain()
            pl.run_scoped(rest, *fwd_scratch(nblk, rows, PAIR * (heads - have), PAIR))
            gives = [pltpu.make_async_remote_copy(src_ref=atv.at[head_rows(have + g), pl.ds(pl.multiple_of(other * rows, rows), rows)],
                                                  dst_ref=ao2.at[span(g, HEAD_DIM)], send_sem=xsend.at[PAIR + g], recv_sem=xrecv.at[PAIR + g], **peer)
                     for g in range(heads - have)]
            for cp in ins:
                cp.wait()

            def products(dyt, wt):
                nw = wt.shape[0]

                def dy_tile(n):
                    return pltpu.make_async_copy(dy_h.at[:, pl.ds(pl.multiple_of(n * cw, cw), cw)], dyt.at[n % PAIR], sem.at[n % PAIR])

                def w_tile(n):
                    return pltpu.make_async_copy(wo_h.at[:, pl.ds(pl.multiple_of(n * cw, cw), cw)], wt.at[n % nw], sem.at[PAIR + n % nw])
                dy_tile(0).start()
                for cp in gives:
                    cp.start()
                ntile = dm // cw
                w1 = [1, PAIR, TRIO, QUAD, 5, 6, 7]
                k1 = h1 + len(turn1)

                @turns(ntile)
                def _(n):
                    @pl.when(n + 1 < ntile)
                    def _():
                        dy_tile(n + 1).start()

                    @pl.when(n == 1)
                    def _():
                        ht_in[0].start()

                    @pl.when(n == QUAD)
                    def _():
                        for i in range(nw - 1):
                            w_tile(i).start()
                    relay.ticks(1, k1 + count(n, w1), k1 + count(n + 1, w1))

                    @pl.when(n == TRIO)
                    def _():
                        keys_whole()

                    @pl.when(n == ntile - 1)
                    def _():
                        kv_tick(0)
                    dy_tile(n).wait()

                    @pl.when(n >= nslot)
                    def _():
                        free(n - nslot)
                    tile[n % nslot] = jnp.dot(atv[...], dyt[n % PAIR], preferred_element_type=F32)
                    rws = pl.ds(pl.multiple_of(c * qw, qw), qw)
                    give([dwo_o.at[rws, pl.ds(pl.multiple_of(n * cw + e * HEAD_DIM, HEAD_DIM), HEAD_DIM)] for e in range(PAIR)], n)
                relay.ticks(PAIR, 0, nblk // PAIR)

                for cp in gives:
                    cp.wait()
                for g in range(heads - have):
                    aob[head_rows(have + g), :] = ao2[span(g, HEAD_DIM), :]
                aT[:, pl.ds(pl.multiple_of(c * qw, qw), qw)] = atv[:, pl.ds(pl.multiple_of(sp * rows, rows), rows)].T
                aT[:, pl.ds(pl.multiple_of(far * qw, qw), qw)] = aob[...].T

                @turns(ntile)
                def _(n):
                    @pl.when(n + nw - 1 < ntile)
                    def _():
                        w_tile(n + nw - 1).start()
                    w_tile(n).wait()
                    cl = pl.ds(pl.multiple_of(n * cw, cw), cw)
                    xo[:, cl] = (xo[:, cl].astype(F32) + jnp.dot(aT[...], wt[n % nw], preferred_element_type=F32)).astype(BF16)
                out = pltpu.make_async_copy(xo, y_o, lq.at[PAIR])
                out.start()
                out.wait()
            pl.run_scoped(products, vm((PAIR, dy_h.shape[0], cw), BF16), vm((TRIO, dm, cw), BF16))
        pl.run_scoped(att_part, vm((qw, dy_h.shape[0]), BF16), vm((qw, rows), BF16), vm((rows, dm), BF16), dma((PAIR * heads,)))
        pl.run_scoped(functools.partial(later, tile, aT, hta, ht_in[0], sem, nslot, give, free), vm((dm - qw, nblk * rows), BF16))

    def later(tile, aT, hta, hta_in, sem, nslot, give, free, htb):
        htb_in = pltpu.make_async_copy(ht_h.at[qw:], htb, lq.at[0])
        htb_in.start()
        nm = dm // qw
        once = jnp.minimum(z + 1, 1)

        def product(rhs_of, cols_of, nr, m, piece):
            free(piece - nslot)


            @turns(once)
            def _(_):
                acc = None
                for r in range(nr):
                    part = dot_nt((hta, htb)[m][:, cols_of(r)], rhs_of(r))
                    acc = part if acc is None else acc + part
                tile[piece % nslot] = acc

        def pair(p, piece, between):
            ha = (z + nz - p) % nz
            hb = jnp.where(p < nz // PAIR, (z + p) % nz, z)
            for m in range(nm):
                product(lambda r: jnp.concatenate([dqa[ha, r], dqa[hb, r]], axis=KEYS), lambda r: span(r, rows), nblk, m, piece + m)
                give([dwq_o.at[span(m, qw), pl.ds(pl.multiple_of(c * qw + h * HEAD_DIM, HEAD_DIM), HEAD_DIM)] for h in (ha, hb)], piece + m)
                if m == 0:
                    between()
        hta_in.wait()
        base = dm // cw
        def small(o):
            return pltpu.make_async_remote_copy(src_ref=sma.at[sp], dst_ref=sma.at[sp], send_sem=ssend.at[0], recv_sem=srecv.at[0],
                                                device_id=(dp, (sp + o) % n_sp), device_id_type=MESH)

        def in_rows(wr, xo, dyo, wkv, dkp, dn):
            ins = [pltpu.make_async_copy(x_h, xo, lq.at[PAIR]), pltpu.make_async_copy(dyo_h, dyo, lq.at[TRIO]),
                   pltpu.make_async_copy(wk_h, wkv.at[0], lq.at[5]), pltpu.make_async_copy(wv_h, wkv.at[1], lq.at[6])]
            for cp in ins:
                cp.start()

            nw = wr.shape[0]

            def w_tile(n):
                return pltpu.make_async_copy(wq_h.at[pl.ds(pl.multiple_of(n * cw, cw), cw)], wr.at[n % nw], sem.at[n % nw])
            for i in range(nw - 1):
                w_tile(i).start()
            dq_give = pltpu.make_async_remote_copy(src_ref=dqa.at[:, other], dst_ref=dqo, send_sem=xsend.at[1], recv_sem=xrecv.at[1], **peer)
            kv_tick(1)
            relay.ticks(PAIR, nblk // PAIR, nblk)
            def own_rows():
                kv_give.wait()
                dq_give.wait()
                for cp in ins:
                    cp.wait()
                for h in range(nz):
                    aT[:, pl.ds(pl.multiple_of(c * qw + h * HEAD_DIM, HEAD_DIM), HEAD_DIM)] = dqa[h, sp].T
                    aT[:, pl.ds(pl.multiple_of(far * qw + h * HEAD_DIM, HEAD_DIM), HEAD_DIM)] = dqo[h].T
                for e in range(PAIR):
                    er = span(e, HEAD_DIM)
                    dkp[e, :, pl.ds(pl.multiple_of(c * HEAD_DIM, HEAD_DIM), HEAD_DIM)] = kva[z, er, pl.ds(pl.multiple_of(c * rows, rows), rows)].T
                    dkp[e, :, pl.ds(pl.multiple_of(far * HEAD_DIM, HEAD_DIM), HEAD_DIM)] = kvo[er, :].T

                @turns(dm // cw)
                def _(n):
                    @pl.when(n + nw - 1 < dm // cw)
                    def _():
                        w_tile(n + nw - 1).start()
                    w_tile(n).wait()
                    rr = pl.ds(pl.multiple_of(n * cw, cw), cw)
                    dn[:, rr] = dot_nt(aT[...], wr[n % nw]) + dot_nt(dkp[0], wkv[0, rr, :]) + dot_nt(dkp[1], wkv[1, rr, :])
                nr = 16
                gain = jnp.concatenate([par[g:g + 1, :] for g in range(dm // HEAD_DIM)], axis=1)

                @turns(rows // nr)
                def _(i):
                    rr = pl.ds(pl.multiple_of(i * nr, nr), nr)
                    xf = xo[rr, :].astype(F32)
                    inv = lax.rsqrt(jnp.mean(xf * xf, axis=-1, keepdims=YES) + NORM_EPS)
                    unit = xf * inv
                    g = dn[rr, :]
                    du = g * gain
                    di = inv * (du - unit * jnp.mean(du * unit, axis=-1, keepdims=YES))
                    xo[rr, :] = (dyo[rr, :].astype(F32) + di).astype(BF16)
                    dn[rr, :] = g * unit
                tot = jnp.sum(dn[...], axis=KEYS, keepdims=YES)
                for j in range(dm // HEAD_DIM):
                    sma[sp, j:j + 1, :] = tot[:, span(j, HEAD_DIM)]
                pltpu.make_async_copy(xo, dx_o, lq.at[PAIR]).start()

                @pl.loop(1, n_sp)
                def _(o):
                    small(o).start()

            @turns(nz // PAIR)
            def _(q):
                @pl.when(q == PAIR)
                def _():
                    kv_tick(PAIR)

                @pl.when(q == TRIO)
                def _():
                    relay.ticks(TRIO, 0, nblk)
                    dq_give.start()
                    own_rows()

                def between():
                    @pl.when(q == 0)
                    def _():
                        htb_in.wait()
                pair(q + 1, base + q * nm, between)
            pltpu.make_async_copy(xo, dx_o, lq.at[PAIR]).wait()
        pl.run_scoped(in_rows, vm((QUAD, cw, dm), BF16), vm((rows, dm), BF16), vm((rows, dm), BF16), vm((PAIR, dm, cw), BF16),
                      vm((PAIR, rows, cw), BF16), vm((rows, dm), F32))

        kv_tick(TRIO)
        kv_out = pltpu.make_async_copy(kva, kv_o, lq.at[0])
        kv_out.start()
        npiece = base + QUAD * nm
        for i in range(nslot):
            free(npiece - nslot + i)

        pltpu.make_async_copy(dwo_o, dwo_o, trecv.at[0]).wait()
        pltpu.make_async_copy(kvf_o, kvf_o, trecv.at[1]).wait()
        pltpu.make_async_copy(kvf_o, kvf_o, tsend.at[0, PAIR]).wait()
        kv_out.wait()
        ref = sma.at[pl.ds(0, n_sp - 1)]
        pltpu.make_async_copy(ref, ref, ssend.at[0]).wait()
        pltpu.make_async_copy(ref, ref, srecv.at[0]).wait()
        ng = dm // HEAD_DIM
        tot = sma[0, 0:ng, :]
        for o in range(1, n_sp):
            tot = tot + sma[o, 0:ng, :]
        smo[0:ng, :] = tot
        for cc in range(PAIR):
            for zz in range(nz):
                smo[ng + cc * nz + zz:ng + cc * nz + zz + 1, :] = sma[zz * PAIR + cc, 16:17, :]
            for e in range(PAIR):
                tot = sma[cc, 17 + e:18 + e, :]
                for zz in range(1, nz):
                    tot = tot + sma[zz * PAIR + cc, 17 + e:18 + e, :]
                smo[PAIR * ng + PAIR * e + cc:PAIR * ng + PAIR * e + cc + 1, :] = tot
        out = pltpu.make_async_copy(smo, small_o, lq.at[PAIR])
        out.start()
        out.wait()
    pl.run_scoped(late, vm((TRIO, qw, cw), F32), vm((rows, dm), BF16), vm((qw, nblk * rows), BF16), dma((6,)))
    relay.finish(ht_h.at[0:7 * HEAD_DIM // PAIR, :])
    kvr.finish(dy_h.at[0:7 * HEAD_DIM * bk // dm, :])
    for d in range(PAIR):
        pltpu.make_async_copy(rs.at[d], rs.at[d], rsend.at[d]).wait()


def k3(n_sp, x, dy_own, par, qt, at, ao, lse, k, kt, v, vt, cs, ht, dyf, wq, wk, wv, wo):
    rows, dm = x.shape
    nblk, seq, nz = qt.shape[0], k.shape[0], n_sp // PAIR
    heads = qt.shape[PAIR] // rows
    npiece = dm // (PAIR * HEAD_DIM) + 5 * (dm // (heads * HEAD_DIM))
    sds, vm, dma = jax.ShapeDtypeStruct, pltpu.VMEM, pltpu.SemaphoreType.DMA
    ns = PAIR * (dm // HEAD_DIM) + 8
    scratch = [vm((seq, PAIR * HEAD_DIM), BF16), vm((HEAD_DIM, seq), BF16), vm((heads * HEAD_DIM - at.shape[0], rows), BF16), vm((HEAD_DIM, seq), F32), vm((seq, HEAD_DIM), F32), vm((seq, HEAD_DIM), F32), vm((nz, nblk, HEAD_DIM, rows), BF16), vm((nz, HEAD_DIM, rows), BF16),
               vm((PAIR, nz - 1, PAIR * rows, HEAD_DIM), F32), vm((nz, PAIR * HEAD_DIM, PAIR * rows), BF16), vm((PAIR * HEAD_DIM, rows), BF16), vm((n_sp, 24, HEAD_DIM), F32), vm((ns, HEAD_DIM), F32),
               dma((PAIR,)), dma((PAIR, QUAD * nblk)), dma((PAIR,)), dma((PAIR, nz - 1)), dma((PAIR,)), dma((PAIR, 8)), dma((5,)), dma((5,)),
               dma((1,)), dma((1,)), dma((QUAD, TRIO)), dma((PAIR,)), dma((QUAD, PAIR)), dma((8,))]
    outs = [sds((rows, dm), BF16), sds((rows, dm), BF16), sds(wq.shape, F32), sds(wo.shape, F32), sds((ns, HEAD_DIM), F32)] + [sds((nz, PAIR * HEAD_DIM, PAIR * rows), BF16)] * PAIR
    return pl.pallas_call(
        functools.partial(k3_kernel, nblk // PAIR, rows, (nz, n_sp, heads)), out_shape=outs, in_specs=[ANY, ANY, VM] + [ANY] * 15, out_specs=[ANY] * len(outs),
        scratch_shapes=scratch, compiler_params=pltpu.CompilerParams(collective_id=PAIR, has_side_effects=YES, vmem_limit_bytes=63 * MIB),
        name='attend_back')(x, dy_own, par, qt, at, ao, lse, k, kt, v, vt, cs, ht, dyf, wq, wk, wv, wo)


def k4_kernel(y_h, dx_h, dwq_h, dwo_h, small, kv_h, kvf_h, ht_h, y_o, dx_o, dwq_o, dwk_o, dwv_o, dwo_o, g_o, bq_o, bk_o, bv_o,
              buf, hbuf, kv, hts, wt, isem, osem, hsem, wsem, ksem):
    nslot, half = buf.shape[0], buf.shape[0]
    dm, rc = dwq_h.shape[0], buf.shape[1]
    c = lax.axis_index('sp') % PAIR
    for i, (src, dst) in enumerate(((y_h, y_o), (dx_h, dx_o))):
        pltpu.make_async_copy(src, hbuf.at[i], hsem.at[i]).start()
    kin = [pltpu.make_async_copy(kv_h, kv.at[c], ksem.at[0]), pltpu.make_async_copy(kvf_h, kv.at[1 - c], ksem.at[1])]
    for cp in kin:
        cp.start()
    ng = dm // HEAD_DIM
    g_o[...] = small[0:ng, :]
    bq_o[...] = small[ng:PAIR * ng, :]
    bk_o[...] = small[PAIR * ng:PAIR * ng + PAIR, :]
    bv_o[...] = small[PAIR * ng + PAIR:PAIR * ng + QUAD, :]
    n = dm // rc
    work = [(src, dst, i) for i in range(n) for src, dst in ((dwq_h, dwq_o), (dwo_h, dwo_o))]

    def into(i):
        return pltpu.make_async_copy(work[i][0].at[pl.ds(work[i][PAIR] * rc, rc)], buf.at[i % nslot], isem.at[i % nslot])

    def out(i):
        return pltpu.make_async_copy(buf.at[i % nslot], work[i][1].at[pl.ds(work[i][PAIR] * rc, rc)], osem.at[i % nslot])
    mr = hts.shape[1]

    def ht_in(m):
        return pltpu.make_async_copy(ht_h.at[pl.ds(pl.multiple_of(m * mr, mr), mr)], hts.at[m % PAIR], wsem.at[m % PAIR])

    def w_out(m):
        return [pltpu.make_async_copy(wt.at[m % PAIR, e], d.at[pl.ds(pl.multiple_of(m * mr, mr), mr)], wsem.at[PAIR + PAIR * e + m % PAIR]) for e, d in enumerate((dwk_o, dwv_o))]
    for i in range(half):
        into(i).start()
    ht_in(0).start()
    for cp in kin:
        cp.wait()
    steps = dm // mr
    per = len(work) // steps
    for m in range(steps):
        if m + 1 < steps:
            ht_in(m + 1).start()
        for i in range(m * per, (m + 1) * per):
            into(i).wait()
            out(i).start()
            if i >= half:
                out(i - half).wait()
            if i + half < len(work):
                into(i + half).start()
        ht_in(m).wait()
        if m >= PAIR:
            for cp in w_out(m - PAIR):
                cp.wait()

        @turns(PAIR)
        def _(p):
            acc = None
            w = kv.shape[TRIO]
            for o in range(kv.shape[1]):
                part = dot_nt(hts[m % PAIR, :, span(o, w)], kv[p, o])
                acc = part if acc is None else acc + part
            cols = pl.ds(pl.multiple_of(p * HEAD_DIM, HEAD_DIM), HEAD_DIM)
            for e in range(PAIR):
                wt[m % PAIR, e, :, cols] = acc[:, span(e, HEAD_DIM)]
        for cp in w_out(m):
            cp.start()
    for i, (src, dst) in enumerate(((y_h, y_o), (dx_h, dx_o))):
        pltpu.make_async_copy(src, hbuf.at[i], hsem.at[i]).wait()
        pltpu.make_async_copy(hbuf.at[i], dst, hsem.at[PAIR + i]).start()
    for i in range(len(work) - half, len(work)):
        out(i).wait()
    for m in (steps - PAIR, steps - 1):
        for cp in w_out(m):
            cp.wait()
    for i, (src, dst) in enumerate(((y_h, y_o), (dx_h, dx_o))):
        pltpu.make_async_copy(hbuf.at[i], dst, hsem.at[PAIR + i]).wait()


def k4(y, dx, dwq, dwo, small, kv, kvf, ht):
    dm, ng = dwq.shape[0], dwq.shape[0] // HEAD_DIM
    sds, vm, dma = jax.ShapeDtypeStruct, pltpu.VMEM, pltpu.SemaphoreType.DMA
    wide = PAIR * HEAD_DIM
    outs = [sds(y.shape, BF16), sds(dx.shape, BF16), sds(dwq.shape, F32), sds((dm, wide), F32), sds((dm, wide), F32), sds(dwo.shape, F32),
            sds((ng, HEAD_DIM), F32), sds((ng, HEAD_DIM), F32), sds((PAIR, HEAD_DIM), F32), sds((PAIR, HEAD_DIM), F32)]
    return pl.pallas_call(
        k4_kernel, out_shape=outs, in_specs=[ANY] * QUAD + [VM] + [ANY] * TRIO, out_specs=[ANY] * 6 + [VM] * QUAD,
        scratch_shapes=[vm((16, 256, dwq.shape[1]), F32), vm((PAIR,) + y.shape, BF16), vm((PAIR,) + kv.shape, BF16), vm((PAIR, dm // QUAD, ht.shape[1]), BF16),
                        vm((PAIR, PAIR, dm // QUAD, wide), F32), dma((16,)), dma((16,)), dma((QUAD,)), dma((6,)), dma((PAIR,))],
        compiler_params=pltpu.CompilerParams(vmem_limit_bytes=60 * MIB), name='place')(y, dx, dwq, dwo, small, kv, kvf, ht)


def solution(mesh):
    n_sp = mesh.shape['sp']

    def step(hidden, d_out, positions, norm_gain, w_query, b_query, w_key, b_key, w_value, b_value, w_out):
        x, dy = hidden[0], d_out[0]
        rows, dm = x.shape
        par = jnp.concatenate([b.astype(F32).reshape(-1, HEAD_DIM) for b in (norm_gain, b_query, b_key, b_value)])
        hf, ht, qt, k, kt, v, vt, cs = k1(n_sp, x, positions, par, w_query, w_key, w_value)
        dyf, at, lse, ao = k2(n_sp, dy, qt, k, vt)
        y, dx, dwq, dwo, small, kv, kvf = k3(n_sp, x, dy, par, qt, at, ao, lse, k, kt, v, vt, cs, ht, dyf, w_query, w_key, w_value, w_out)
        y, dx, dwq, dwk, dwv, dwo, dg, dbq, dbk, dbv = k4(y, dx, dwq, dwo, small, kv, kvf, ht)
        return y[None], dx[None], dg.reshape(-1), dwq, dbq.reshape(-1), dwk, dbk.reshape(-1), dwv, dbv.reshape(-1), dwo

    seq_spec = P('dp', 'sp', None)
    in_specs = (seq_spec, seq_spec, P('dp', 'sp')) + (P(),) * 8
    out_specs = (seq_spec, seq_spec, P('dp'), P('dp', None), P('dp'), P('dp', None), P('dp'), P('dp', None), P('dp'), P('dp', None))
    return jax.shard_map(step, mesh=mesh, in_specs=in_specs, out_specs=out_specs, check_vma=False)
```

```python
import functools, math
import jax
import jax.numpy as jnp
from jax import lax
from jax.experimental import pallas as pl
from jax.experimental.pallas import tpu as pltpu
from jax.sharding import PartitionSpec as P

HEAD_DIM = 128
ROPE_BASE = 1000000.0
NORM_EPS = 1e-6
MESH = pl.DeviceIdType.MESH
PAIR, TRIO, QUAD, OCTET = 2, 3, 4, 8
TOP = slice(0, 1)
KEYS = 0
YES = True
MIB = 1 << 20
NSUB = PAIR
SCALE = HEAD_DIM ** -0.5
F32 = jnp.float32
BF16 = jnp.bfloat16
ANY = pl.BlockSpec(memory_space=pl.ANY)
VM = pl.BlockSpec(memory_space=pltpu.VMEM)


def span(i, n):
    return slice(i * n, (i + 1) * n)


def turns(n):
    return pl.loop(0, n)


class Ring:
    def __init__(self, full, own, rows, nz, sems):
        self.full, self.own, self.rows, self.nz = full, own, rows, nz
        self.send, self.recv, self.drecv = sems
        self.sp = lax.axis_index('sp')
        self.dp = lax.axis_index('dp')
        self.z, self.c = self.sp // PAIR, self.sp % PAIR
        self.sub = rows // (PAIR * NSUB)
        self.nsend = 7 * NSUB

    def dev(self, z, c):
        return (self.dp, z * PAIR + c)

    def where(self, d, j, z):
        s = j // (PAIR * NSUB)
        r = j % (PAIR * NSUB)
        half = (r // NSUB + d) % PAIR
        origin = (z + (self.nz - s if d == 0 else s)) % self.nz
        return pl.multiple_of((origin * PAIR + self.c) * self.rows + half * (self.rows // PAIR) + (r % NSUB) * self.sub, self.sub)

    def ici(self, d, j, src=None):
        off = self.where(d, j, self.z)
        to = (self.z + (1 if d == 0 else self.nz - 1)) % self.nz
        return pltpu.make_async_remote_copy(
            src_ref=self.full.at[pl.ds(off, self.sub)] if src is None else src,
            dst_ref=self.full.at[pl.ds(off, self.sub)],
            send_sem=self.send.at[d], recv_sem=self.recv.at[d, j],
            device_id=self.dev(to, self.c), device_id_type=MESH)

    def d2d(self, d, j):
        frm = (self.z + (self.nz - 1 if d == 0 else 1)) % self.nz
        off = self.where(d, j, frm)
        return pltpu.make_async_remote_copy(
            src_ref=self.full.at[pl.ds(off, self.sub)], dst_ref=self.full.at[pl.ds(off, self.sub)],
            send_sem=self.send.at[PAIR], recv_sem=self.drecv.at[j // (PAIR * NSUB)],
            device_id=self.dev(self.z, 1 - self.c), device_id_type=MESH)

    def d2d_own(self):
        off = pl.multiple_of(self.sp * self.rows, self.rows)
        return pltpu.make_async_remote_copy(
            src_ref=self.own, dst_ref=self.full.at[pl.ds(off, self.rows)],
            send_sem=self.send.at[TRIO], recv_sem=self.drecv.at[QUAD],
            device_id=self.dev(self.z, 1 - self.c), device_id_type=MESH)

    def start(self):
        @turns(PAIR * NSUB)
        def _(j):
            for d in range(PAIR):
                half = (j // NSUB + d) % PAIR
                off = pl.multiple_of(half * (self.rows // PAIR) + (j % NSUB) * self.sub, self.sub)
                self.ici(d, j, self.own.at[pl.ds(off, self.sub)]).start()
        self.d2d_own().start()

    def tick(self, j):
        for d in range(PAIR):
            self.ici(d, j).wait_recv()

            @pl.when(j + PAIR * NSUB < self.nsend)
            def _():
                self.ici(d, j + PAIR * NSUB).start()
            self.d2d(d, j).start()

    def total(self, rows, sem):
        ref = self.full.at[pl.ds(0, rows)]
        pltpu.make_async_copy(ref, ref, sem).wait()

    def finish_sends(self):
        each = self.nsend * self.sub
        self.total(each, self.send.at[0])
        self.total(each, self.send.at[1])
        self.total(PAIR * each, self.send.at[PAIR])
        self.d2d_own().wait_send()

    def wait_other(self, s):
        self.total(self.rows if s == TRIO else PAIR * self.rows, self.drecv.at[s])


def ring_sems(nz):
    return [pltpu.SemaphoreType.DMA((QUAD,)), pltpu.SemaphoreType.DMA((PAIR, 7 * NSUB)), pltpu.SemaphoreType.DMA((5,))]


def greet_all(n_sp):
    sp, dp = lax.axis_index('sp'), lax.axis_index('dp')
    bar = pltpu.get_barrier_semaphore()

    @pl.loop(1, n_sp)
    def _(o):
        pl.semaphore_signal(bar, inc=1, device_id=(dp, (sp + o) % n_sp), device_id_type=MESH)

    def all_here():
        pl.semaphore_wait(bar, n_sp - 1)
    return all_here


def greet(peers):
    bar = pltpu.get_barrier_semaphore()
    for p in peers:
        pl.semaphore_signal(bar, inc=1, device_id=p, device_id_type=MESH)
    pl.semaphore_wait(bar, len(peers))


def k1_kernel(n_sp, x_h, pos, par, wq, wk, wv, hf, ht, qt, k_o, kt_o, v_o, vt_o, cs_o, q2_o,
              pos_all, wq_v, wk_v, wv_v, hb, htb, qs, ks, kts, vs, vts, cst, q2s, send, recv, drecv, psend, precv, lsem, wsem, osem):
    nz = n_sp // PAIR
    rows, dm = x_h.shape
    qw = wq_v.shape[1]
    sp, dp = lax.axis_index('sp'), lax.axis_index('dp')
    z, c = sp // PAIR, sp % PAIR
    far = 1 - c
    heads = qw // HEAD_DIM
    half_dim = HEAD_DIM // PAIR
    ng = dm // HEAD_DIM
    mine = pl.ds(pl.multiple_of(sp * rows, rows), rows)
    ring = Ring(hf, hf.at[mine], rows, nz, (send, recv, drecv))
    x_in = pltpu.make_async_copy(x_h, hb, lsem.at[0])
    x_in.start()
    all_here = greet_all(n_sp)
    pos_copy = pltpu.make_async_copy(pos, pos_all.at[sp], lsem.at[1])
    pos_copy.start()

    def head_of(g):
        return (z + g) % heads

    wcopies = [pltpu.make_async_copy(wq.at[:, pl.ds(pl.multiple_of(c * qw + head_of(g) * HEAD_DIM, HEAD_DIM), HEAD_DIM)],
                                     wq_v.at[:, span(g, HEAD_DIM)], wsem.at[g]) for g in range(heads)]
    cols = pl.ds(pl.multiple_of(c * HEAD_DIM, HEAD_DIM), HEAD_DIM)
    wcopies += [pltpu.make_async_copy(wk.at[:, cols], wk_v, lsem.at[PAIR]), pltpu.make_async_copy(wv.at[:, cols], wv_v, lsem.at[TRIO])]
    for w in wcopies:
        w.start()
    x_in.wait()
    gain = jnp.concatenate([par[g:g + 1, :] for g in range(ng)], axis=1)
    nr = 16

    @turns(rows // nr)
    def _(i):
        rr = pl.ds(pl.multiple_of(i * nr, nr), nr)
        xf = hb[rr, :].astype(F32)
        inv = lax.rsqrt(jnp.mean(xf * xf, axis=-1, keepdims=YES) + NORM_EPS)
        hb[rr, :] = (xf * inv * gain).astype(BF16)
    own_out = pltpu.make_async_copy(hb, hf.at[mine], lsem.at[0])
    own_out.start()
    all_here()

    def pos_send(o):
        return pltpu.make_async_remote_copy(src_ref=pos, dst_ref=pos_all.at[sp], send_sem=psend.at[0], recv_sem=precv.at[0],
                                            device_id=(dp, (sp + o) % n_sp), device_id_type=MESH)

    @pl.loop(1, n_sp)
    def _(o):
        pos_send(o).start()
    own_out.wait()
    ring.start()
    for w in wcopies:
        w.wait()
    pos_copy.wait()
    others = pos_all.at[pl.ds(0, n_sp - 1)]
    pltpu.make_async_copy(others, others, psend.at[0]).wait()
    pltpu.make_async_copy(others, others, precv.at[0]).wait()

    freq = jnp.exp(lax.broadcasted_iota(jnp.int32, (half_dim, 1), 0).astype(F32) * (-2.0 / HEAD_DIM * math.log(ROPE_BASE)))

    def outs(blk):
        cols = pl.ds(pl.multiple_of(blk * rows, rows), rows)
        return [pltpu.make_async_copy(htb, ht.at[:, cols], osem.at[0]),
                pltpu.make_async_copy(qs, qt.at[blk], osem.at[1]),
                pltpu.make_async_copy(ks, k_o.at[cols], osem.at[PAIR]),
                pltpu.make_async_copy(kts, kt_o.at[:, cols], osem.at[TRIO]),
                pltpu.make_async_copy(vs, v_o.at[cols], osem.at[QUAD]),
                pltpu.make_async_copy(vts, vt_o.at[:, cols], osem.at[5]),
                pltpu.make_async_copy(q2s, q2_o.at[blk], osem.at[6])]

    def table(blk):
        cols = pl.ds(pl.multiple_of(blk * rows, rows), rows)
        ang = freq * pos_all[blk].astype(F32)
        cst[0:half_dim, cols] = jnp.cos(ang)
        cst[half_dim:, cols] = jnp.sin(ang)

    def compute(n, blk):
        load = pltpu.make_async_copy(hf.at[pl.ds(pl.multiple_of(blk * rows, rows), rows)], hb, lsem.at[0])
        load.start()
        load.wait()
        @pl.when(n > 0)
        def _():
            for o in outs(blk):
                o.wait()
        cols = pl.ds(pl.multiple_of(blk * rows, rows), rows)
        cos, sin = cst[0:half_dim, cols], cst[half_dim:, cols]
        h = hb[...]
        htb[...] = h.T

        def rope_t(t):
            a, b = t[:half_dim], t[half_dim:]
            return jnp.concatenate([a * cos - b * sin, b * cos + a * sin], axis=KEYS)
        for g in range(heads // PAIR):
            cols = slice(g * PAIR * HEAD_DIM, (g + 1) * PAIR * HEAD_DIM)
            bias = jnp.concatenate([par[pl.ds(ng + c * heads + head_of(g * PAIR + e), 1), :] for e in range(PAIR)], axis=1)
            q = jnp.dot(h, wq_v[:, cols], preferred_element_type=F32) + bias
            t = q.T
            for e in range(PAIR):
                hd = g * PAIR + e
                r = rope_t(t[span(e, HEAD_DIM)]).astype(BF16)
                qs[:, span(hd, rows)] = r
                q2s[:, span(hd, rows)] = split_scaled(r, LOG2E * SCALE)
        k = jnp.dot(h, wk_v[...], preferred_element_type=F32) + par[pl.ds(PAIR * ng + c, 1), :]
        kt = rope_t(k.T)
        kts[...] = kt.astype(BF16)
        ks[...] = kt.T.astype(BF16)
        v = jnp.dot(h, wv_v[...], preferred_element_type=F32) + par[pl.ds(PAIR * ng + PAIR + c, 1), :]
        vs[...] = v.astype(BF16)
        vts[...] = v.T.astype(BF16)
        for o in outs(blk):
            o.start()

    table_out = pltpu.make_async_copy(cst, cs_o, osem.at[7])
    table(sp)
    table(z * PAIR + 1 - c)

    @turns(n_sp)
    def _(n):
        m = n - PAIR
        s = m // QUAD
        b = jnp.where(s == TRIO, (m % QUAD) * PAIR, m % QUAD)
        other = jnp.where(n < PAIR, n, b // PAIR)
        left = b % PAIR == 0
        dist = jnp.where(n < PAIR, 0, s + 1)

        @pl.when((n >= PAIR) & (m % QUAD == 0))
        def _():
            @turns(jnp.where(s == TRIO, NSUB, PAIR * NSUB))
            def _(r):
                ring.tick(s * PAIR * NSUB + r)

        @pl.when(n == 1)
        def _():
            ring.d2d_own().wait_recv()

        for h in range(QUAD):
            @pl.when((n >= PAIR) & (other == 1) & left & (s == h))
            def _():
                ring.wait_other(h)
        zb = (z + jnp.where(left, nz - dist, dist)) % nz
        cb = jnp.where(other == 1, 1 - c, c)
        compute(n, zb * PAIR + cb)

        @pl.when(n == 1)
        def _():
            pl.loop(0, n_sp)(table)
            table_out.start()
    for o in outs(0):
        o.wait()
    table_out.wait()
    ring.finish_sends()


def k1(n_sp, x, pos, par, wq, wk, wv):
    rows, dm = x.shape
    seq = rows * n_sp
    nz = n_sp // PAIR
    qw = wq.shape[1] // PAIR
    heads = qw // HEAD_DIM
    sds = jax.ShapeDtypeStruct
    outs = [sds((seq, dm), BF16), sds((dm, seq), BF16), sds((n_sp, HEAD_DIM, heads * rows), BF16),
            sds((seq, HEAD_DIM), BF16), sds((HEAD_DIM, seq), BF16), sds((seq, HEAD_DIM), BF16), sds((HEAD_DIM, seq), BF16),
            sds((HEAD_DIM, seq), F32), sds((n_sp, PAIR * HEAD_DIM, heads * rows), BF16)]
    vm, dma = pltpu.VMEM, pltpu.SemaphoreType.DMA
    scratch = [vm((n_sp,) + pos.shape, jnp.int32), vm((dm, qw), BF16), vm((dm, HEAD_DIM), BF16), vm((dm, HEAD_DIM), BF16),
               vm((rows, dm), BF16), vm((dm, rows), BF16), vm((HEAD_DIM, heads * rows), BF16),
               vm((rows, HEAD_DIM), BF16), vm((HEAD_DIM, rows), BF16), vm((rows, HEAD_DIM), BF16), vm((HEAD_DIM, rows), BF16),
               vm((HEAD_DIM, seq), F32), vm((PAIR * HEAD_DIM, heads * rows), BF16)] + ring_sems(nz) + [dma((1,)), dma((1,)), dma((QUAD,)), dma((heads,)), dma((OCTET,))]
    return pl.pallas_call(
        functools.partial(k1_kernel, n_sp), out_shape=outs,
        in_specs=[ANY, ANY, VM, ANY, ANY, ANY], out_specs=[ANY] * len(outs), scratch_shapes=scratch,
        compiler_params=pltpu.CompilerParams(collective_id=0, has_side_effects=YES, vmem_limit_bytes=60 * MIB),
        name='gather_project')(x, pos, par, wq, wk, wv)


LOG2E = math.log2(math.e)
NEG = -1e30

def split_scaled(q, scale):
    qs = q.astype(F32) * scale
    hi = qs.astype(BF16)
    lo = (qs - hi.astype(F32)).astype(BF16)
    return jnp.concatenate([hi, lo], axis=KEYS)

def decode(n, nblk):
    one = int if isinstance(n, int) else (lambda x: x.astype(jnp.int32))
    j = sum(one(n >= i * (i + 1)) for i in range(1, nblk // PAIR))
    r = n - j * (j + 1)
    odd = one(r > j)
    return PAIR * j + odd, r - odd * (j + 1)

def fwd_steps(nblk):
    return (nblk // PAIR) * (nblk // PAIR + 1)

def decode_up(n, nq):
    one = int if isinstance(n, int) else (lambda x: x.astype(jnp.int32))
    i = sum(one(n >= m * (m + 1) // PAIR) for m in range(1, nq))
    return i, n - i * (i + 1) // PAIR


def causal_bias(bias, bk, rows):
    d = lax.broadcasted_iota(jnp.int32, (bk, rows), 0) - lax.broadcasted_iota(jnp.int32, (bk, rows), 1)
    bias[0] = jnp.zeros((bk, rows), F32)
    bias[1] = jnp.where(d <= 0, 0.0, NEG)
    bias[PAIR] = jnp.where(d <= rows, 0.0, NEG)


class Fwd:
    def __init__(self, nblk, rows, heads, first, wide, q2h, sink, lse, kk, vt, q2, acc, mx, cm, ls, al, rt, lsv, sb, pb, bias, qsem, osem):
        self.__dict__.update(locals())
        self.bk = PAIR * rows
        self.groups = heads * wide
        self.cols = [span(u, rows) for u in range(self.groups)]
        self.halves = (range(0, self.groups // PAIR), range(self.groups // PAIR, self.groups))
        self.nq = nblk // wide
        self.nstep = fwd_steps(nblk) if wide == 1 else self.nq * (self.nq + 1) // PAIR

    def where(self, n):
        if self.wide == 1:
            i, t = decode(n, self.nblk)
            return i, t, t == i // PAIR
        i, t = decode_up(n, self.nq)
        return i, t, t == i

    def load_q(self, i):
        w = self.heads * self.rows
        src = slice(self.first * self.rows, self.first * self.rows + w)
        return [pltpu.make_async_copy(self.q2h.at[self.wide * i + e, :, src], self.q2.at[i % PAIR, :, span(e, w)], self.qsem.at[i % PAIR, e])
                for e in range(self.wide)]

    def prepare(self):
        for cp in self.load_q(0) + self.load_q(1):
            cp.start()
        causal_bias(self.bias, self.bk, self.rows)
        self.acc[...] = jnp.zeros_like(self.acc)
        self.pb[...] = jnp.zeros_like(self.pb)
        self.ls[...] = jnp.zeros_like(self.ls)
        self.al[...] = jnp.zeros_like(self.al)
        self.mx[...] = jnp.zeros_like(self.mx)
        for cp in self.load_q(0) + self.load_q(1):
            cp.wait()
        self.scores(0, 0, YES)

    def keys(self, t):
        return pl.ds(pl.multiple_of(t * self.bk, self.bk), self.bk)

    def scores(self, n, part, masked):
        i, t, last = self.where(n)
        kb = self.kk[self.keys(t), :]
        for u in self.halves[part]:
            kind = jnp.where(last, 1 + (i % PAIR if self.wide == 1 else u // self.heads), 0)
            s = jnp.dot(kb, self.q2[i % PAIR, :, self.cols[u]], preferred_element_type=F32)
            if masked:
                s = s + self.bias[kind]
            self.sb[u] = s
            self.cm[:, self.cols[u]] = jnp.max(s.reshape(self.bk // OCTET, OCTET, self.rows), axis=KEYS)

    def soft(self, n, part):
        i, t, last = self.where(n)
        for u in self.halves[part]:
            c = self.cols[u]
            m0 = jnp.where(t == 0, NEG, self.mx[TOP, c])
            m1 = jnp.maximum(m0, jnp.max(self.cm[:, c], axis=KEYS, keepdims=YES))
            p = jnp.exp2(self.sb[u] - m1)
            a = jnp.exp2(m0 - m1)
            self.mx[TOP, c] = m1
            self.al[TOP, c] = a
            self.ls[:, c] = self.ls[:, c] * a + jnp.sum(p.reshape(self.bk // OCTET, OCTET, self.rows), axis=KEYS)
            self.pb[u] = p.astype(BF16)

    def values(self, n, part):
        i, t, last = self.where(n)
        vb = self.vt[:, self.keys(t)]
        for u in self.halves[part]:
            c = self.cols[u]
            self.acc[:, c] = self.acc[:, c] * self.al[TOP, c] + jnp.dot(vb, self.pb[u], preferred_element_type=F32)

    def out_lse(self, i):
        return pltpu.make_async_copy(self.lsv, self.lse.at[i], self.osem)

    def finish(self, i, part):
        self.sink.before(i, part)
        for u in self.halves[part]:
            c = self.cols[u]
            self.sink.store(u % self.heads, self.wide * i + u // self.heads, (self.acc[:, c] * self.rt[TOP, c]).astype(BF16))
        self.sink.after(i, part)

    def end_block(self, i):
        tot = jnp.sum(self.ls[...], axis=KEYS, keepdims=YES)
        self.rt[TOP, :] = 1.0 / tot
        if self.lse is not None:
            @pl.when(i > 0)
            def _():
                self.out_lse(i).wait()
            self.lsv[TOP, :] = self.mx[TOP, :] + jnp.log2(tot)
            self.out_lse(i).start()
        self.finish(i, 0)

        @pl.when(i + PAIR < self.nq)
        def _():
            for cp in self.load_q(i + PAIR):
                cp.start()

    def step(self, n, masked):
        n1 = jnp.minimum(n + 1, self.nstep - 1)
        self.scores(n, 1, masked)
        self.soft(n, 0)
        self.values(jnp.maximum(n - 1, 0), 1)
        self.scores(n1, 0, masked)
        self.soft(n, 1)
        self.values(n, 0)

    def run(self, on_step):
        @turns(self.nstep)
        def _(n):
            on_step(n)
            i, t, last = self.where(n)

            @pl.when(last & (i > 0) & (i + 1 < self.nq))
            def _():
                for cp in self.load_q(i + 1):
                    cp.wait()
            if self.wide == 1:
                self.step(n, YES)
            else:
                masked = last | self.where(n + 1)[PAIR]

                @pl.when(masked)
                def _():
                    self.step(n, YES)

                @pl.when(jnp.logical_not(masked))
                def _():
                    self.step(n, False)

            @pl.when((t == 0) & (n > 0))
            def _():
                self.finish(i - 1, 1)

            @pl.when(last)
            def _():
                self.end_block(i)

    def drain(self):
        self.values(self.nstep - 1, 1)
        self.finish(self.nq - 1, 1)
        if self.lse is not None:
            self.out_lse(self.nq - 1).wait()


def fwd_scratch(nblk, rows, groups, wide):
    vm = pltpu.VMEM
    w, bk = groups * rows, PAIR * rows
    return [vm((PAIR, PAIR * HEAD_DIM, w), BF16), vm((HEAD_DIM, w), F32)] + [vm((OCTET, w), F32)] * 6 + [
            vm((groups, bk, rows), F32), vm((groups, bk, rows), BF16), vm((TRIO, bk, rows), F32),
            pltpu.SemaphoreType.DMA((PAIR, wide)), pltpu.SemaphoreType.DMA]


NT = (((1,), (1,)), ((), ()))

def dot_nt(a, b):
    return lax.dot_general(a, b, NT, preferred_element_type=F32)

def bwd_steps(nq):
    return nq * (nq + 1) // PAIR

class Bwd:
    def __init__(self, nq, rows, qt, q2h, kk, kt, vv, dat, dlt, lsv, qb, q2, cs, dk, dv, dq, dbq, sb, dpb, pb, dsb, bias, dqs, psem):
        self.__dict__.update(locals())
        self.bk = PAIR * rows
        self.nstep = bwd_steps(nq)
        self.cols = [slice(0, rows), slice(rows, PAIR * rows)]

    def loads(self, i):
        slot = i % PAIR
        return [pltpu.make_async_copy(self.qt.at[PAIR * i + e, :, 0:self.rows], self.qb.at[slot, :, self.cols[e]], self.psem.at[slot, e]) for e in range(PAIR)] + [
            pltpu.make_async_copy(self.q2h.at[PAIR * i + e, :, 0:self.rows], self.q2.at[slot, :, self.cols[e]], self.psem.at[slot, PAIR + e]) for e in range(PAIR)]

    def clear(self):
        for cp in self.loads(0) + self.loads(1):
            cp.start()
        causal_bias(self.bias, self.bk, self.rows)
        self.dk[...] = jnp.zeros_like(self.dk)
        self.dv[...] = jnp.zeros_like(self.dv)
        self.dq[...] = jnp.zeros_like(self.dq)
        self.dbq[...] = jnp.zeros_like(self.dbq)
        self.pb[...] = jnp.zeros_like(self.pb)
        self.dsb[...] = jnp.zeros_like(self.dsb)

    def prepare(self):
        for cp in self.loads(0) + self.loads(1):
            cp.wait()
        self.scores(0, 0)

    def keys(self, t):
        return pl.ds(pl.multiple_of(t * self.bk, self.bk), self.bk)

    def qcols(self, i, e):
        return pl.ds(pl.multiple_of(i * self.bk + e * self.rows, self.rows), self.rows)

    def scores(self, n, e):
        i, t = decode_up(n, self.nq)
        kind = jnp.where(t == i, 1 + e, 0)
        s = jnp.dot(self.kk[self.keys(t), :], self.q2[i % PAIR, :, self.cols[e]], preferred_element_type=F32)
        self.sb[e] = s + self.bias[kind]
        self.dpb[e] = jnp.dot(self.vv[self.keys(t), :], self.dat[:, self.qcols(i, e)], preferred_element_type=F32)

    def soft(self, n, e):
        i, t = decode_up(n, self.nq)
        c = self.qcols(i, e)
        p = jnp.exp2(self.sb[e] - self.lsv[TOP, c])
        self.pb[e] = p.astype(BF16)
        self.dsb[e] = (p * (self.dpb[e] - self.dlt[TOP, c])).astype(BF16)

    def grads(self, n, e):
        i, t = decode_up(n, self.nq)
        r = self.keys(t)
        self.dv[r, :] += dot_nt(self.pb[e], self.dat[:, self.qcols(i, e)])
        self.dk[r, :] += dot_nt(self.dsb[e], self.qb[i % PAIR, :, self.cols[e]])
        keep = jnp.where(t == 0, 0.0, 1.0)
        self.dq[:, self.cols[e]] = self.dq[:, self.cols[e]] * keep + jnp.dot(self.kt[:, self.keys(t)], self.dsb[e], preferred_element_type=F32)

    def step(self, n):
        n1 = jnp.minimum(n + 1, self.nstep - 1)
        self.scores(n, 1)
        self.soft(n, 0)
        self.grads(jnp.maximum(n - 1, 0), 1)
        self.scores(n1, 0)
        self.soft(n, 1)
        self.grads(n, 0)

    def finish(self, i, e):
        c = self.qcols(i, e)
        g = self.dq[:, self.cols[e]] * SCALE
        hd = HEAD_DIM // PAIR
        cos, sin = self.cs[0:hd, c], self.cs[hd:, c]
        a, b = g[:hd], g[hd:]
        a, b = a * cos + b * sin, b * cos - a * sin
        self.dbq[0:hd, :] += a
        self.dbq[hd:, :] += b
        blk = PAIR * i + e
        self.dqs[blk, 0:hd, :] = a.astype(BF16)
        self.dqs[blk, hd:, :] = b.astype(BF16)

    def run(self, on_step=lambda n: None):
        @turns(self.nstep)
        def _(n):
            on_step(n)
            i, t = decode_up(n, self.nq)

            @pl.when((t == i) & (i > 0) & (i + 1 < self.nq))
            def _():
                for cp in self.loads(i + 1):
                    cp.wait()
            self.step(n)

            @pl.when((t == 0) & (n > 0))
            def _():
                self.finish(i - 1, 1)

                @pl.when(i + 1 < self.nq)
                def _():
                    for cp in self.loads(i + 1):
                        cp.start()

            @pl.when(t == i)
            def _():
                self.finish(i, 0)
        self.grads(self.nstep - 1, 1)
        self.finish(self.nq - 1, 1)


def bwd_scratch(nq, rows):
    vm = pltpu.VMEM
    bk, seq = PAIR * rows, PAIR * rows * nq
    return [vm((seq, PAIR * HEAD_DIM), BF16), vm((HEAD_DIM, seq), BF16), vm((seq, HEAD_DIM), BF16), vm((HEAD_DIM, seq), BF16), vm((OCTET, seq), F32), vm((OCTET, seq), F32),
            vm((PAIR, HEAD_DIM, bk), BF16), vm((PAIR, PAIR * HEAD_DIM, bk), BF16), vm((HEAD_DIM, seq), F32), vm((seq, HEAD_DIM), F32), vm((seq, HEAD_DIM), F32),
            vm((HEAD_DIM, bk), F32), vm((HEAD_DIM, rows), F32), vm((PAIR, bk, rows), F32), vm((PAIR, bk, rows), F32), vm((PAIR, bk, rows), BF16), vm((PAIR, bk, rows), BF16),
            vm((TRIO, bk, rows), F32), vm((PAIR * nq, HEAD_DIM, rows), BF16), pltpu.SemaphoreType.DMA((PAIR, QUAD)), pltpu.SemaphoreType.DMA((PAIR * nq,))]


def load_bwd(k_h, kt_h, v_h, cs_h, lse_h, rows, nblk, kk, kt, vv, cs, lsv, sem):
    cps = [pltpu.make_async_copy(k_h, kk.at[:, 0:HEAD_DIM], sem.at[0]), pltpu.make_async_copy(k_h, kk.at[:, HEAD_DIM:], sem.at[1]),
           pltpu.make_async_copy(kt_h, kt, sem.at[PAIR]), pltpu.make_async_copy(v_h, vv, sem.at[TRIO]), pltpu.make_async_copy(cs_h, cs, sem.at[QUAD])]
    for c in cps:
        c.start()

    cps += [pltpu.make_async_copy(lse_h.at[b, :, 0:rows], lsv.at[:, span(b, rows)], sem.at[5 + b]) for b in range(nblk)]
    for c in cps[5:]:
        c.start()
    return cps


class GradAtt:
    def __init__(self, dy_h, at_h, nb, dat, dlt, wo_v, dyb, atb, sem):
        self.__dict__.update(locals())
        self.blk = dyb.shape[1]

    def copies(self, b):
        s = b % PAIR
        r = pl.ds(pl.multiple_of(b * self.blk, self.blk), self.blk)
        return [pltpu.make_async_copy(self.dy_h.at[r], self.dyb.at[s], self.sem.at[s]),
                pltpu.make_async_copy(self.at_h.at[0:HEAD_DIM, r], self.atb.at[s], self.sem.at[PAIR + s])]

    def start(self, b):
        for c in self.copies(b):
            c.start()

    def block(self, b):
        for c in self.copies(b):
            c.wait()
        d = dot_nt(self.dyb[b % PAIR], self.wo_v[...]).T.astype(BF16)
        r = pl.ds(pl.multiple_of(b * self.blk, self.blk), self.blk)
        self.dat[:, r] = d
        self.dlt[TOP, r] = jnp.sum(d.astype(F32) * self.atb[b % PAIR].astype(F32), axis=KEYS, keepdims=YES)


class Rows:
    def __init__(self, at, ats, rows, sem):
        self.at, self.ats, self.rows, self.sem = at, ats, rows, sem

    def copy(self, i, part):
        cut = self.ats.shape[0] // HEAD_DIM // PAIR * HEAD_DIM
        r = slice(cut, None) if part else slice(0, cut)
        return pltpu.make_async_copy(self.ats.at[r], self.at.at[r, pl.ds(pl.multiple_of(i * self.rows, self.rows), self.rows)], self.sem.at[part])

    def before(self, i, part):
        @pl.when(i > 0)
        def _():
            self.copy(i, part).wait()

    def store(self, g, blk, value):
        self.ats[span(g, HEAD_DIM), :] = value

    def after(self, i, part):
        self.copy(i, part).start()


def k2_kernel(n_sp, own_dy, q2h, k_h, vt_h, dyf, at, lse, ao, kk, vt, ats, *scr):
    *scr, asem, send, recv, drecv, lsem, xsem = scr
    rows = own_dy.shape[0]
    heads = at.shape[0] // HEAD_DIM
    nz = n_sp // PAIR
    sp, dp = lax.axis_index('sp'), lax.axis_index('dp')
    ring = Ring(dyf, own_dy, rows, nz, (send, recv, drecv))
    loads = [pltpu.make_async_copy(k_h, kk.at[:, 0:HEAD_DIM], lsem.at[0]), pltpu.make_async_copy(k_h, kk.at[:, HEAD_DIM:], lsem.at[1]),
             pltpu.make_async_copy(vt_h, vt, lsem.at[PAIR])]
    for c in loads:
        c.start()
    greet(((ring.dp, (ring.z + 1) % nz * PAIR + ring.c), (ring.dp, (ring.z + nz - 1) % nz * PAIR + ring.c), (ring.dp, ring.z * PAIR + 1 - ring.c)))
    ring.start()
    mine = pltpu.make_async_copy(own_dy, dyf.at[pl.ds(pl.multiple_of(sp * rows, rows), rows)], lsem.at[TRIO])
    mine.start()
    for c in loads:
        c.wait()
    sink = Rows(at, ats, rows, asem)
    f = Fwd(n_sp, rows, heads, 0, 1, q2h, sink, lse, kk, vt, *scr)
    f.prepare()

    def due(n):
        return jnp.clip((n - TRIO) // 6, 0, ring.nsend)

    def on_step(n):
        @pl.loop(due(n), due(n + 1))
        def _(j):
            ring.tick(j)
    f.run(on_step)
    f.drain()
    for part in range(PAIR):
        sink.copy(0, part).wait()
    other = (sp // PAIR) * PAIR + 1 - sp % PAIR
    give = pltpu.make_async_remote_copy(
        src_ref=at.at[:, pl.ds(pl.multiple_of(other * rows, rows), rows)], dst_ref=ao, send_sem=xsem.at[0], recv_sem=xsem.at[1],
        device_id=(dp, other), device_id_type=MESH)
    give.start()

    @pl.loop(due(f.nstep), ring.nsend)
    def _(j):
        ring.tick(j)

    for s in range(QUAD):
        ring.wait_other(s)
    ring.d2d_own().wait_recv()
    give.wait()
    mine.wait()
    ring.finish_sends()


def k2(n_sp, own_dy, q2, k, vt):
    rows, dm = own_dy.shape
    seq = rows * n_sp
    heads = q2.shape[PAIR] // rows * 5 // OCTET
    sds, vm, dma = jax.ShapeDtypeStruct, pltpu.VMEM, pltpu.SemaphoreType.DMA
    outs = [sds((seq, dm), BF16), sds((heads * HEAD_DIM, seq), BF16), sds((n_sp, OCTET, heads * rows), F32), sds((heads * HEAD_DIM, rows), BF16)]
    return pl.pallas_call(
        functools.partial(k2_kernel, n_sp), out_shape=outs, in_specs=[ANY] * QUAD, out_specs=[ANY] * QUAD,
        scratch_shapes=[vm((seq, PAIR * HEAD_DIM), BF16), vm((HEAD_DIM, seq), BF16), vm((heads * HEAD_DIM, rows), BF16)] + fwd_scratch(n_sp, rows, heads, 1)
        + [dma((PAIR,))] + ring_sems(n_sp // PAIR) + [dma((QUAD,)), dma((PAIR,))],
        compiler_params=pltpu.CompilerParams(collective_id=1, has_side_effects=YES, vmem_limit_bytes=62 * MIB),
        name='gather_attend')(own_dy, q2, k, vt)


TICK0 = (5, 6, 7, 9, 13, 15, 18, 19, 21, 24, 31, 32, 34, 35)
TICK1 = (10, 20, 25, 26, 27, 33)


class Relay:
    def __init__(self, blk, nr, nz, send, recv):
        self.blk, self.nr, self.nz, self.send, self.recv = blk, nr, nz, send, recv
        sp = lax.axis_index('sp')
        self.dp, self.z, self.c = lax.axis_index('dp'), sp // PAIR, sp % PAIR

    def copy(self, d, s, r):
        origin = (self.z + (self.nz - s if d == 0 else s)) % self.nz
        to = (self.z + (1 if d == 0 else self.nz - 1)) % self.nz
        ref = self.blk(origin, r)
        i = s * self.nr + r
        return pltpu.make_async_remote_copy(src_ref=ref, dst_ref=ref, send_sem=self.send.at[d], recv_sem=self.recv.at[d, i],
                                            device_id=(self.dp, to * PAIR + self.c), device_id_type=MESH)

    def own(self, r):
        for d in range(PAIR):
            self.copy(d, 0, r).start()

    def tick(self, s, r):
        for d in range(PAIR):
            if s == TRIO:
                @pl.when(r % PAIR == d)
                def _():
                    self.copy(d, TRIO, r).wait_recv()
            else:
                self.copy(d, s, r).wait_recv()
                if s == PAIR:
                    @pl.when(r % PAIR == d)
                    def _():
                        self.copy(d, TRIO, r).start()
                else:
                    self.copy(d, s + 1, r).start()

    def ticks(self, s, lo, hi):
        @pl.loop(lo, hi)
        def _(r):
            self.tick(s, r)

    def finish(self, ref):
        for d in range(PAIR):
            pltpu.make_async_copy(ref, ref, self.send.at[d]).wait()


def k3_kernel(nq, rows, dims, x_h, dyo_h, par, qt, q2h, at, ao, lse, k_h, kt_h, v_h, vt_h, cs_h, ht_h, dy_h, wq_h, wk_h, wv_h, wo_h,
              y_o, dx_o, dwq_o, dwo_o, small_o, kv_o, kvf_o,
              kk, vt, ao2, cs, dk, dv, dqa, dqo, rs, kva, kvo, sma, smo, qsend, qrecv, rsend, rrecv, ksend, krecv, xsend, xrecv, ssend, srecv, tsend, trecv, tl, lq):
    nz, n_sp, heads = dims
    nblk = PAIR * nq
    hd = HEAD_DIM // PAIR
    qw = heads * HEAD_DIM
    bk = PAIR * rows
    dm = x_h.shape[1]
    cw = PAIR * HEAD_DIM
    vm = pltpu.VMEM
    dma = pltpu.SemaphoreType.DMA
    sp, dp = lax.axis_index('sp'), lax.axis_index('dp')
    z, c = sp // PAIR, sp % PAIR
    far = 1 - c
    other = z * PAIR + 1 - c
    peer = dict(device_id=(dp, other), device_id_type=MESH)

    relay = Relay(lambda o, r: dqa.at[o, r], nblk, nz, qsend, qrecv)
    kvr = Relay(lambda o, r: kva.at[o, pl.ds(pl.multiple_of(r * HEAD_DIM, HEAD_DIM), HEAD_DIM)], PAIR, nz, ksend, krecv)
    all_here = greet_all(n_sp)
    sma[sp] = jnp.zeros(sma.shape[1:], F32)

    nstep = bwd_steps(nq)
    own_at = [(r // PAIR + 1) * (r // PAIR + PAIR) // PAIR + r % PAIR + PAIR for r in range(nblk)]

    def count(n, at_step):
        return sum((n >= a).astype(jnp.int32) for a in at_step)

    def back(*scr):
        *scr, wo_v, dyb, atb, sem, sem2 = scr
        kt, vv, dat, dlt, lsv, qb, q2, dq, dbq, sb, dpb, pb, dsb, bias, psem = scr
        row0 = pl.multiple_of(c * qw + z * HEAD_DIM, HEAD_DIM)
        w_in = pltpu.make_async_copy(wo_h.at[pl.ds(row0, HEAD_DIM)], wo_v, sem2.at[QUAD])
        w_in.start()
        vt_in = pltpu.make_async_copy(vt_h, vt, lq.at[0])
        vt_in.start()
        ga = GradAtt(dy_h, at, nq, dat, dlt, wo_v, dyb, atb, sem2)
        ga.start(0)
        kin = load_bwd(k_h, kt_h, v_h, cs_h, lse, rows, nblk, kk, kt, vv, cs, lsv, sem)
        ga.start(1)
        b = Bwd(nq, rows, qt, q2h, kk, kt, vv, dat, dlt, lsv, qb, q2, cs, dk, dv, dq, dbq, sb, dpb, pb, dsb, bias, dqa.at[z], psem)
        b.clear()
        w_in.wait()
        ga.block(0)
        for cp in kin:
            cp.wait()
        vt_in.wait()
        all_here()
        b.prepare()
        t0 = [min(t, nstep) + 1 for t in TICK0]
        t1 = [min(t, nstep) + 1 for t in TICK1]

        def on_step(n):
            @pl.loop(count(n, own_at), count(n + 1, own_at))
            def _(r):
                relay.own(r)
            relay.ticks(0, count(n, t0), count(n + 1, t0))
            relay.ticks(1, count(n, t1), count(n + 1, t1))
            i, t = decode_up(n, nq)

            @pl.when((t == 0) & (i + 1 < nq))
            def _():
                @pl.when(i + PAIR < nq)
                def _():
                    ga.start(i + PAIR)
                ga.block(i + 1)
        b.run(on_step)
        own_in = sum(1 for a in own_at if a <= nstep)

        @pl.loop(own_in, nblk)
        def _(r):
            relay.own(r)
        sma[sp, 16:17, :] = jnp.sum(dbq[...].T, axis=KEYS, keepdims=YES)
    scr = bwd_scratch(nq, rows)
    keep = scr[1:OCTET] + scr[11:18] + [scr[19]]
    pl.run_scoped(back, *keep, vm((HEAD_DIM, dm), BF16), vm((PAIR, bk, dm), BF16), vm((PAIR, HEAD_DIM, bk), BF16), dma((5 + nblk,)), dma((5,)))
    h0, h1 = sum(1 for t in TICK0 if t + 1 <= nstep), sum(1 for t in TICK1 if t + 1 <= nstep)

    def rs_block(d, s):
        b = (z + (PAIR * nz - 1 - s if d == 0 else 1 + s)) % nz
        return (dk if d == 0 else dv).at[pl.ds(pl.multiple_of(b * bk, bk), bk)]

    def rs_copy(d, s):
        to = (z + (1 if d == 0 else nz - 1)) % nz
        return pltpu.make_async_remote_copy(src_ref=rs_block(d, 0) if s == 0 else rs.at[d, s - 1], dst_ref=rs.at[d, s],
                                            send_sem=rsend.at[d], recv_sem=rrecv.at[d, s], device_id=(dp, to * PAIR + c), device_id_type=MESH)
    for d in range(PAIR):
        rs_copy(d, 0).start()

    def rs_step(s):
        for d in range(PAIR):
            rs_copy(d, s - 1).wait_recv()
            rs[d, s - 1] = rs[d, s - 1] + rs_block(d, s)[...]
        for d in range(PAIR):
            rs_copy(d, s).start()

    kv_give = pltpu.make_async_remote_copy(src_ref=kva.at[z, :, pl.ds(pl.multiple_of(far * rows, rows), rows)], dst_ref=kvo,
                                           send_sem=xsend.at[0], recv_sem=xrecv.at[0], **peer)

    def keys_whole():
        for d in range(PAIR):
            rs_copy(d, nz - PAIR).wait_recv()
        own = pl.ds(pl.multiple_of(z * bk, bk), bk)
        g = ((rs[0, nz - PAIR] + dk[own, :]) * SCALE).T
        a, b = g[:hd], g[hd:]
        cos, sin = cs[0:hd, own], cs[hd:, own]
        g = jnp.concatenate([a * cos + b * sin, b * cos - a * sin], axis=KEYS)
        sma[sp, 17:18, :] = jnp.sum(g.T, axis=KEYS, keepdims=YES)
        kva[z, 0:HEAD_DIM, :] = g.astype(BF16)
        g = rs[1, nz - PAIR] + dv[own, :]
        sma[sp, 18:19, :] = jnp.sum(g, axis=KEYS, keepdims=YES)
        kva[z, HEAD_DIM:, :] = g.T.astype(BF16)
        for r in range(PAIR):
            kvr.own(r)
        kv_give.start()
        kv_far(z).start()

    def kv_far(o):
        return pltpu.make_async_remote_copy(src_ref=kva.at[o], dst_ref=kvf_o.at[o], send_sem=tsend.at[0, PAIR], recv_sem=trecv.at[1], **peer)

    def kv_tick(s):
        kvr.ticks(s, 0, PAIR)
        for o in (((z + nz - 1 - s) % nz, (z + 1 + s) % nz) if s < TRIO else ((z + nz // PAIR) % nz,)):
            kv_far(o).start()

    def late(tile, aT, hta, sem):
        nslot = tile.shape[0]
        ht_in = [pltpu.make_async_copy(ht_h.at[0:qw], hta, lq.at[1])]

        def put(dst, piece, e):
            slot = piece % nslot
            src = tile.at[slot, :, span(e, HEAD_DIM)]
            return (pltpu.make_async_copy(src, dst, tl.at[slot, e]),
                    pltpu.make_async_remote_copy(src_ref=src, dst_ref=dst, send_sem=tsend.at[slot, e], recv_sem=trecv.at[0], **peer))

        def give(dsts, piece):
            for e in range(PAIR):
                for cp in put(dsts[e], piece, e):
                    cp.start()

        def free(piece):
            for e in range(PAIR):
                a, b = put(dwo_o.at[0:qw, 0:HEAD_DIM], piece, e)
                a.wait()
                b.wait_send()

        def att_part(atv, aob, xo, hsem):
            have = at.shape[0] // HEAD_DIM

            def head_rows(g):
                return pl.ds(pl.multiple_of((z + g) % heads * HEAD_DIM, HEAD_DIM), HEAD_DIM)

            def spread(src, dst, base):
                return [pltpu.make_async_copy(src.at[span(g, HEAD_DIM)], dst.at[head_rows(g)], hsem.at[base + g]) for g in range(have)]
            ins = spread(at, atv, 0) + spread(ao, aob, heads) + [pltpu.make_async_copy(x_h, xo, lq.at[TRIO])]
            for cp in ins:
                cp.start()
            turn_rs, turn0, turn1 = [6, 12, 18, 24, 30, 36], [PAIR, PAIR], [QUAD, 15, 27]

            class Here:
                def before(self, i, part):
                    pass

                def store(self, g, blk, value):
                    atv[head_rows(have + g), pl.ds(pl.multiple_of(blk * rows, rows), rows)] = value

                def after(self, i, part):
                    pass

            def rest(*fscr):
                f = Fwd(nblk, rows, heads - have, have, PAIR, q2h, Here(), None, kk, vt, *fscr)
                f.prepare()

                def on_step(n):
                    relay.ticks(0, h0 + count(n, turn0), h0 + count(n + 1, turn0))
                    relay.ticks(1, h1 + count(n, turn1), h1 + count(n + 1, turn1))
                    for s in range(1, nz - 1):
                        @pl.when(n + 1 == turn_rs[s - 1])
                        def _():
                            rs_step(s)
                f.run(on_step)
                f.drain()
            pl.run_scoped(rest, *fwd_scratch(nblk, rows, PAIR * (heads - have), PAIR))
            gives = [pltpu.make_async_remote_copy(src_ref=atv.at[head_rows(have + g), pl.ds(pl.multiple_of(other * rows, rows), rows)],
                                                  dst_ref=ao2.at[span(g, HEAD_DIM)], send_sem=xsend.at[PAIR + g], recv_sem=xrecv.at[PAIR + g], **peer)
                     for g in range(heads - have)]
            for cp in ins:
                cp.wait()

            def products(dyt, wt):
                nw = wt.shape[0]

                def dy_tile(n):
                    return pltpu.make_async_copy(dy_h.at[:, pl.ds(pl.multiple_of(n * cw, cw), cw)], dyt.at[n % PAIR], sem.at[n % PAIR])

                def w_tile(n):
                    return pltpu.make_async_copy(wo_h.at[:, pl.ds(pl.multiple_of(n * cw, cw), cw)], wt.at[n % nw], sem.at[PAIR + n % nw])
                dy_tile(0).start()
                for cp in gives:
                    cp.start()
                ntile = dm // cw
                w1 = [1, PAIR, TRIO, QUAD, 5, 6, 7]
                k1 = h1 + len(turn1)

                @turns(ntile)
                def _(n):
                    @pl.when(n + 1 < ntile)
                    def _():
                        dy_tile(n + 1).start()

                    @pl.when(n == 1)
                    def _():
                        ht_in[0].start()

                    @pl.when(n == QUAD)
                    def _():
                        for i in range(nw - 1):
                            w_tile(i).start()
                    relay.ticks(1, k1 + count(n, w1), k1 + count(n + 1, w1))

                    @pl.when(n == TRIO)
                    def _():
                        keys_whole()

                    @pl.when(n == ntile - 1)
                    def _():
                        kv_tick(0)
                    dy_tile(n).wait()

                    @pl.when(n >= nslot)
                    def _():
                        free(n - nslot)
                    tile[n % nslot] = jnp.dot(atv[...], dyt[n % PAIR], preferred_element_type=F32)
                    rws = pl.ds(pl.multiple_of(c * qw, qw), qw)
                    give([dwo_o.at[rws, pl.ds(pl.multiple_of(n * cw + e * HEAD_DIM, HEAD_DIM), HEAD_DIM)] for e in range(PAIR)], n)
                relay.ticks(PAIR, 0, nblk // PAIR)

                for cp in gives:
                    cp.wait()
                for g in range(heads - have):
                    aob[head_rows(have + g), :] = ao2[span(g, HEAD_DIM), :]
                aT[:, pl.ds(pl.multiple_of(c * qw, qw), qw)] = atv[:, pl.ds(pl.multiple_of(sp * rows, rows), rows)].T
                aT[:, pl.ds(pl.multiple_of(far * qw, qw), qw)] = aob[...].T

                @turns(ntile)
                def _(n):
                    @pl.when(n + nw - 1 < ntile)
                    def _():
                        w_tile(n + nw - 1).start()
                    w_tile(n).wait()
                    cl = pl.ds(pl.multiple_of(n * cw, cw), cw)
                    xo[:, cl] = (xo[:, cl].astype(F32) + jnp.dot(aT[...], wt[n % nw], preferred_element_type=F32)).astype(BF16)
                out = pltpu.make_async_copy(xo, y_o, lq.at[PAIR])
                out.start()
                out.wait()
            pl.run_scoped(products, vm((PAIR, dy_h.shape[0], cw), BF16), vm((TRIO, dm, cw), BF16))
        pl.run_scoped(att_part, vm((qw, dy_h.shape[0]), BF16), vm((qw, rows), BF16), vm((rows, dm), BF16), dma((PAIR * heads,)))
        pl.run_scoped(functools.partial(later, tile, aT, hta, ht_in[0], sem, nslot, give, free), vm((dm - qw, nblk * rows), BF16))

    def later(tile, aT, hta, hta_in, sem, nslot, give, free, htb):
        htb_in = pltpu.make_async_copy(ht_h.at[qw:], htb, lq.at[0])
        htb_in.start()
        nm = dm // qw
        once = jnp.minimum(z + 1, 1)

        def product(rhs_of, cols_of, nr, m, piece):
            free(piece - nslot)


            @turns(once)
            def _(_):
                acc = None
                for r in range(nr):
                    part = dot_nt((hta, htb)[m][:, cols_of(r)], rhs_of(r))
                    acc = part if acc is None else acc + part
                tile[piece % nslot] = acc

        def pair(p, piece, between):
            ha = (z + nz - p) % nz
            hb = jnp.where(p < nz // PAIR, (z + p) % nz, z)
            for m in range(nm):
                product(lambda r: jnp.concatenate([dqa[ha, r], dqa[hb, r]], axis=KEYS), lambda r: span(r, rows), nblk, m, piece + m)
                give([dwq_o.at[span(m, qw), pl.ds(pl.multiple_of(c * qw + h * HEAD_DIM, HEAD_DIM), HEAD_DIM)] for h in (ha, hb)], piece + m)
                if m == 0:
                    between()
        hta_in.wait()
        base = dm // cw
        def small(o):
            return pltpu.make_async_remote_copy(src_ref=sma.at[sp], dst_ref=sma.at[sp], send_sem=ssend.at[0], recv_sem=srecv.at[0],
                                                device_id=(dp, (sp + o) % n_sp), device_id_type=MESH)

        def in_rows(wr, xo, dyo, wkv, dkp, dn):
            ins = [pltpu.make_async_copy(x_h, xo, lq.at[PAIR]), pltpu.make_async_copy(dyo_h, dyo, lq.at[TRIO]),
                   pltpu.make_async_copy(wk_h, wkv.at[0], lq.at[5]), pltpu.make_async_copy(wv_h, wkv.at[1], lq.at[6])]
            for cp in ins:
                cp.start()

            nw = wr.shape[0]

            def w_tile(n):
                return pltpu.make_async_copy(wq_h.at[pl.ds(pl.multiple_of(n * cw, cw), cw)], wr.at[n % nw], sem.at[n % nw])
            for i in range(nw - 1):
                w_tile(i).start()
            dq_give = pltpu.make_async_remote_copy(src_ref=dqa.at[:, other], dst_ref=dqo, send_sem=xsend.at[1], recv_sem=xrecv.at[1], **peer)
            kv_tick(1)
            relay.ticks(PAIR, nblk // PAIR, nblk)
            def own_rows():
                kv_give.wait()
                dq_give.wait()
                for cp in ins:
                    cp.wait()
                for h in range(nz):
                    aT[:, pl.ds(pl.multiple_of(c * qw + h * HEAD_DIM, HEAD_DIM), HEAD_DIM)] = dqa[h, sp].T
                    aT[:, pl.ds(pl.multiple_of(far * qw + h * HEAD_DIM, HEAD_DIM), HEAD_DIM)] = dqo[h].T
                for e in range(PAIR):
                    er = span(e, HEAD_DIM)
                    dkp[e, :, pl.ds(pl.multiple_of(c * HEAD_DIM, HEAD_DIM), HEAD_DIM)] = kva[z, er, pl.ds(pl.multiple_of(c * rows, rows), rows)].T
                    dkp[e, :, pl.ds(pl.multiple_of(far * HEAD_DIM, HEAD_DIM), HEAD_DIM)] = kvo[er, :].T

                @turns(dm // cw)
                def _(n):
                    @pl.when(n + nw - 1 < dm // cw)
                    def _():
                        w_tile(n + nw - 1).start()
                    w_tile(n).wait()
                    rr = pl.ds(pl.multiple_of(n * cw, cw), cw)
                    dn[:, rr] = dot_nt(aT[...], wr[n % nw]) + dot_nt(dkp[0], wkv[0, rr, :]) + dot_nt(dkp[1], wkv[1, rr, :])
                nr = 16
                gain = jnp.concatenate([par[g:g + 1, :] for g in range(dm // HEAD_DIM)], axis=1)

                @turns(rows // nr)
                def _(i):
                    rr = pl.ds(pl.multiple_of(i * nr, nr), nr)
                    xf = xo[rr, :].astype(F32)
                    inv = lax.rsqrt(jnp.mean(xf * xf, axis=-1, keepdims=YES) + NORM_EPS)
                    unit = xf * inv
                    g = dn[rr, :]
                    du = g * gain
                    di = inv * (du - unit * jnp.mean(du * unit, axis=-1, keepdims=YES))
                    xo[rr, :] = (dyo[rr, :].astype(F32) + di).astype(BF16)
                    dn[rr, :] = g * unit
                tot = jnp.sum(dn[...], axis=KEYS, keepdims=YES)
                for j in range(dm // HEAD_DIM):
                    sma[sp, j:j + 1, :] = tot[:, span(j, HEAD_DIM)]
                pltpu.make_async_copy(xo, dx_o, lq.at[PAIR]).start()

                @pl.loop(1, n_sp)
                def _(o):
                    small(o).start()

            @turns(nz // PAIR)
            def _(q):
                @pl.when(q == PAIR)
                def _():
                    kv_tick(PAIR)

                @pl.when(q == TRIO)
                def _():
                    relay.ticks(TRIO, 0, nblk)
                    dq_give.start()
                    own_rows()

                def between():
                    @pl.when(q == 0)
                    def _():
                        htb_in.wait()
                pair(q + 1, base + q * nm, between)
            pltpu.make_async_copy(xo, dx_o, lq.at[PAIR]).wait()
        pl.run_scoped(in_rows, vm((QUAD, cw, dm), BF16), vm((rows, dm), BF16), vm((rows, dm), BF16), vm((PAIR, dm, cw), BF16),
                      vm((PAIR, rows, cw), BF16), vm((rows, dm), F32))

        kv_tick(TRIO)
        kv_out = pltpu.make_async_copy(kva, kv_o, lq.at[0])
        kv_out.start()
        npiece = base + QUAD * nm
        for i in range(nslot):
            free(npiece - nslot + i)

        pltpu.make_async_copy(dwo_o, dwo_o, trecv.at[0]).wait()
        pltpu.make_async_copy(kvf_o, kvf_o, trecv.at[1]).wait()
        pltpu.make_async_copy(kvf_o, kvf_o, tsend.at[0, PAIR]).wait()
        kv_out.wait()
        ref = sma.at[pl.ds(0, n_sp - 1)]
        pltpu.make_async_copy(ref, ref, ssend.at[0]).wait()
        pltpu.make_async_copy(ref, ref, srecv.at[0]).wait()
        ng = dm // HEAD_DIM
        tot = sma[0, 0:ng, :]
        for o in range(1, n_sp):
            tot = tot + sma[o, 0:ng, :]
        smo[0:ng, :] = tot
        for cc in range(PAIR):
            for zz in range(nz):
                smo[ng + cc * nz + zz:ng + cc * nz + zz + 1, :] = sma[zz * PAIR + cc, 16:17, :]
            for e in range(PAIR):
                tot = sma[cc, 17 + e:18 + e, :]
                for zz in range(1, nz):
                    tot = tot + sma[zz * PAIR + cc, 17 + e:18 + e, :]
                smo[PAIR * ng + PAIR * e + cc:PAIR * ng + PAIR * e + cc + 1, :] = tot
        out = pltpu.make_async_copy(smo, small_o, lq.at[PAIR])
        out.start()
        out.wait()
    pl.run_scoped(late, vm((TRIO, qw, cw), F32), vm((rows, dm), BF16), vm((qw, nblk * rows), BF16), dma((6,)))
    relay.finish(ht_h.at[0:7 * HEAD_DIM // PAIR, :])
    kvr.finish(dy_h.at[0:7 * HEAD_DIM * bk // dm, :])
    for d in range(PAIR):
        pltpu.make_async_copy(rs.at[d], rs.at[d], rsend.at[d]).wait()


def k3(n_sp, x, dy_own, par, qt, q2, at, ao, lse, k, kt, v, vt, cs, ht, dyf, wq, wk, wv, wo):
    rows, dm = x.shape
    nblk, seq, nz = qt.shape[0], k.shape[0], n_sp // PAIR
    heads = qt.shape[PAIR] // rows
    npiece = dm // (PAIR * HEAD_DIM) + 5 * (dm // (heads * HEAD_DIM))
    sds, vm, dma = jax.ShapeDtypeStruct, pltpu.VMEM, pltpu.SemaphoreType.DMA
    ns = PAIR * (dm // HEAD_DIM) + OCTET
    scratch = [vm((seq, PAIR * HEAD_DIM), BF16), vm((HEAD_DIM, seq), BF16), vm((heads * HEAD_DIM - at.shape[0], rows), BF16), vm((HEAD_DIM, seq), F32), vm((seq, HEAD_DIM), F32), vm((seq, HEAD_DIM), F32), vm((nz, nblk, HEAD_DIM, rows), BF16), vm((nz, HEAD_DIM, rows), BF16),
               vm((PAIR, nz - 1, PAIR * rows, HEAD_DIM), F32), vm((nz, PAIR * HEAD_DIM, PAIR * rows), BF16), vm((PAIR * HEAD_DIM, rows), BF16), vm((n_sp, 24, HEAD_DIM), F32), vm((ns, HEAD_DIM), F32),
               dma((PAIR,)), dma((PAIR, QUAD * nblk)), dma((PAIR,)), dma((PAIR, nz - 1)), dma((PAIR,)), dma((PAIR, OCTET)), dma((5,)), dma((5,)),
               dma((1,)), dma((1,)), dma((QUAD, TRIO)), dma((PAIR,)), dma((QUAD, PAIR)), dma((OCTET,))]
    outs = [sds((rows, dm), BF16), sds((rows, dm), BF16), sds(wq.shape, F32), sds(wo.shape, F32), sds((ns, HEAD_DIM), F32)] + [sds((nz, PAIR * HEAD_DIM, PAIR * rows), BF16)] * PAIR
    return pl.pallas_call(
        functools.partial(k3_kernel, nblk // PAIR, rows, (nz, n_sp, heads)), out_shape=outs, in_specs=[ANY, ANY, VM] + [ANY] * 16, out_specs=[ANY] * len(outs),
        scratch_shapes=scratch, compiler_params=pltpu.CompilerParams(collective_id=PAIR, has_side_effects=YES, vmem_limit_bytes=63 * MIB),
        name='attend_back')(x, dy_own, par, qt, q2, at, ao, lse, k, kt, v, vt, cs, ht, dyf, wq, wk, wv, wo)


def k4_kernel(y_h, dx_h, dwq_h, dwo_h, small, kv_h, kvf_h, ht_h, y_o, dx_o, dwq_o, dwk_o, dwv_o, dwo_o, g_o, bq_o, bk_o, bv_o,
              buf, hbuf, kv, hts, wt, isem, osem, hsem, wsem, ksem):
    nslot, half = buf.shape[0], buf.shape[0]
    dm, rc = dwq_h.shape[0], buf.shape[1]
    c = lax.axis_index('sp') % PAIR
    for i, (src, dst) in enumerate(((y_h, y_o), (dx_h, dx_o))):
        pltpu.make_async_copy(src, hbuf.at[i], hsem.at[i]).start()
    kin = [pltpu.make_async_copy(kv_h, kv.at[c], ksem.at[0]), pltpu.make_async_copy(kvf_h, kv.at[1 - c], ksem.at[1])]
    for cp in kin:
        cp.start()
    ng = dm // HEAD_DIM
    g_o[...] = small[0:ng, :]
    bq_o[...] = small[ng:PAIR * ng, :]
    bk_o[...] = small[PAIR * ng:PAIR * ng + PAIR, :]
    bv_o[...] = small[PAIR * ng + PAIR:PAIR * ng + QUAD, :]
    n = dm // rc
    work = [(src, dst, i) for i in range(n) for src, dst in ((dwq_h, dwq_o), (dwo_h, dwo_o))]

    def into(i):
        return pltpu.make_async_copy(work[i][0].at[pl.ds(work[i][PAIR] * rc, rc)], buf.at[i % nslot], isem.at[i % nslot])

    def out(i):
        return pltpu.make_async_copy(buf.at[i % nslot], work[i][1].at[pl.ds(work[i][PAIR] * rc, rc)], osem.at[i % nslot])
    mr = hts.shape[1]

    def ht_in(m):
        return pltpu.make_async_copy(ht_h.at[pl.ds(pl.multiple_of(m * mr, mr), mr)], hts.at[m % PAIR], wsem.at[m % PAIR])

    def w_out(m):
        return [pltpu.make_async_copy(wt.at[m % PAIR, e], d.at[pl.ds(pl.multiple_of(m * mr, mr), mr)], wsem.at[PAIR + PAIR * e + m % PAIR]) for e, d in enumerate((dwk_o, dwv_o))]
    for i in range(half):
        into(i).start()
    ht_in(0).start()
    for cp in kin:
        cp.wait()
    steps = dm // mr
    per = len(work) // steps
    for m in range(steps):
        if m + 1 < steps:
            ht_in(m + 1).start()
        for i in range(m * per, (m + 1) * per):
            into(i).wait()
            out(i).start()
            if i >= half:
                out(i - half).wait()
            if i + half < len(work):
                into(i + half).start()
        ht_in(m).wait()
        if m >= PAIR:
            for cp in w_out(m - PAIR):
                cp.wait()

        @turns(PAIR)
        def _(p):
            acc = None
            w = kv.shape[TRIO]
            for o in range(kv.shape[1]):
                part = dot_nt(hts[m % PAIR, :, span(o, w)], kv[p, o])
                acc = part if acc is None else acc + part
            cols = pl.ds(pl.multiple_of(p * HEAD_DIM, HEAD_DIM), HEAD_DIM)
            for e in range(PAIR):
                wt[m % PAIR, e, :, cols] = acc[:, span(e, HEAD_DIM)]
        for cp in w_out(m):
            cp.start()
    for i, (src, dst) in enumerate(((y_h, y_o), (dx_h, dx_o))):
        pltpu.make_async_copy(src, hbuf.at[i], hsem.at[i]).wait()
        pltpu.make_async_copy(hbuf.at[i], dst, hsem.at[PAIR + i]).start()
    for i in range(len(work) - half, len(work)):
        out(i).wait()
    for m in (steps - PAIR, steps - 1):
        for cp in w_out(m):
            cp.wait()
    for i, (src, dst) in enumerate(((y_h, y_o), (dx_h, dx_o))):
        pltpu.make_async_copy(hbuf.at[i], dst, hsem.at[PAIR + i]).wait()


def k4(y, dx, dwq, dwo, small, kv, kvf, ht):
    dm, ng = dwq.shape[0], dwq.shape[0] // HEAD_DIM
    sds, vm, dma = jax.ShapeDtypeStruct, pltpu.VMEM, pltpu.SemaphoreType.DMA
    wide = PAIR * HEAD_DIM
    outs = [sds(y.shape, BF16), sds(dx.shape, BF16), sds(dwq.shape, F32), sds((dm, wide), F32), sds((dm, wide), F32), sds(dwo.shape, F32),
            sds((ng, HEAD_DIM), F32), sds((ng, HEAD_DIM), F32), sds((PAIR, HEAD_DIM), F32), sds((PAIR, HEAD_DIM), F32)]
    return pl.pallas_call(
        k4_kernel, out_shape=outs, in_specs=[ANY] * QUAD + [VM] + [ANY] * TRIO, out_specs=[ANY] * 6 + [VM] * QUAD,
        scratch_shapes=[vm((16, 256, dwq.shape[1]), F32), vm((PAIR,) + y.shape, BF16), vm((PAIR,) + kv.shape, BF16), vm((PAIR, dm // QUAD, ht.shape[1]), BF16),
                        vm((PAIR, PAIR, dm // QUAD, wide), F32), dma((16,)), dma((16,)), dma((QUAD,)), dma((6,)), dma((PAIR,))],
        compiler_params=pltpu.CompilerParams(vmem_limit_bytes=60 * MIB), name='place')(y, dx, dwq, dwo, small, kv, kvf, ht)


def solution(mesh):
    n_sp = mesh.shape['sp']

    def step(hidden, d_out, positions, norm_gain, w_query, b_query, w_key, b_key, w_value, b_value, w_out):
        x, dy = hidden[0], d_out[0]
        rows, dm = x.shape
        par = jnp.concatenate([b.astype(F32).reshape(-1, HEAD_DIM) for b in (norm_gain, b_query, b_key, b_value)])
        hf, ht, qt, k, kt, v, vt, cs, q2 = k1(n_sp, x, positions, par, w_query, w_key, w_value)
        dyf, at, lse, ao = k2(n_sp, dy, q2, k, vt)
        y, dx, dwq, dwo, small, kv, kvf = k3(n_sp, x, dy, par, qt, q2, at, ao, lse, k, kt, v, vt, cs, ht, dyf, w_query, w_key, w_value, w_out)
        y, dx, dwq, dwk, dwv, dwo, dg, dbq, dbk, dbv = k4(y, dx, dwq, dwo, small, kv, kvf, ht)
        return y[None], dx[None], dg.reshape(-1), dwq, dbq.reshape(-1), dwk, dbk.reshape(-1), dwv, dbv.reshape(-1), dwo

    seq_spec = P('dp', 'sp', None)
    in_specs = (seq_spec, seq_spec, P('dp', 'sp')) + (P(),) * OCTET
    out_specs = (seq_spec, seq_spec, P('dp'), P('dp', None), P('dp'), P('dp', None), P('dp'), P('dp', None), P('dp'), P('dp', None))
    return jax.shard_map(step, mesh=mesh, in_specs=in_specs, out_specs=out_specs, check_vma=False)
```
